128 devices in a mesh: dp: 2 (over x_hi), seq: 8 (over x_lo, z), tensor: 8 (over y, core).
Axes of the slice: x: 4 (x_hi: 2, x_lo: 2; x = x_hi * 2 + x_lo), y: 4, z: 4, core: 2. Of those that a mesh axis runs over, the one named last changes fastest.
Arguments:
- image_states: bfloat16 [2, 4096, 3072], P('dp', 'seq', 'tensor'), may hold values from -6 to 6
- text_states: bfloat16 [4, 512, 3072], P(None, 'seq', 'tensor'), may hold values from -6 to 6
- image_qkv: bfloat16 [3072, 3, 3072], P(None, None, 'tensor'), may hold values from -0.109375 to 0.109375
- text_qkv: bfloat16 [3072, 3, 3072], P(None, None, 'tensor'), may hold values from -0.109375 to 0.109375
- image_out: bfloat16 [3072, 3072], P('tensor'), may hold values from -0.109375 to 0.109375
- final_weight: bfloat16 [3072, 64], replicated, may hold values from -0.109375 to 0.109375
- query_gain: float32 [128], replicated, may hold values from 1.5 to 2.5
- key_gain: float32 [128], replicated, may hold values from 1.5 to 2.5
- modulation: float32 [10, 7, 3072], replicated, may hold values from -3 to 3
- latent: float32 [2, 4096, 64], P('dp', ('seq', 'tensor')), may hold values from -6 to 6
- old_velocity: bfloat16 [2, 4096, 64], P('dp', ('seq', 'tensor')), may hold values from -6 to 6
- rollout_noise: float32 [2, 4096, 64], P('dp', ('seq', 'tensor')), may hold values from -6 to 6
- group_ids: int32 [2], P('dp'), may hold values from 0 to 3
- text_lengths: int32 [4], replicated, may hold values from 128 to 512
- step_ids: int32 [2], P('dp'), may hold values from 0 to 9
Outputs:
- step_mean: float32 [2, 4096, 64], P('dp', ('seq', 'tensor'))
- log_ratio: float32 [2], P('dp')
The draws below stay inside these ranges and needn't reach their ends.
All inputs are finite; a program needn't handle non-finite values.
Results may differ from the reference program's by a relative error of at most 0.0023.
Values may be sent and summed in bfloat16 or wider, within the bound.
A program may use at most 192 MiB of HBM per device.

```python
import math
import jax
import jax.numpy as jnp
from jax import lax

D = 3072
HEADS = 24
HEAD_DIM = 128
CH = 64
STEPS_ALL = 10
PROMPTS = 4
IMG = 4096
TXT = 512
SAMPLES = 2


def touch_ends(array, own_key, smallest, largest):
    longest = array.shape.index(max(array.shape))
    spots = []
    for shift in (0, 1):
        where = [jax.random.randint(jax.random.fold_in(own_key, axis), (), 0, length) for axis, length in enumerate(array.shape)]
        where[longest] = (where[longest] + shift) % array.shape[longest]
        spots.append(tuple(where))
    return array.at[spots[0]].set(smallest).at[spots[1]].set(largest)


def block_levels(stream_key, extent, pieces, least, largest):
    def one(position, shards_of):
        heights = jax.random.uniform(jax.random.fold_in(jax.random.fold_in(stream_key, 6), position), (shards_of,), jnp.float32, least / len(pieces), largest / len(pieces))
        return jnp.repeat(jnp.exp(heights), extent[position] // shards_of).reshape((-1,) + (1,) * (len(extent) - position - 1))

    loudness = one(*pieces[0])
    for cut in pieces[1:]:
        loudness = loudness * one(*cut)
    return loudness


def bell_draw(key, shape, scale, bound, split=(), held_as=jnp.bfloat16):
    entries = jax.random.normal(key, shape, jnp.float32) * scale
    if len(split) > 0:
        entries = block_levels(key, shape, split, -0.22, 0.18) * entries
    return jnp.clip(entries, min=-bound, max=bound).astype(held_as)


def setup_inputs(seed: int = 0) -> dict:
    key_list = jax.random.split(jax.random.key(seed), 16)
    return {
        "image_states": bell_draw(key_list[0], (SAMPLES, IMG, D), 1.0, 6.0, ((0, 2), (1, 8), (2, 8))),
        "text_states": bell_draw(key_list[1], (PROMPTS, TXT, D), 1.0, 6.0, ((1, 8), (2, 8))),
        "image_qkv": bell_draw(key_list[2], (D, 3, D), D ** -0.5, 0.109375, ((2, 8),)),
        "text_qkv": bell_draw(key_list[3], (D, 3, D), D ** -0.5, 0.109375, ((2, 8),)),
        "image_out": bell_draw(key_list[4], (D, D), D ** -0.5, 0.109375, ((0, 8),)),
        "final_weight": bell_draw(key_list[5], (D, CH), D ** -0.5, 0.109375),
        "query_gain": jnp.clip(jax.random.uniform(key_list[6], (HEAD_DIM,), jnp.float32, 1.5, 2.5), 1.5, 2.5),
        "key_gain": jnp.clip(jax.random.uniform(key_list[7], (HEAD_DIM,), jnp.float32, 1.5, 2.5), 1.5, 2.5),
        "modulation": bell_draw(key_list[8], (STEPS_ALL, 7, D), 0.5, 3.0, (), jnp.float32),
        "latent": bell_draw(key_list[9], (SAMPLES, IMG, CH), 1.0, 6.0, ((0, 2), (1, 64)), jnp.float32),
        "old_velocity": bell_draw(key_list[10], (SAMPLES, IMG, CH), 1.0, 6.0, ((0, 2), (1, 64))),
        "rollout_noise": bell_draw(key_list[11], (SAMPLES, IMG, CH), 1.0, 6.0, ((0, 2), (1, 64)), jnp.float32),
        "group_ids": jax.random.randint(key_list[12], (SAMPLES,), 0, PROMPTS).astype(jnp.int32),
        "text_lengths": touch_ends(jax.random.randint(key_list[13], (PROMPTS,), TXT // 4, TXT + 1), jax.random.fold_in(key_list[13], 1), TXT // 4, TXT).astype(jnp.int32),
        "step_ids": jax.random.randint(key_list[14], (SAMPLES,), 0, STEPS_ALL).astype(jnp.int32),
    }


NORM_EPSILON = 1e-06
NOISE_LEVEL = 0.7

def layer_norm(values):
    row_mean = lax.optimization_barrier(jnp.mean(values, axis=-1, keepdims=True))
    centred = values - row_mean
    row_var = lax.optimization_barrier(jnp.mean(centred * centred, axis=-1, keepdims=True))
    return centred * lax.rsqrt(row_var + NORM_EPSILON)

def head_norm(values, gain_vector):
    mean_square = lax.optimization_barrier(jnp.mean(values * values, axis=-1, keepdims=True))
    return (values * lax.rsqrt(mean_square + NORM_EPSILON) * gain_vector).astype(jnp.bfloat16)

def plan(step_values, total_steps):
    step_count = total_steps + 1.0
    flow_time = (total_steps - step_values.astype(jnp.float32)) / step_count
    step_delta = -1.0 / step_count
    noise_sigma = NOISE_LEVEL * jnp.sqrt(flow_time / (1.0 - flow_time))
    spread = noise_sigma * jnp.sqrt(1.0 / step_count)
    return (flow_time, step_delta, noise_sigma, spread)

def drift_mean(latent_state, velocity, flow_time, step_delta, noise_sigma):
    drift = velocity + noise_sigma * noise_sigma / (2.0 * flow_time) * (latent_state + (1.0 - flow_time) * velocity)
    return latent_state + drift * step_delta

def reference(image_states, text_states, image_qkv, text_qkv, image_out, final_weight, query_gain, key_gain, modulation, latent, old_velocity, rollout_noise, group_ids, text_lengths, step_ids):
    score_scale = 1.0 / math.sqrt(HEAD_DIM)

    def one_sample(index):
        modrows = modulation[step_ids[index]]
        image_f = image_states[index].astype(jnp.float32)
        text_rows = text_states[group_ids[index]].astype(jnp.float32)
        normed_img = (layer_norm(image_f) * (1.0 + modrows[1]) + modrows[0]).astype(jnp.bfloat16)
        normed_txt = (layer_norm(text_rows) * (1.0 + modrows[4]) + modrows[3]).astype(jnp.bfloat16)
        qkv_img = jnp.dot(normed_img, image_qkv.reshape(D, 3 * D), preferred_element_type=jnp.float32).reshape(IMG, 3, HEADS, HEAD_DIM)
        qkv_txt = jnp.dot(normed_txt, text_qkv.reshape(D, 3 * D), preferred_element_type=jnp.float32).reshape(TXT, 3, HEADS, HEAD_DIM)
        queries = head_norm(qkv_img[:, 0], query_gain)
        key_rows = head_norm(jnp.concatenate([qkv_txt[:, 1], qkv_img[:, 1]], axis=0), key_gain)
        value_rows = jnp.concatenate([qkv_txt[:, 2], qkv_img[:, 2]], axis=0).astype(jnp.bfloat16)
        text_valid = jnp.arange(TXT, dtype=jnp.int32) < text_lengths[group_ids[index]]
        key_valid = jnp.concatenate([text_valid.astype(jnp.float32), jnp.ones((IMG,), jnp.float32)])

        def one_head(head):
            query_head = queries[:, head]
            key_head = key_rows[:, head]
            value_head = value_rows[:, head]
            scores = jnp.dot(query_head, key_head.T, preferred_element_type=jnp.float32) * score_scale
            weights = jnp.exp(scores) * key_valid[None, :]
            denominator = lax.optimization_barrier(jnp.sum(weights, axis=-1))
            numerator = jnp.dot(weights.astype(jnp.bfloat16), value_head, preferred_element_type=jnp.float32)
            return (numerator / denominator[:, None]).astype(jnp.bfloat16)
        attended = lax.map(one_head, jnp.arange(HEADS, dtype=jnp.int32))
        attended = jnp.transpose(attended, (1, 0, 2)).reshape(IMG, D)
        projected = jnp.dot(attended, image_out, preferred_element_type=jnp.float32)
        resid = image_f + modrows[2] * projected
        final_normed = (layer_norm(resid) * (1.0 + modrows[6]) + modrows[5]).astype(jnp.bfloat16)
        return jnp.dot(final_normed, final_weight, preferred_element_type=jnp.float32)
    velocity = lax.map(one_sample, jnp.arange(SAMPLES, dtype=jnp.int32))
    flow_time, step_delta, noise_sigma, spread = plan(step_ids, STEPS_ALL)
    flow_e = flow_time[:, None, None]
    sigma_e = noise_sigma[:, None, None]
    step_mean = drift_mean(latent, velocity, flow_e, step_delta, sigma_e)
    mean_old = drift_mean(latent, old_velocity.astype(jnp.float32), flow_e, step_delta, sigma_e)
    shifted = rollout_noise + (mean_old - step_mean) / spread[:, None, None]
    log_ratio = lax.optimization_barrier(jnp.sum(rollout_noise * rollout_noise - shifted * shifted, axis=(1, 2))) * 0.5 / (IMG * CH)
    return (step_mean, log_ratio)
```

```python
import functools
import math

import jax
import jax.numpy as jnp
from jax import lax
from jax.experimental import pallas as pl
from jax.experimental.pallas import tpu as pltpu
from jax.sharding import PartitionSpec as P

NORM_EPSILON = 1e-06
NOISE_LEVEL = 0.7
F32 = jnp.float32
BF16 = jnp.bfloat16

TXT, IMG, TOK = 64, 512, 576
FEAT, PAIR, WIDTH = 384, 768, 3072
HEADS, HD = 3, 128
CH = 64
RING = 4
PARTS = ((0, 256), (256, 320))
VROWS = HD + 16
PAD = 640


def remote(src, dst, send, recv, where):
    return pltpu.make_async_remote_copy(
        src_ref=src,
        dst_ref=dst,
        send_sem=send,
        recv_sem=recv,
        device_id=where,
        device_id_type=pl.DeviceIdType.MESH,
    )


def piece(part, sub):
    start, rows = PARTS[part]
    return pl.ds(start + sub * (rows // 2), rows // 2)


def block(
    step_ref,
    group_ref,
    length_ref,
    x_ref,
    text_ref,
    wi_hbm,
    wt_hbm,
    wo_hbm,
    fw_ref,
    qg_ref,
    kg_ref,
    mod_ref,
    lat_ref,
    old_ref,
    noise_ref,
    mean_ref,
    ratio_ref,
    wi,
    wt,
    wo,
    xg,
    modv,
    st_col,
    st_all,
    stat,
    acc,
    qall,
    kv,
    oacc,
    osend,
    orecv,
    atts,
    attb,
    pso,
    pdir,
    pacc,
    pown,
    ropp,
    rdir,
    racc,
    rat1,
    rat2,
    w_sem,
    st_s,
    st_r,
    own_s,
    own_r,
    y_s,
    y_r,
    l_s,
    l_r,
    z_s,
    z_r,
    q_s,
    q_r,
    o_s,
    o_r,
    a_s,
    a_r,
    wo_s,
    wo_r,
    p_s,
    p_r,
    r1_s,
    r1_r,
    r2_s,
    r2_r,
):
    t = lax.axis_index("tensor")
    s = lax.axis_index("seq")
    y, c = lax.div(t, 2), lax.rem(t, 2)
    xlo, z = lax.div(s, RING), lax.rem(s, RING)
    yp, ym, yo = lax.rem(y + 1, RING), lax.rem(y + 3, RING), lax.rem(y + 2, RING)
    zp, zm, zo = lax.rem(z + 1, RING), lax.rem(z + 3, RING), lax.rem(z + 2, RING)
    mate = {"tensor": y * 2 + (1 - c)}
    y_dev = ({"tensor": yp * 2 + c}, {"tensor": ym * 2 + c})
    z_dev = ({"seq": xlo * RING + zp}, {"seq": xlo * RING + zm})
    x_dev = {"seq": (1 - xlo) * RING + z}
    cols = pl.ds(pl.multiple_of(c * FEAT, 128), FEAT)
    mate_cols = pl.ds(pl.multiple_of((1 - c) * FEAT, 128), FEAT)

    loads = []
    for j in range(3):
        loads.append(
            pltpu.make_async_copy(wi_hbm.at[j], wi.at[:, pl.ds(j * FEAT, FEAT)], w_sem.at[j])
        )
        loads.append(
            pltpu.make_async_copy(wt_hbm.at[j], wt.at[:, pl.ds(j * FEAT, FEAT)], w_sem.at[3 + j])
        )
    my_wo = wo.at[pl.ds(pl.multiple_of(c * FEAT, 128), FEAT)]
    wo_load = pltpu.make_async_copy(wo_hbm, my_wo, w_sem.at[6])
    for copy in loads:
        copy.start()
    wo_load.start()

    barrier = pltpu.get_barrier_semaphore()
    for j in range(1, 8):
        pl.semaphore_signal(
            barrier,
            inc=1,
            device_id={"tensor": lax.rem(t + j, 8)},
            device_id_type=pl.DeviceIdType.MESH,
        )
        pl.semaphore_signal(
            barrier,
            inc=1,
            device_id={"seq": lax.rem(s + j, 8)},
            device_id_type=pl.DeviceIdType.MESH,
        )

    group = group_ref[0]
    step = step_ref[0]
    xg[y, pl.ds(0, TXT), cols] = text_ref[group]
    xg[y, pl.ds(TXT, IMG), cols] = x_ref[0]

    mine = xg[y, :, cols].astype(F32)
    part_mean = jnp.mean(mine, axis=-1, keepdims=True)
    centred = mine - part_mean
    part_sq = jnp.sum(centred * centred, axis=-1, keepdims=True)
    lane = lax.broadcasted_iota(jnp.int32, (TOK, 128), 1)
    st_col[pl.ds(0, TOK), :] = jnp.where(lane == 0, part_mean, jnp.where(lane == 1, part_sq, 0.0))
    st_col[pl.ds(TOK, PAD - TOK), :] = jnp.zeros((PAD - TOK, 128), F32)
    st_all[t] = st_col[...].T[0:8, :]

    for i in range(RING):
        modv[i, pl.ds(0, 7), :] = mod_ref[step, :, pl.ds(i * PAIR, PAIR)]

    pl.semaphore_wait(barrier, 14)

    def peer_copy(buf, send, recv, axis, me, j):
        slot = buf.at[me]
        return remote(slot, slot, send.at[j], recv.at[j], {axis: lax.rem(me + j, 8)})

    def peer_arrival(buf, send, recv, axis, me, j):
        slot = buf.at[lax.rem(me + 8 - j, 8)]
        return remote(slot, slot, send.at[j], recv.at[j], {axis: lax.rem(me + j, 8)})

    stat_sends = [peer_copy(st_all, st_s, st_r, "tensor", t, j) for j in range(1, 8)]
    for copy in stat_sends:
        copy.start()

    def y_slot(d, k, sending):
        if k < 2:
            return (y if sending else (ym, yp)[d]), (k if d == 0 else 1 - k)
        return ((ym, yp)[d] if sending else yo), d

    def y_send(d, part, k):
        slot, sub = y_slot(d, k, True)
        ref = xg.at[slot, piece(part, sub), cols]
        return remote(ref, ref, y_s.at[d, part, k], y_r.at[d, part, k], y_dev[d])

    def y_arrival(d, part, k):
        slot, sub = y_slot(d, k, False)
        ref = xg.at[slot, piece(part, sub), cols]
        return remote(ref, ref, y_s.at[d, part, k], y_r.at[d, part, k], y_dev[d])

    def relay(d, part, k):
        slot, sub = y_slot(d, k, False)
        ref = xg.at[slot, piece(part, sub), cols]
        return remote(ref, ref, l_s.at[d, part, k], l_r.at[d, part, k], mate)

    def relay_arrival(d, part, k):
        slot, sub = y_slot(d, k, False)
        ref = xg.at[slot, piece(part, sub), mate_cols]
        return remote(ref, ref, l_s.at[d, part, k], l_r.at[d, part, k], mate)

    def own_copy(part, columns):
        ref = xg.at[y, pl.ds(*PARTS[part]), columns]
        return remote(ref, ref, own_s.at[part], own_r.at[part], mate)

    sends = list(stat_sends)

    def go(copy):
        copy.start()
        sends.append(copy)

    def y_own(part):
        for k in range(2):
            for d in range(2):
                go(y_send(d, part, k))

    y_own(0)
    go(own_copy(0, cols))
    go(own_copy(1, cols))

    for j in range(1, 8):
        peer_arrival(st_all, st_s, st_r, "tensor", t, j).wait_recv()
    means = st_all[:, 0, :]
    squares = st_all[:, 1, :]
    mean = jnp.mean(means, axis=0, keepdims=True)
    off = means - mean
    total_sq = jnp.sum(squares, axis=0, keepdims=True) + FEAT * jnp.sum(
        off * off, axis=0, keepdims=True
    )
    scale = lax.rsqrt(total_sq * (1.0 / WIDTH) + NORM_EPSILON)
    sub_row = lax.broadcasted_iota(jnp.int32, (128, PAD), 0)
    stat[...] = jnp.where(sub_row == 0, mean, jnp.where(sub_row == 1, scale, 0.0)).T

    for copy in loads:
        copy.wait()

    def project_rows(slot, start, rows, weight, shift_row, scale_row, first):
        at = pl.ds(start, rows)
        v = xg[slot, at, :].astype(F32)
        n = (v - stat[at, 0:1]) * stat[at, 1:2]
        n = n * (1.0 + modv[slot, pl.ds(scale_row, 1), :]) + modv[slot, pl.ds(shift_row, 1), :]
        w = weight[pl.ds(pl.multiple_of(slot * PAIR, 128), PAIR), :]
        p = jnp.dot(n.astype(BF16), w, preferred_element_type=F32)
        if first:
            acc[at, :] = p
        else:
            acc[at, :] += p

    def project(slot, part, first=False):
        start, rows = PARTS[part]
        if part == 0:
            project_rows(slot, TXT, rows - TXT, wi, 0, 1, first)
            project_rows(slot, 0, TXT, wt, 3, 4, first)
        else:
            project_rows(slot, start, rows, wi, 0, 1, first)

    score_scale = math.log2(math.e) / math.sqrt(HD)

    def head_norm(values, gain):
        square = jnp.mean(values * values, axis=-1, keepdims=True)
        return (values * lax.rsqrt(square + NORM_EPSILON) * gain).astype(BF16)

    def finish(part):
        start, rows = PARTS[part]
        at = pl.ds(start, rows)
        for h in range(HEADS):
            keys = acc[at, pl.ds(FEAT + h * HD, HD)]
            kv[z, at, pl.ds(h * HD, HD)] = head_norm(keys, kg_ref[...])
        kv[z, at, pl.ds(FEAT, FEAT)] = acc[at, pl.ds(2 * FEAT, FEAT)].astype(BF16)
        first = max(start, TXT)
        img = pl.ds(first, start + rows - first)
        for h in range(HEADS):
            query = acc[img, pl.ds(h * HD, HD)]
            qall[0, pl.ds(first - TXT, start + rows - first), pl.ds(h * HD, HD)] = head_norm(
                query, qg_ref[...] * score_scale
            )

    def z_slot(d, k, sending):
        if k < 2:
            return (z if sending else (zm, zp)[d]), (k if d == 0 else 1 - k)
        return ((zm, zp)[d] if sending else zo), d

    def z_send(d, part, k):
        slot, sub = z_slot(d, k, True)
        ref = kv.at[slot, piece(part, sub)]
        return remote(ref, ref, z_s.at[d, part, k], z_r.at[d, part, k], z_dev[d])

    def z_arrival(d, part, k):
        slot, sub = z_slot(d, k, False)
        ref = kv.at[slot, piece(part, sub)]
        return remote(ref, ref, z_s.at[d, part, k], z_r.at[d, part, k], z_dev[d])

    def q_copy(part):
        start, rows = PARTS[part]
        first = max(start, TXT)
        at = pl.ds(first - TXT, start + rows - first)
        return remote(qall.at[0, at], qall.at[1, at], q_s.at[part], q_r.at[part], x_dev)

    def z_own(part):
        for k in range(2):
            for d in range(2):
                go(z_send(d, part, k))

    for part in range(2):
        own_copy(part, mate_cols).wait_recv()
        project(y, part, first=True)
        for d in range(2):
            y_arrival(d, part, 0).wait_recv()
            go(y_send(d, part, 2))
            go(relay(d, part, 0))
        if part == 0:
            y_own(1)
        for d in range(2):
            y_arrival(d, part, 1).wait_recv()
            go(relay(d, part, 1))
        for k in range(2):
            for d in range(2):
                relay_arrival(d, part, k).wait_recv()
        project(ym, part)
        project(yp, part)
        for d in range(2):
            y_arrival(d, part, 2).wait_recv()
            go(relay(d, part, 2))
        for d in range(2):
            relay_arrival(d, part, 2).wait_recv()
        project(yo, part)
        finish(part)
        if part == 0:
            z_own(0)
        go(q_copy(part))

    wo_load.wait()
    wo_send = remote(my_wo, my_wo, wo_s.at[0], wo_r.at[0], mate)
    go(wo_send)

    length = length_ref[group]

    def attend(slot, part, sets, first=False):
        start, rows = PARTS[part]
        at = pl.ds(start, rows)

        def one_head(h, carry):
            at_k = pl.ds(pl.multiple_of(h * HD, 128), HD)
            at_v = pl.ds(pl.multiple_of(FEAT + h * HD, 128), HD)
            keys = kv[slot, at, at_k]
            vals = kv[slot, at, at_v].astype(F32).T
            ones = jnp.ones((VROWS - HD, rows), F32)
            if part == 0:
                pos = lax.broadcasted_iota(jnp.int32, (1, rows), 1)
                used = (pos >= TXT) | (pos + (xlo * RING + slot) * TXT < length)
                vals = jnp.where(used, vals, 0.0)
                ones = jnp.where(used, ones, 0.0)
            ext = jnp.concatenate([vals, ones], axis=0).astype(BF16)
            for q in sets:
                scores = lax.dot_general(
                    keys,
                    qall[q, :, at_k],
                    (((1,), (1,)), ((), ())),
                    preferred_element_type=F32,
                )
                e = jnp.exp2(scores).astype(BF16)
                o = jnp.dot(ext, e, preferred_element_type=F32)
                if first:
                    oacc[q, h] = o
                else:
                    oacc[q, h] += o
            return carry

        lax.fori_loop(0, HEADS, one_head, 0)

    for part in range(2):
        for d in range(2):
            z_arrival(d, part, 0).wait_recv()
            go(z_send(d, part, 2))
        if part == 0:
            z_own(1)
            q_wait = [q_copy(0), q_copy(1)]
            for copy in q_wait:
                copy.wait_recv()
            attend(z, 0, (1, 0), first=True)
            attend(z, 1, (1, 0))
        for d in range(2):
            z_arrival(d, part, 1).wait_recv()
        attend(zm, part, (1, 0))
        attend(zp, part, (1, 0))
        for d in range(2):
            z_arrival(d, part, 2).wait_recv()
        if part == 0:
            attend(zo, part, (1, 0))
    attend(zo, 1, (1,))

    order = (yo, yp, ym, y)

    def o_copy(j):
        return remote(osend.at[j], orecv.at[j], o_s.at[j], o_r.at[j], x_dev)

    def lanes(i):
        return pl.ds(pl.multiple_of(i * 128, 128), 128)

    for j in range(RING):
        at = lanes(order[j])
        for h in range(HEADS):
            osend[j, pl.ds(h * HD, HD), :] = oacc[1, h, pl.ds(0, HD), at].astype(BF16)
        whole = jnp.concatenate([oacc[1, h, pl.ds(HD, 1), at] for h in range(HEADS)], axis=0)
        high = whole.astype(BF16)
        rest = whole - high.astype(F32)
        middle = rest.astype(BF16)
        low = (rest - middle.astype(F32)).astype(BF16)
        osend[j, pl.ds(FEAT, 16), :] = jnp.concatenate(
            [high.astype(F32), middle.astype(F32), low.astype(F32), jnp.zeros((7, 128), F32)],
            axis=0,
        ).astype(BF16)
        go(o_copy(j))
    attend(zo, 1, (0,))

    def a_copy(j, columns):
        return remote(
            atts.at[j, pl.ds(pl.multiple_of((1 - c) * CH, CH), CH)],
            attb.at[j, :, columns],
            a_s.at[j],
            a_r.at[j],
            mate,
        )

    def combine(j):
        at = lanes(order[j])
        o_copy(j).wait_recv()
        tail = orecv[j, pl.ds(FEAT, 16), :].astype(F32)
        heads = []
        for h in range(HEADS):
            num = oacc[0, h, pl.ds(0, HD), at] + orecv[j, pl.ds(h * HD, HD), :].astype(F32)
            den = oacc[0, h, pl.ds(HD, 1), at] + (
                tail[h : h + 1] + tail[3 + h : 4 + h] + tail[6 + h : 7 + h]
            )
            heads.append((num / den).T)
        atts[j] = jnp.concatenate(heads, axis=1).astype(BF16)
        go(a_copy(j, cols))
        attb[j, :, cols] = atts[j, pl.ds(pl.multiple_of(c * CH, CH), CH), :]

    half = WIDTH // 2
    sides = (pl.ds(0, half), pl.ds(half, half))

    def p_copy(d, k):
        src = (pso.at[d], pdir.at[d], pacc.at[d])[k]
        dst = (ropp.at[d], rdir.at[d], racc.at[d])[k]
        return remote(src, dst, p_s.at[d, k], p_r.at[d, k], y_dev[d])

    def out_rows(j):
        a_copy(j, mate_cols).wait_recv()
        return jnp.dot(attb[j], wo[...], preferred_element_type=F32)

    def dispatch(j):
        p = out_rows(j)
        if j == 0:
            for d in range(2):
                pso[d] = p[:, d * half : (d + 1) * half].astype(BF16)
                go(p_copy(d, 0))
        elif j < 3:
            d = j - 1
            keep, direct = d, 1 - d
            pdir[d] = p[:, direct * half : (direct + 1) * half].astype(BF16)
            go(p_copy(d, 1))
            pown[:, sides[keep]] = p[:, keep * half : (keep + 1) * half]

    remote(my_wo, wo.at[pl.ds(pl.multiple_of((1 - c) * FEAT, 128), FEAT)], wo_s.at[0], wo_r.at[0], mate).wait_recv()
    for j in range(RING):
        combine(j)
        if j >= 1:
            dispatch(j - 1)
    last = out_rows(3)
    for d in range(2):
        p_copy(d, 0).wait_recv()
        pacc[d] = (pown[:, sides[d]] + ropp[d].astype(F32)).astype(BF16)
        go(p_copy(d, 2))
    pown[...] = last
    for d in range(2):
        p_copy(d, 1).wait_recv()
        pown[:, sides[1 - d]] += rdir[d].astype(F32)
    for d in range(2):
        p_copy(d, 2).wait_recv()
        pown[:, sides[d]] += racc[d].astype(F32)

    rows = pl.ds(pl.multiple_of(TXT + t * CH, CH), CH)
    resid = jnp.concatenate(
        [
            xg[i, rows, :].astype(F32)
            + modv[i, pl.ds(2, 1), :] * pown[:, pl.ds(i * PAIR, PAIR)]
            for i in range(RING)
        ],
        axis=1,
    )
    row_mean = jnp.mean(resid, axis=-1, keepdims=True)
    resid = resid - row_mean
    row_var = jnp.mean(resid * resid, axis=-1, keepdims=True)
    resid = resid * lax.rsqrt(row_var + NORM_EPSILON)
    velocity = jnp.zeros((CH, CH), F32)
    for i in range(RING):
        n = resid[:, i * PAIR : (i + 1) * PAIR] * (1.0 + modv[i, pl.ds(6, 1), :]) + modv[
            i, pl.ds(5, 1), :
        ]
        velocity += lax.dot_general(
            n.astype(BF16),
            fw_ref[:, pl.ds(i * PAIR, PAIR)],
            (((1,), (1,)), ((), ())),
            preferred_element_type=F32,
        )

    total_steps = mod_ref.shape[0]
    count = total_steps + 1.0
    step_delta = -1.0 / count
    flow = (total_steps - jnp.full((1, CH), step, jnp.int32).astype(F32)) / count
    sigma = NOISE_LEVEL * jnp.sqrt(flow / (1.0 - flow))
    spread = sigma * math.sqrt(1.0 / count)
    pull = sigma * sigma / (2.0 * flow)

    def drift(state, v):
        return state + (v + pull * (state + (1.0 - flow) * v)) * step_delta

    latent = lat_ref[0]
    noise = noise_ref[0]
    step_mean = drift(latent, velocity)
    mean_ref[0] = step_mean
    shifted = noise + (drift(latent, old_ref[0].astype(F32)) - step_mean) / spread
    gap = noise * noise - shifted * shifted
    gap = jnp.sum(jnp.sum(gap, axis=1, keepdims=True), axis=0, keepdims=True) * 0.5
    rat1[t] = jnp.broadcast_to(gap, (8, 128))
    for j in range(1, 8):
        go(peer_copy(rat1, r1_s, r1_r, "tensor", t, j))
    for j in range(1, 8):
        peer_arrival(rat1, r1_s, r1_r, "tensor", t, j).wait_recv()
    rat2[s] = jnp.sum(rat1[...], axis=0)
    for j in range(1, 8):
        go(peer_copy(rat2, r2_s, r2_r, "seq", s, j))
    for j in range(1, 8):
        peer_arrival(rat2, r2_s, r2_r, "seq", s, j).wait_recv()
    elements = 64 * CH * CH
    ratio = jnp.sum(rat2[...], axis=0) / elements
    ratio_ref[0] = ratio[0, 0]
    for copy in sends:
        copy.wait_send()


def shards(
    image_states,
    text_states,
    image_qkv,
    text_qkv,
    image_out,
    final_weight,
    query_gain,
    key_gain,
    modulation,
    latent,
    old_velocity,
    rollout_noise,
    group_ids,
    text_lengths,
    step_ids,
):
    smem = pl.BlockSpec(memory_space=pltpu.SMEM)
    vmem = pl.BlockSpec(memory_space=pltpu.VMEM)
    hbm = pl.BlockSpec(memory_space=pl.ANY)
    dma = pltpu.SemaphoreType.DMA
    half = WIDTH // 2
    return pl.pallas_call(
        block,
        out_shape=(
            jax.ShapeDtypeStruct(latent.shape, F32),
            jax.ShapeDtypeStruct((1,), F32),
        ),
        in_specs=[smem, smem, smem, vmem, vmem, hbm, hbm, hbm] + [vmem] * 7,
        out_specs=(vmem, smem),
        scratch_shapes=[
            pltpu.VMEM((WIDTH, 3 * FEAT), BF16),
            pltpu.VMEM((WIDTH, 3 * FEAT), BF16),
            pltpu.VMEM((PAIR, WIDTH), BF16),
            pltpu.VMEM((RING, TOK, PAIR), BF16),
            pltpu.VMEM((RING, 8, PAIR), F32),
            pltpu.VMEM((PAD, 128), F32),
            pltpu.VMEM((8, 8, PAD), F32),
            pltpu.VMEM((PAD, 128), F32),
            pltpu.VMEM((TOK, 3 * FEAT), F32),
            pltpu.VMEM((2, IMG, FEAT), BF16),
            pltpu.VMEM((RING, TOK, PAIR), BF16),
            pltpu.VMEM((2, HEADS, VROWS, IMG), F32),
            pltpu.VMEM((RING, FEAT + 16, 128), BF16),
            pltpu.VMEM((RING, FEAT + 16, 128), BF16),
            pltpu.VMEM((RING, 128, FEAT), BF16),
            pltpu.VMEM((RING, CH, PAIR), BF16),
            pltpu.VMEM((2, CH, half), BF16),
            pltpu.VMEM((2, CH, half), BF16),
            pltpu.VMEM((2, CH, half), BF16),
            pltpu.VMEM((CH, WIDTH), F32),
            pltpu.VMEM((2, CH, half), BF16),
            pltpu.VMEM((2, CH, half), BF16),
            pltpu.VMEM((2, CH, half), BF16),
            pltpu.VMEM((8, 8, 128), F32),
            pltpu.VMEM((8, 8, 128), F32),
            dma((7,)),
            dma((8,)),
            dma((8,)),
            dma((2,)),
            dma((2,)),
            dma((2, 2, 3)),
            dma((2, 2, 3)),
            dma((2, 2, 3)),
            dma((2, 2, 3)),
            dma((2, 2, 3)),
            dma((2, 2, 3)),
            dma((2,)),
            dma((2,)),
            dma((RING,)),
            dma((RING,)),
            dma((RING,)),
            dma((RING,)),
            dma((1,)),
            dma((1,)),
            dma((2, 3)),
            dma((2, 3)),
            dma((8,)),
            dma((8,)),
            dma((8,)),
            dma((8,)),
        ],
        compiler_params=pltpu.CompilerParams(
            collective_id=0, has_side_effects=True, vmem_limit_bytes=62 * 1024 * 1024
        ),
    )(
        step_ids,
        group_ids,
        text_lengths,
        image_states,
        text_states,
        jnp.transpose(image_qkv, (1, 0, 2)),
        jnp.transpose(text_qkv, (1, 0, 2)),
        image_out,
        final_weight.T,
        query_gain.reshape(1, HD),
        key_gain.reshape(1, HD),
        modulation,
        latent,
        old_velocity,
        rollout_noise,
    )


def solution(mesh):
    placed = (
        P("dp", "seq", "tensor"),
        P(None, "seq", "tensor"),
        P(None, None, "tensor"),
        P(None, None, "tensor"),
        P("tensor", None),
        P(),
        P(),
        P(),
        P(),
        P("dp", ("seq", "tensor"), None),
        P("dp", ("seq", "tensor"), None),
        P("dp", ("seq", "tensor"), None),
        P("dp"),
        P(),
        P("dp"),
    )
    return jax.shard_map(
        shards,
        mesh=mesh,
        in_specs=placed,
        out_specs=(P("dp", ("seq", "tensor"), None), P("dp")),
        check_vma=False,
    )
```

```python
import functools
import math

import jax
import jax.numpy as jnp
from jax import lax
from jax.experimental import pallas as pl
from jax.experimental.pallas import tpu as pltpu
from jax.sharding import PartitionSpec as P

NORM_EPSILON = 1e-06
NOISE_LEVEL = 0.7
F32 = jnp.float32
BF16 = jnp.bfloat16

TXT, IMG, TOK = 64, 512, 576
FEAT, PAIR, WIDTH = 384, 768, 3072
HEADS, HD = 3, 128
CH = 64
RING = 4
PARTS = ((0, 128), (128, 256), (384, 192))
VROWS = HD + 16
PAD = 640


def remote(src, dst, send, recv, where):
    return pltpu.make_async_remote_copy(
        src_ref=src,
        dst_ref=dst,
        send_sem=send,
        recv_sem=recv,
        device_id=where,
        device_id_type=pl.DeviceIdType.MESH,
    )


def piece(part, sub):
    start, rows = PARTS[part]
    return pl.ds(start + sub * (rows // 2), rows // 2)


def block(
    step_hbm,
    group_hbm,
    length_hbm,
    x_hbm,
    text_hbm,
    wi_hbm,
    wt_hbm,
    wo_hbm,
    fw_hbm,
    qg_hbm,
    kg_hbm,
    mod_hbm,
    lat_hbm,
    old_hbm,
    noise_hbm,
    mean_ref,
    ratio_ref,
    step_ref,
    group_ref,
    length_ref,
    text_ref,
    wi,
    wt,
    wo,
    fw_ref,
    qg_ref,
    kg_ref,
    mod_ref,
    lat_ref,
    old_ref,
    noise_ref,
    xg,
    modv,
    st_col,
    st_all,
    stat,
    acc,
    qall,
    kv,
    oacc,
    osend,
    orecv,
    atts,
    attb,
    pso,
    pdir,
    pacc,
    pown,
    ropp,
    rdir,
    racc,
    rat,
    w_sem,
    st_s,
    st_r,
    own_s,
    own_r,
    y_s,
    y_r,
    l_s,
    l_r,
    z_s,
    z_r,
    q_s,
    q_r,
    o_s,
    o_r,
    a_s,
    a_r,
    wo_s,
    wo_r,
    p_s,
    p_r,
    r_s,
    r_r,
):
    t = lax.axis_index("tensor")
    s = lax.axis_index("seq")
    y, c = lax.div(t, 2), lax.rem(t, 2)
    xlo, z = lax.div(s, RING), lax.rem(s, RING)
    yp, ym, yo = lax.rem(y + 1, RING), lax.rem(y + 3, RING), lax.rem(y + 2, RING)
    zp, zm, zo = lax.rem(z + 1, RING), lax.rem(z + 3, RING), lax.rem(z + 2, RING)
    mate = {"tensor": y * 2 + (1 - c)}
    y_dev = ({"tensor": yp * 2 + c}, {"tensor": ym * 2 + c})
    z_dev = ({"seq": xlo * RING + zp}, {"seq": xlo * RING + zm})
    x_dev = {"seq": (1 - xlo) * RING + z}
    cols = pl.ds(pl.multiple_of(c * FEAT, 128), FEAT)
    mate_cols = pl.ds(pl.multiple_of((1 - c) * FEAT, 128), FEAT)

    barrier = pltpu.get_barrier_semaphore()
    for j in range(1, 8):
        pl.semaphore_signal(
            barrier,
            inc=1,
            device_id={"tensor": lax.rem(t + j, 8)},
            device_id_type=pl.DeviceIdType.MESH,
        )
        pl.semaphore_signal(
            barrier,
            inc=1,
            device_id={"seq": lax.rem(s + j, 8)},
            device_id_type=pl.DeviceIdType.MESH,
        )

    def local(src, dst, k):
        copy = pltpu.make_async_copy(src, dst, w_sem.at[k])
        copy.start()
        return copy

    x_load = local(x_hbm.at[0], xg.at[y, pl.ds(TXT, IMG), cols], 7)
    text_load = local(text_hbm, text_ref, 8)
    group_load = local(group_hbm, group_ref, 9)
    small = [
        local(step_hbm, step_ref, 10),
        local(length_hbm, length_ref, 11),
        local(mod_hbm, mod_ref, 12),
        local(qg_hbm, qg_ref, 13),
        local(kg_hbm, kg_ref, 14),
    ]
    loads = []
    for j in range(3):
        loads.append(local(wt_hbm.at[j], wt.at[:, pl.ds(j * FEAT, FEAT)], 3 + j))
        loads.append(local(wi_hbm.at[j], wi.at[:, pl.ds(j * FEAT, FEAT)], j))
    my_wo = wo.at[pl.ds(pl.multiple_of(c * FEAT, 128), FEAT)]
    late = [
        local(wo_hbm, my_wo, 6),
        local(fw_hbm, fw_ref, 15),
        local(lat_hbm.at[0], lat_ref, 16),
        local(old_hbm.at[0], old_ref, 17),
        local(noise_hbm.at[0], noise_ref, 18),
    ]

    text_load.wait()
    group_load.wait()
    group = group_ref[0]
    xg[y, pl.ds(0, TXT), cols] = text_ref[group]
    x_load.wait()
    pl.semaphore_wait(barrier, 14)

    def peer_copy(buf, send, recv, axis, me, j):
        slot = buf.at[me]
        return remote(slot, slot, send.at[j], recv.at[j], {axis: lax.rem(me + j, 8)})

    def peer_arrival(buf, send, recv, axis, me, j):
        slot = buf.at[lax.rem(me + 8 - j, 8)]
        return remote(slot, slot, send.at[j], recv.at[j], {axis: lax.rem(me + j, 8)})

    def y_slot(d, k, sending):
        if k < 2:
            return (y if sending else (ym, yp)[d]), (k if d == 0 else 1 - k)
        return ((ym, yp)[d] if sending else yo), d

    def y_send(d, part, k):
        slot, sub = y_slot(d, k, True)
        ref = xg.at[slot, piece(part, sub), cols]
        return remote(ref, ref, y_s.at[d, part, k], y_r.at[d, part, k], y_dev[d])

    def y_arrival(d, part, k):
        slot, sub = y_slot(d, k, False)
        ref = xg.at[slot, piece(part, sub), cols]
        return remote(ref, ref, y_s.at[d, part, k], y_r.at[d, part, k], y_dev[d])

    def relay(d, part, k):
        slot, sub = y_slot(d, k, False)
        ref = xg.at[slot, piece(part, sub), cols]
        return remote(ref, ref, l_s.at[d, part, k], l_r.at[d, part, k], mate)

    def relay_arrival(d, part, k):
        slot, sub = y_slot(d, k, False)
        ref = xg.at[slot, piece(part, sub), mate_cols]
        return remote(ref, ref, l_s.at[d, part, k], l_r.at[d, part, k], mate)

    def own_copy(columns):
        ref = xg.at[y, :, columns]
        return remote(ref, ref, own_s.at[0], own_r.at[0], mate)

    sends = []

    def go(copy):
        copy.start()
        sends.append(copy)

    def y_own(part):
        for k in range(2):
            for d in range(2):
                go(y_send(d, part, k))

    y_own(0)

    mine = xg[y, :, cols].astype(F32)
    part_mean = jnp.mean(mine, axis=-1, keepdims=True)
    centred = mine - part_mean
    part_sq = jnp.sum(centred * centred, axis=-1, keepdims=True)
    lane = lax.broadcasted_iota(jnp.int32, (TOK, 128), 1)
    st_col[pl.ds(0, TOK), :] = jnp.where(lane == 0, part_mean, jnp.where(lane == 1, part_sq, 0.0))
    st_col[pl.ds(TOK, PAD - TOK), :] = jnp.zeros((PAD - TOK, 128), F32)
    st_all[t] = st_col[...].T[0:2, :]
    for j in range(1, 8):
        go(peer_copy(st_all, st_s, st_r, "tensor", t, j))
    go(own_copy(cols))

    def y_first(part):
        for d in range(2):
            y_arrival(d, part, 0).wait_recv()
            go(y_send(d, part, 2))
            go(relay(d, part, 0))

    def y_relay(part, k):
        for d in range(2):
            y_arrival(d, part, k).wait_recv()
            go(relay(d, part, k))

    def y_ready(part, k):
        for d in range(2):
            relay_arrival(d, part, k).wait_recv()

    for copy in small:
        copy.wait()
    step = step_ref[0]
    for i in range(RING):
        modv[i, pl.ds(0, 7), :] = mod_ref[step, :, pl.ds(i * PAIR, PAIR)]

    y_first(0)
    y_own(1)
    y_relay(0, 1)

    for j in range(1, 8):
        peer_arrival(st_all, st_s, st_r, "tensor", t, j).wait_recv()
    means = st_all[:, 0, :]
    squares = st_all[:, 1, :]
    mean = jnp.mean(means, axis=0, keepdims=True)
    off = means - mean
    total_sq = jnp.sum(squares, axis=0, keepdims=True) + FEAT * jnp.sum(
        off * off, axis=0, keepdims=True
    )
    scale = lax.rsqrt(total_sq * (1.0 / WIDTH) + NORM_EPSILON)
    sub_row = lax.broadcasted_iota(jnp.int32, (128, PAD), 0)
    stat[...] = jnp.where(sub_row == 0, mean, jnp.where(sub_row == 1, scale, 0.0)).T

    for copy in loads:
        copy.wait()

    def project_rows(slot, start, rows, weight, shift_row, scale_row, first):
        at = pl.ds(start, rows)
        v = xg[slot, at, :].astype(F32)
        n = (v - stat[at, 0:1]) * stat[at, 1:2]
        n = n * (1.0 + modv[slot, pl.ds(scale_row, 1), :]) + modv[slot, pl.ds(shift_row, 1), :]
        w = weight[pl.ds(pl.multiple_of(slot * PAIR, 128), PAIR), :]
        p = jnp.dot(n.astype(BF16), w, preferred_element_type=F32)
        if first:
            acc[at, :] = p
        else:
            acc[at, :] += p

    def project(slot, part, first=False):
        start, rows = PARTS[part]
        if part == 0:
            project_rows(slot, TXT, rows - TXT, wi, 0, 1, first)
            project_rows(slot, 0, TXT, wt, 3, 4, first)
        else:
            project_rows(slot, start, rows, wi, 0, 1, first)

    score_scale = math.log2(math.e) / math.sqrt(HD)

    def head_norm(values, gain):
        square = jnp.mean(values * values, axis=-1, keepdims=True)
        return (values * lax.rsqrt(square + NORM_EPSILON) * gain).astype(BF16)

    def finish(part):
        start, rows = PARTS[part]
        at = pl.ds(start, rows)
        for h in range(HEADS):
            keys = acc[at, pl.ds(FEAT + h * HD, HD)]
            kv[z, at, pl.ds(h * HD, HD)] = head_norm(keys, kg_ref[...])
        kv[z, at, pl.ds(FEAT, FEAT)] = acc[at, pl.ds(2 * FEAT, FEAT)].astype(BF16)
        first = max(start, TXT)
        img = pl.ds(first, start + rows - first)
        for h in range(HEADS):
            query = acc[img, pl.ds(h * HD, HD)]
            qall[0, pl.ds(first - TXT, start + rows - first), pl.ds(h * HD, HD)] = head_norm(
                query, qg_ref[...] * score_scale
            )

    def z_slot(d, k, sending):
        if k < 2:
            return (z if sending else (zm, zp)[d]), (k if d == 0 else 1 - k)
        return ((zm, zp)[d] if sending else zo), d

    def z_send(d, part, k):
        slot, sub = z_slot(d, k, True)
        ref = kv.at[slot, piece(part, sub)]
        return remote(ref, ref, z_s.at[d, part, k], z_r.at[d, part, k], z_dev[d])

    def z_arrival(d, part, k):
        slot, sub = z_slot(d, k, False)
        ref = kv.at[slot, piece(part, sub)]
        return remote(ref, ref, z_s.at[d, part, k], z_r.at[d, part, k], z_dev[d])

    def q_copy(part):
        start, rows = PARTS[part]
        first = max(start, TXT)
        at = pl.ds(first - TXT, start + rows - first)
        return remote(qall.at[0, at], qall.at[1, at], q_s.at[part], q_r.at[part], x_dev)

    def z_own(part):
        for k in range(2):
            for d in range(2):
                go(z_send(d, part, k))

    def z_first(part):
        for d in range(2):
            z_arrival(d, part, 0).wait_recv()
            go(z_send(d, part, 2))

    def z_wait(part, k):
        for d in range(2):
            z_arrival(d, part, k).wait_recv()

    own_copy(mate_cols).wait_recv()
    project(y, 0, first=True)
    y_ready(0, 0)
    y_ready(0, 1)
    project(ym, 0)
    project(yp, 0)
    y_relay(0, 2)
    y_ready(0, 2)
    project(yo, 0)
    finish(0)
    z_own(0)
    go(q_copy(0))

    y_first(1)
    y_own(2)
    project(y, 1, first=True)
    y_relay(1, 1)
    y_ready(1, 0)
    y_ready(1, 1)
    project(ym, 1)
    project(yp, 1)
    z_first(0)
    y_relay(1, 2)
    project(y, 2, first=True)
    y_ready(1, 2)
    project(yo, 1)
    finish(1)
    z_own(1)
    go(q_copy(1))

    y_first(2)
    y_relay(2, 1)
    y_ready(2, 0)
    y_ready(2, 1)
    project(ym, 2)
    project(yp, 2)
    y_relay(2, 2)
    y_ready(2, 2)
    project(yo, 2)
    finish(2)
    go(q_copy(2))

    for copy in late:
        copy.wait()
    wo_send = remote(my_wo, my_wo, wo_s.at[0], wo_r.at[0], mate)
    go(wo_send)

    length = length_ref[group]

    def values(slot, start, rows, h):
        vals = kv[slot, pl.ds(start, rows), pl.ds(FEAT + h * HD, HD)].astype(F32).T
        ones = jnp.ones((VROWS - HD, rows), F32)
        if start == 0:
            pos = lax.broadcasted_iota(jnp.int32, (1, rows), 1)
            used = (pos >= TXT) | (pos + (xlo * RING + slot) * TXT < length)
            vals = jnp.where(used, vals, 0.0)
            ones = jnp.where(used, ones, 0.0)
        return jnp.concatenate([vals, ones], axis=0).astype(BF16)

    def weighted(slot, start, rows, h, ext, q, at_q):
        scores = lax.dot_general(
            kv[slot, pl.ds(start, rows), pl.ds(h * HD, HD)],
            qall[q, at_q, pl.ds(h * HD, HD)],
            (((1,), (1,)), ((), ())),
            preferred_element_type=F32,
        )
        return jnp.dot(ext, jnp.exp2(scores).astype(BF16), preferred_element_type=F32)

    def attend(slot, start, rows, sets, first=False):
        for h in range(HEADS):
            ext = values(slot, start, rows, h)
            for q in sets:
                o = weighted(slot, start, rows, h, ext, q, pl.ds(0, IMG))
                if first:
                    oacc[q, h] = o
                else:
                    oacc[q, h] += o

    attend(z, 0, TOK, (0,), first=True)
    z_first(1)
    z_own(2)
    z_wait(0, 1)
    z_wait(0, 2)
    for part in range(3):
        q_copy(part).wait_recv()
    attend(z, 0, TOK, (1,), first=True)
    for slot in (zm, zp, zo):
        attend(slot, *PARTS[0], (1, 0))
    z_wait(1, 1)
    attend(zm, *PARTS[1], (1, 0))
    attend(zp, *PARTS[1], (1, 0))
    z_first(2)
    z_wait(1, 2)
    attend(zo, *PARTS[1], (1, 0))
    z_wait(2, 1)
    attend(zm, *PARTS[2], (1, 0))
    attend(zp, *PARTS[2], (1, 0))
    z_wait(2, 2)

    order = (yo, yp, ym, y)

    def o_copy(j):
        return remote(osend.at[j], orecv.at[j], o_s.at[j], o_r.at[j], x_dev)

    def lanes(i):
        return pl.ds(pl.multiple_of(i * 128, 128), 128)

    last = [values(zo, *PARTS[2], h) for h in range(HEADS)]
    for j in range(RING):
        at = lanes(order[j])
        dens = []
        for h in range(HEADS):
            o = oacc[1, h, :, at] + weighted(zo, *PARTS[2], h, last[h], 1, at)
            osend[j, pl.ds(h * HD, HD), :] = o[:HD].astype(BF16)
            dens.append(o[HD : HD + 1])
        whole = jnp.concatenate(dens, axis=0)
        high = whole.astype(BF16)
        rest = whole - high.astype(F32)
        middle = rest.astype(BF16)
        low = (rest - middle.astype(F32)).astype(BF16)
        osend[j, pl.ds(FEAT, 16), :] = jnp.concatenate(
            [high.astype(F32), middle.astype(F32), low.astype(F32), jnp.zeros((7, 128), F32)],
            axis=0,
        ).astype(BF16)
        go(o_copy(j))
    attend(zo, *PARTS[2], (0,))

    def a_copy(j, columns):
        return remote(
            atts.at[j, pl.ds(pl.multiple_of((1 - c) * CH, CH), CH)],
            attb.at[j, :, columns],
            a_s.at[j],
            a_r.at[j],
            mate,
        )

    def combine(j):
        at = lanes(order[j])
        o_copy(j).wait_recv()
        tail = orecv[j, pl.ds(FEAT, 16), :].astype(F32)
        heads = []
        for h in range(HEADS):
            num = oacc[0, h, pl.ds(0, HD), at] + orecv[j, pl.ds(h * HD, HD), :].astype(F32)
            den = oacc[0, h, pl.ds(HD, 1), at] + (
                tail[h : h + 1] + tail[3 + h : 4 + h] + tail[6 + h : 7 + h]
            )
            heads.append((num / den).T)
        atts[j] = jnp.concatenate(heads, axis=1).astype(BF16)
        go(a_copy(j, cols))
        attb[j, :, cols] = atts[j, pl.ds(pl.multiple_of(c * CH, CH), CH), :]

    half = WIDTH // 2
    sides = (pl.ds(0, half), pl.ds(half, half))

    def p_copy(d, k):
        src = (pso.at[d], pdir.at[d], pacc.at[d])[k]
        dst = (ropp.at[d], rdir.at[d], racc.at[d])[k]
        return remote(src, dst, p_s.at[d, k], p_r.at[d, k], y_dev[d])

    def out_side(j, d):
        return jnp.dot(attb[j], wo[:, sides[d]], preferred_element_type=F32)

    def dispatch(j):
        a_copy(j, mate_cols).wait_recv()
        if j == 0:
            for d in range(2):
                pso[d] = out_side(0, d).astype(BF16)
                go(p_copy(d, 0))
        else:
            keep, direct = j - 1, 2 - j
            pdir[keep] = out_side(j, direct).astype(BF16)
            go(p_copy(keep, 1))
            pown[:, sides[keep]] = out_side(j, keep)

    remote(my_wo, wo.at[pl.ds(pl.multiple_of((1 - c) * FEAT, 128), FEAT)], wo_s.at[0], wo_r.at[0], mate).wait_recv()
    for j in range(RING):
        combine(j)
        if j >= 1:
            dispatch(j - 1)
    a_copy(3, mate_cols).wait_recv()
    mine = [out_side(3, d) for d in range(2)]
    for d in range(2):
        p_copy(d, 0).wait_recv()
        pacc[d] = (pown[:, sides[d]] + ropp[d].astype(F32)).astype(BF16)
        go(p_copy(d, 2))
    for d in range(2):
        p_copy(1 - d, 1).wait_recv()
        pown[:, sides[d]] = mine[d] + rdir[1 - d].astype(F32)
    for d in range(2):
        p_copy(d, 2).wait_recv()
        pown[:, sides[d]] += racc[d].astype(F32)

    rows = pl.ds(pl.multiple_of(TXT + t * CH, CH), CH)
    resid = jnp.concatenate(
        [
            xg[i, rows, :].astype(F32)
            + modv[i, pl.ds(2, 1), :] * pown[:, pl.ds(i * PAIR, PAIR)]
            for i in range(RING)
        ],
        axis=1,
    )
    row_mean = jnp.mean(resid, axis=-1, keepdims=True)
    resid = resid - row_mean
    row_var = jnp.mean(resid * resid, axis=-1, keepdims=True)
    resid = resid * lax.rsqrt(row_var + NORM_EPSILON)
    velocity = jnp.zeros((CH, CH), F32)
    for i in range(RING):
        n = resid[:, i * PAIR : (i + 1) * PAIR] * (1.0 + modv[i, pl.ds(6, 1), :]) + modv[
            i, pl.ds(5, 1), :
        ]
        velocity += lax.dot_general(
            n.astype(BF16),
            fw_ref[:, pl.ds(i * PAIR, PAIR)],
            (((1,), (1,)), ((), ())),
            preferred_element_type=F32,
        )

    total_steps = mod_ref.shape[0]
    count = total_steps + 1.0
    step_delta = -1.0 / count
    flow = (total_steps - jnp.full((1, CH), step, jnp.int32).astype(F32)) / count
    sigma = NOISE_LEVEL * jnp.sqrt(flow / (1.0 - flow))
    spread = sigma * math.sqrt(1.0 / count)
    pull = sigma * sigma / (2.0 * flow)

    def drift(state, v):
        return state + (v + pull * (state + (1.0 - flow) * v)) * step_delta

    latent = lat_ref[...]
    noise = noise_ref[...]
    step_mean = drift(latent, velocity)
    mean_ref[0] = step_mean
    shifted = noise + (drift(latent, old_ref[...].astype(F32)) - step_mean) / spread
    gap = noise * noise - shifted * shifted
    gap = jnp.sum(jnp.sum(gap, axis=1, keepdims=True), axis=0, keepdims=True) * 0.5
    me = s * 8 + t
    rat[me] = jnp.broadcast_to(gap, (1, 128))

    def tell(j, carry):
        other = lax.rem(me + j, 64)
        where = {"seq": lax.div(other, 8), "tensor": lax.rem(other, 8)}
        remote(rat.at[me], rat.at[me], r_s.at[0], r_r.at[0], where).start()
        return carry

    lax.fori_loop(1, 64, tell, 0)
    told = rat.at[pl.ds(0, 63)]
    everyone = remote(told, told, r_s.at[0], r_r.at[0], mate)
    everyone.wait_recv()
    elements = 64 * CH * CH
    ratio = jnp.sum(rat[...], axis=0) / elements
    ratio_ref[0] = ratio[0, 0]
    everyone.wait_send()
    for copy in sends:
        copy.wait_send()


def shards(
    image_states,
    text_states,
    image_qkv,
    text_qkv,
    image_out,
    final_weight,
    query_gain,
    key_gain,
    modulation,
    latent,
    old_velocity,
    rollout_noise,
    group_ids,
    text_lengths,
    step_ids,
):
    smem = pl.BlockSpec(memory_space=pltpu.SMEM)
    vmem = pl.BlockSpec(memory_space=pltpu.VMEM)
    hbm = pl.BlockSpec(memory_space=pl.ANY)
    dma = pltpu.SemaphoreType.DMA
    half = WIDTH // 2
    return pl.pallas_call(
        block,
        out_shape=(
            jax.ShapeDtypeStruct(latent.shape, F32),
            jax.ShapeDtypeStruct((1,), F32),
        ),
        in_specs=[hbm] * 15,
        out_specs=(vmem, smem),
        scratch_shapes=[
            pltpu.SMEM((1,), jnp.int32),
            pltpu.SMEM((1,), jnp.int32),
            pltpu.SMEM((4,), jnp.int32),
            pltpu.VMEM(text_states.shape, BF16),
            pltpu.VMEM((WIDTH, 3 * FEAT), BF16),
            pltpu.VMEM((WIDTH, 3 * FEAT), BF16),
            pltpu.VMEM((PAIR, WIDTH), BF16),
            pltpu.VMEM((CH, WIDTH), BF16),
            pltpu.VMEM((1, HD), F32),
            pltpu.VMEM((1, HD), F32),
            pltpu.VMEM(modulation.shape, F32),
            pltpu.VMEM((CH, CH), F32),
            pltpu.VMEM((CH, CH), BF16),
            pltpu.VMEM((CH, CH), F32),
            pltpu.VMEM((RING, TOK, PAIR), BF16),
            pltpu.VMEM((RING, 8, PAIR), F32),
            pltpu.VMEM((PAD, 128), F32),
            pltpu.VMEM((8, 2, PAD), F32),
            pltpu.VMEM((PAD, 128), F32),
            pltpu.VMEM((TOK, 3 * FEAT), F32),
            pltpu.VMEM((2, IMG, FEAT), BF16),
            pltpu.VMEM((RING, TOK, PAIR), BF16),
            pltpu.VMEM((2, HEADS, VROWS, IMG), F32),
            pltpu.VMEM((RING, FEAT + 16, 128), BF16),
            pltpu.VMEM((RING, FEAT + 16, 128), BF16),
            pltpu.VMEM((RING, 128, FEAT), BF16),
            pltpu.VMEM((RING, CH, PAIR), BF16),
            pltpu.VMEM((2, CH, half), BF16),
            pltpu.VMEM((2, CH, half), BF16),
            pltpu.VMEM((2, CH, half), BF16),
            pltpu.VMEM((CH, WIDTH), F32),
            pltpu.VMEM((2, CH, half), BF16),
            pltpu.VMEM((2, CH, half), BF16),
            pltpu.VMEM((2, CH, half), BF16),
            pltpu.VMEM((64, 1, 128), F32),
            dma((19,)),
            dma((8,)),
            dma((8,)),
            dma((1,)),
            dma((1,)),
            dma((2, 3, 3)),
            dma((2, 3, 3)),
            dma((2, 3, 3)),
            dma((2, 3, 3)),
            dma((2, 3, 3)),
            dma((2, 3, 3)),
            dma((3,)),
            dma((3,)),
            dma((RING,)),
            dma((RING,)),
            dma((RING,)),
            dma((RING,)),
            dma((1,)),
            dma((1,)),
            dma((2, 3)),
            dma((2, 3)),
            dma((1,)),
            dma((1,)),
        ],
        compiler_params=pltpu.CompilerParams(
            collective_id=0, has_side_effects=True, vmem_limit_bytes=62 * 1024 * 1024
        ),
    )(
        step_ids,
        group_ids,
        text_lengths,
        image_states,
        text_states,
        jnp.transpose(image_qkv, (1, 0, 2)),
        jnp.transpose(text_qkv, (1, 0, 2)),
        image_out,
        final_weight.T,
        query_gain.reshape(1, HD),
        key_gain.reshape(1, HD),
        modulation,
        latent,
        old_velocity,
        rollout_noise,
    )


def solution(mesh):
    placed = (
        P("dp", "seq", "tensor"),
        P(None, "seq", "tensor"),
        P(None, None, "tensor"),
        P(None, None, "tensor"),
        P("tensor", None),
        P(),
        P(),
        P(),
        P(),
        P("dp", ("seq", "tensor"), None),
        P("dp", ("seq", "tensor"), None),
        P("dp", ("seq", "tensor"), None),
        P("dp"),
        P(),
        P("dp"),
    )
    return jax.shard_map(
        shards,
        mesh=mesh,
        in_specs=placed,
        out_specs=(P("dp", ("seq", "tensor"), None), P("dp")),
        check_vma=False,
    )
```

```python
import functools
import math

import jax
import jax.numpy as jnp
from jax import lax
from jax.experimental import pallas as pl
from jax.experimental.pallas import tpu as pltpu
from jax.sharding import PartitionSpec as P

NORM_EPSILON = 1e-06
NOISE_LEVEL = 0.7
F32 = jnp.float32
BF16 = jnp.bfloat16

TXT, IMG, TOK = 64, 512, 576
FEAT, PAIR, WIDTH = 384, 768, 3072
HEADS, HD = 3, 128
CH = 64
RING = 4
HEAD_ROWS = 128
PARTS = ((0, 128), (128, 256), (384, 192))
GROUPS = ((0, 0, 3),) + tuple((part, h, 1) for h in range(3) for part in (1, 2))
VROWS = HD + 16
PAD = 640


def remote(src, dst, send, recv, where):
    return pltpu.make_async_remote_copy(
        src_ref=src,
        dst_ref=dst,
        send_sem=send,
        recv_sem=recv,
        device_id=where,
        device_id_type=pl.DeviceIdType.MESH,
    )


def piece(part, sub):
    start, rows = PARTS[part]
    return pl.ds(start + sub * (rows // 2), rows // 2)


def block(
    step_hbm,
    group_hbm,
    length_hbm,
    x_hbm,
    text_hbm,
    wi_hbm,
    wt_hbm,
    wo_hbm,
    fw_hbm,
    qg_hbm,
    kg_hbm,
    mod_hbm,
    lat_hbm,
    old_hbm,
    noise_hbm,
    mean_ref,
    ratio_ref,
    step_ref,
    group_ref,
    length_ref,
    text_ref,
    wi,
    wt,
    wo,
    fw_ref,
    qg_ref,
    kg_ref,
    mod_ref,
    lat_ref,
    old_ref,
    noise_ref,
    xg,
    modv,
    st_col,
    st_all,
    stat,
    acc,
    qall,
    kv,
    oacc,
    osend,
    orecv,
    atts,
    attb,
    pso,
    pdir,
    pacc,
    pown,
    ropp,
    rdir,
    racc,
    rat,
    w_sem,
    st_s,
    st_r,
    own_s,
    own_r,
    y_s,
    y_r,
    l_s,
    l_r,
    z_s,
    z_r,
    q_s,
    q_r,
    o_s,
    o_r,
    a_s,
    a_r,
    wo_s,
    wo_r,
    p_s,
    p_r,
    r_s,
    r_r,
):
    t = lax.axis_index("tensor")
    s = lax.axis_index("seq")
    y, c = lax.div(t, 2), lax.rem(t, 2)
    xlo, z = lax.div(s, RING), lax.rem(s, RING)
    yp, ym, yo = lax.rem(y + 1, RING), lax.rem(y + 3, RING), lax.rem(y + 2, RING)
    zp, zm, zo = lax.rem(z + 1, RING), lax.rem(z + 3, RING), lax.rem(z + 2, RING)
    mate = {"tensor": y * 2 + (1 - c)}
    y_dev = ({"tensor": yp * 2 + c}, {"tensor": ym * 2 + c})
    z_dev = ({"seq": xlo * RING + zp}, {"seq": xlo * RING + zm})
    x_dev = {"seq": (1 - xlo) * RING + z}
    cols = pl.ds(pl.multiple_of(c * FEAT, 128), FEAT)
    mate_cols = pl.ds(pl.multiple_of((1 - c) * FEAT, 128), FEAT)

    barrier = pltpu.get_barrier_semaphore()
    for j in range(1, 8):
        pl.semaphore_signal(
            barrier,
            inc=1,
            device_id={"tensor": lax.rem(t + j, 8)},
            device_id_type=pl.DeviceIdType.MESH,
        )
        pl.semaphore_signal(
            barrier,
            inc=1,
            device_id={"seq": lax.rem(s + j, 8)},
            device_id_type=pl.DeviceIdType.MESH,
        )

    def local(src, dst, k):
        copy = pltpu.make_async_copy(src, dst, w_sem.at[k])
        copy.start()
        return copy

    head_rows = pl.ds(0, HEAD_ROWS)
    rest_rows = pl.ds(HEAD_ROWS, IMG - HEAD_ROWS)
    moved_rows = pl.ds(HEAD_ROWS + TXT, IMG - HEAD_ROWS)
    x_load = local(x_hbm.at[0, head_rows], xg.at[y, head_rows, cols], 7)
    x_rest = local(x_hbm.at[0, rest_rows], xg.at[y, moved_rows, cols], 19)
    text_load = local(text_hbm, text_ref, 8)
    group_load = local(group_hbm, group_ref, 9)
    small = [
        local(step_hbm, step_ref, 10),
        local(length_hbm, length_ref, 11),
        local(mod_hbm, mod_ref, 12),
        local(qg_hbm, qg_ref, 13),
        local(kg_hbm, kg_ref, 14),
    ]
    loads = []
    for j in range(3):
        loads.append(local(wt_hbm.at[j], wt.at[:, pl.ds(j * FEAT, FEAT)], 3 + j))
        loads.append(local(wi_hbm.at[j], wi.at[:, pl.ds(j * FEAT, FEAT)], j))
    my_wo = wo.at[pl.ds(pl.multiple_of(c * FEAT, 128), FEAT)]
    late = [
        local(wo_hbm, my_wo, 6),
        local(fw_hbm, fw_ref, 15),
        local(lat_hbm.at[0], lat_ref, 16),
        local(old_hbm.at[0], old_ref, 17),
        local(noise_hbm.at[0], noise_ref, 18),
    ]

    text_load.wait()
    group_load.wait()
    group = group_ref[0]
    xg[y, pl.ds(HEAD_ROWS, TXT), cols] = text_ref[group]
    x_load.wait()
    x_rest.wait()

    mine = xg[y, :, cols].astype(F32)
    part_mean = jnp.mean(mine, axis=-1, keepdims=True)
    centred = mine - part_mean
    part_sq = jnp.sum(centred * centred, axis=-1, keepdims=True)
    lane = lax.broadcasted_iota(jnp.int32, (TOK, 128), 1)
    st_col[pl.ds(0, TOK), :] = jnp.where(lane == 0, part_mean, jnp.where(lane == 1, part_sq, 0.0))
    st_col[pl.ds(TOK, PAD - TOK), :] = jnp.zeros((PAD - TOK, 128), F32)
    st_all[t] = st_col[...].T[0:2, :]

    pl.semaphore_wait(barrier, 14)

    def peer_copy(buf, send, recv, axis, me, j):
        slot = buf.at[me]
        return remote(slot, slot, send.at[j], recv.at[j], {axis: lax.rem(me + j, 8)})

    def peer_arrival(buf, send, recv, axis, me, j):
        slot = buf.at[lax.rem(me + 8 - j, 8)]
        return remote(slot, slot, send.at[j], recv.at[j], {axis: lax.rem(me + j, 8)})

    def y_slot(d, k, sending):
        if k < 2:
            return (y if sending else (ym, yp)[d]), (k if d == 0 else 1 - k)
        return ((ym, yp)[d] if sending else yo), d

    def y_send(d, part, k):
        slot, sub = y_slot(d, k, True)
        ref = xg.at[slot, piece(part, sub), cols]
        return remote(ref, ref, y_s.at[d, part, k], y_r.at[d, part, k], y_dev[d])

    def y_arrival(d, part, k):
        slot, sub = y_slot(d, k, False)
        ref = xg.at[slot, piece(part, sub), cols]
        return remote(ref, ref, y_s.at[d, part, k], y_r.at[d, part, k], y_dev[d])

    def relay(d, part, k):
        slot, sub = y_slot(d, k, False)
        ref = xg.at[slot, piece(part, sub), cols]
        return remote(ref, ref, l_s.at[d, part, k], l_r.at[d, part, k], mate)

    def relay_arrival(d, part, k):
        slot, sub = y_slot(d, k, False)
        ref = xg.at[slot, piece(part, sub), mate_cols]
        return remote(ref, ref, l_s.at[d, part, k], l_r.at[d, part, k], mate)

    def own_copy(columns):
        ref = xg.at[y, :, columns]
        return remote(ref, ref, own_s.at[0], own_r.at[0], mate)

    sends = []

    def go(copy):
        copy.start()
        sends.append(copy)

    def y_own(part):
        for k in range(2):
            for d in range(2):
                go(y_send(d, part, k))

    for j in range(1, 8):
        go(peer_copy(st_all, st_s, st_r, "tensor", t, j))
    y_own(0)
    go(own_copy(cols))

    def y_first(part):
        for d in range(2):
            y_arrival(d, part, 0).wait_recv()
            go(y_send(d, part, 2))
            go(relay(d, part, 0))

    def y_relay(part, k):
        for d in range(2):
            y_arrival(d, part, k).wait_recv()
            go(relay(d, part, k))

    def y_ready(part, k):
        for d in range(2):
            relay_arrival(d, part, k).wait_recv()

    for copy in small:
        copy.wait()
    step = step_ref[0]
    for i in range(RING):
        modv[i, pl.ds(0, 7), :] = mod_ref[step, :, pl.ds(i * PAIR, PAIR)]

    y_first(0)
    y_own(1)
    y_relay(0, 1)

    for j in range(1, 8):
        peer_arrival(st_all, st_s, st_r, "tensor", t, j).wait_recv()
    means = st_all[:, 0, :]
    squares = st_all[:, 1, :]
    mean = jnp.mean(means, axis=0, keepdims=True)
    off = means - mean
    total_sq = jnp.sum(squares, axis=0, keepdims=True) + FEAT * jnp.sum(
        off * off, axis=0, keepdims=True
    )
    scale = lax.rsqrt(total_sq * (1.0 / WIDTH) + NORM_EPSILON)
    sub_row = lax.broadcasted_iota(jnp.int32, (128, PAD), 0)
    stat[...] = jnp.where(sub_row == 0, mean, jnp.where(sub_row == 1, scale, 0.0)).T

    for copy in loads:
        copy.wait()

    def project_rows(slot, start, rows, weight, shift_row, scale_row, first):
        at = pl.ds(start, rows)
        v = xg[slot, at, :].astype(F32)
        n = (v - stat[at, 0:1]) * stat[at, 1:2]
        n = n * (1.0 + modv[slot, pl.ds(scale_row, 1), :]) + modv[slot, pl.ds(shift_row, 1), :]
        w = weight[pl.ds(pl.multiple_of(slot * PAIR, 128), PAIR), :]
        p = jnp.dot(n.astype(BF16), w, preferred_element_type=F32)
        if first:
            acc[at, :] = p
        else:
            acc[at, :] += p

    def project(slot, part, first=False):
        start, rows = PARTS[part]
        if part == 1:
            project_rows(slot, start + TXT, rows - TXT, wi, 0, 1, first)
            project_rows(slot, start, TXT, wt, 3, 4, first)
        else:
            project_rows(slot, start, rows, wi, 0, 1, first)

    score_scale = math.log2(math.e) / math.sqrt(HD)

    def head_norm(values, gain):
        square = jnp.mean(values * values, axis=-1, keepdims=True)
        return (values * lax.rsqrt(square + NORM_EPSILON) * gain).astype(BF16)

    def q_rows(part):
        start, rows = PARTS[part]
        if part == 0:
            return start, start, rows
        skip = TXT if part == 1 else 0
        return start + skip, start + skip - TXT, rows - skip

    def finish(part):
        at = pl.ds(*PARTS[part])
        for h in range(HEADS):
            keys = acc[at, pl.ds(FEAT + h * HD, HD)]
            kv[z, at, pl.ds(2 * h * HD, HD)] = head_norm(keys, kg_ref[...])
            vals = acc[at, pl.ds(2 * FEAT + h * HD, HD)]
            kv[z, at, pl.ds((2 * h + 1) * HD, HD)] = vals.astype(BF16)
        token, query, rows = q_rows(part)
        for h in range(HEADS):
            q = acc[pl.ds(token, rows), pl.ds(h * HD, HD)]
            qall[0, pl.ds(query, rows), pl.ds(h * HD, HD)] = head_norm(
                q, qg_ref[...] * score_scale
            )

    def z_slot(d, k, sending):
        if k < 2:
            return (z if sending else (zm, zp)[d]), (k if d == 0 else 1 - k)
        return ((zm, zp)[d] if sending else zo), d

    def z_copy(d, g, k, sending):
        slot, sub = z_slot(d, k, sending)
        part, h, heads = GROUPS[g]
        ref = kv.at[slot, piece(part, sub), pl.ds(2 * h * HD, 2 * heads * HD)]
        return remote(ref, ref, z_s.at[d, g, k], z_r.at[d, g, k], z_dev[d])

    def q_copy(part):
        _, query, rows = q_rows(part)
        at = pl.ds(query, rows)
        return remote(qall.at[0, at], qall.at[1, at], q_s.at[part], q_r.at[part], x_dev)

    def z_own(g):
        for k in range(2):
            for d in range(2):
                go(z_copy(d, g, k, True))

    def z_first(g):
        for d in range(2):
            z_copy(d, g, 0, False).wait_recv()
            go(z_copy(d, g, 2, True))

    def z_wait(g, k):
        for d in range(2):
            z_copy(d, g, k, False).wait_recv()

    own_copy(mate_cols).wait_recv()
    project(y, 0, first=True)
    y_ready(0, 0)
    y_ready(0, 1)
    project(ym, 0)
    project(yp, 0)
    y_relay(0, 2)
    y_ready(0, 2)
    project(yo, 0)
    finish(0)
    z_own(0)
    go(q_copy(0))

    y_first(1)
    y_own(2)
    project(y, 1, first=True)
    y_relay(1, 1)
    y_ready(1, 0)
    y_ready(1, 1)
    project(ym, 1)
    project(yp, 1)
    z_first(0)
    y_relay(1, 2)
    project(y, 2, first=True)
    y_ready(1, 2)
    project(yo, 1)
    finish(1)
    z_own(1)
    z_own(3)
    go(q_copy(1))

    y_first(2)
    y_relay(2, 1)
    y_ready(2, 0)
    y_ready(2, 1)
    project(ym, 2)
    project(yp, 2)
    z_first(1)
    y_relay(2, 2)
    y_ready(2, 2)
    project(yo, 2)
    finish(2)
    z_own(2)
    go(q_copy(2))

    for copy in late:
        copy.wait()
    wo_send = remote(my_wo, my_wo, wo_s.at[0], wo_r.at[0], mate)
    go(wo_send)

    length = length_ref[group]

    def values(slot, start, rows, h):
        at = pl.ds(start, rows)
        vals = kv[slot, at, pl.ds((2 * h + 1) * HD, HD)].astype(F32).T
        ones = jnp.ones((VROWS - HD, rows), F32)
        if start <= HEAD_ROWS:
            pos = start - HEAD_ROWS + lax.broadcasted_iota(jnp.int32, (1, rows), 1)
            used = (pos < 0) | (pos >= TXT) | (pos + (xlo * RING + slot) * TXT < length)
            vals = jnp.where(used, vals, 0.0)
            ones = jnp.where(used, ones, 0.0)
        return jnp.concatenate([vals, ones], axis=0).astype(BF16)

    def weighted(slot, start, rows, h, ext, q, at_q):
        scores = lax.dot_general(
            kv[slot, pl.ds(start, rows), pl.ds(2 * h * HD, HD)],
            qall[q, at_q, pl.ds(h * HD, HD)],
            (((1,), (1,)), ((), ())),
            preferred_element_type=F32,
        )
        return jnp.dot(ext, jnp.exp2(scores).astype(BF16), preferred_element_type=F32)

    def attend(slot, h, sets, start=0, rows=TOK, first=False):
        ext = values(slot, start, rows, h)
        for q in sets:
            o = weighted(slot, start, rows, h, ext, q, pl.ds(0, IMG))
            if first:
                oacc[q, h] = o
            else:
                oacc[q, h] += o

    def o_copy(h, at, k=0):
        ref_at = (osend.at[h, :, at], orecv.at[h, :, at])
        return remote(*ref_at, o_s.at[h + k], o_r.at[h + k], x_dev)

    def pack(o, h, at):
        den = o[HD : HD + 1]
        high = den.astype(BF16).astype(F32)
        middle = (den - high).astype(BF16).astype(F32)
        low = den - high - middle
        osend[h, pl.ds(0, HD), at] = o[:HD].astype(BF16)
        pad = jnp.zeros((VROWS - HD - 3, den.shape[1]), F32)
        osend[h, pl.ds(HD, VROWS - HD), at] = jnp.concatenate(
            [high, middle, low, pad], axis=0
        ).astype(BF16)

    whole = pl.ds(0, IMG)

    for h in range(HEADS):
        attend(z, h, (0,), first=True)
    z_first(3)
    z_own(4)
    z_wait(0, 1)
    z_wait(0, 2)
    z_wait(1, 1)
    z_first(2)
    z_own(5)
    for part in range(3):
        q_copy(part).wait_recv()
    for h in range(HEADS):
        attend(z, h, (1,), first=True)
    z_wait(2, 1)
    attend(zm, 0, (1, 0))
    attend(zp, 0, (1, 0))
    z_first(4)
    z_own(6)
    z_wait(3, 1)
    z_wait(4, 1)
    attend(zm, 1, (1, 0))
    z_wait(1, 2)
    z_wait(2, 2)
    attend(zo, 0, (1, 0))
    pack(oacc[1, 0], 0, whole)
    go(o_copy(0, whole))
    z_first(5)
    attend(zp, 1, (1, 0))
    z_wait(3, 2)
    z_wait(4, 2)
    attend(zo, 1, (1, 0))
    pack(oacc[1, 1], 1, whole)
    go(o_copy(1, whole))
    z_first(6)
    z_wait(5, 1)
    z_wait(6, 1)
    attend(zm, 2, (1, 0))
    attend(zp, 2, (1, 0))
    z_wait(5, 2)
    attend(zo, 2, (1, 0), 0, PARTS[2][0])
    z_wait(6, 2)

    order = (yo, yp, ym, y)

    def lanes(i):
        return pl.ds(pl.multiple_of(i * 128, 128), 128)

    last = values(zo, *PARTS[2], 2)
    for j in range(RING):
        at = lanes(order[j])
        pack(oacc[1, 2, :, at] + weighted(zo, *PARTS[2], 2, last, 1, at), 2, at)
        go(o_copy(2, at, j))
    attend(zo, 2, (0,), *PARTS[2])

    for h in range(2):
        o_copy(h, whole).wait_recv()

    def a_copy(j, columns):
        return remote(
            atts.at[j, pl.ds(pl.multiple_of((1 - c) * CH, CH), CH)],
            attb.at[j, :, columns],
            a_s.at[j],
            a_r.at[j],
            mate,
        )

    def combine(j):
        at = lanes(order[j])
        o_copy(2, at, j).wait_recv()
        heads = []
        for h in range(HEADS):
            tail = orecv[h, pl.ds(HD, VROWS - HD), at].astype(F32)
            num = oacc[0, h, pl.ds(0, HD), at] + orecv[h, pl.ds(0, HD), at].astype(F32)
            den = oacc[0, h, pl.ds(HD, 1), at] + (tail[0:1] + tail[1:2] + tail[2:3])
            heads.append((num / den).T)
        atts[j] = jnp.concatenate(heads, axis=1).astype(BF16)
        go(a_copy(j, cols))
        attb[j, :, cols] = atts[j, pl.ds(pl.multiple_of(c * CH, CH), CH), :]

    half = WIDTH // 2
    sides = (pl.ds(0, half), pl.ds(half, half))

    def p_copy(d, k):
        src = (pso.at[d], pdir.at[d], pacc.at[d])[k]
        dst = (ropp.at[d], rdir.at[d], racc.at[d])[k]
        return remote(src, dst, p_s.at[d, k], p_r.at[d, k], y_dev[d])

    def out_side(j, d):
        return jnp.dot(attb[j], wo[:, sides[d]], preferred_element_type=F32)

    def dispatch(j):
        a_copy(j, mate_cols).wait_recv()
        if j == 0:
            for d in range(2):
                pso[d] = out_side(0, d).astype(BF16)
                go(p_copy(d, 0))
        else:
            keep, direct = j - 1, 2 - j
            pdir[keep] = out_side(j, direct).astype(BF16)
            go(p_copy(keep, 1))
            pown[:, sides[keep]] = out_side(j, keep)

    remote(my_wo, wo.at[pl.ds(pl.multiple_of((1 - c) * FEAT, 128), FEAT)], wo_s.at[0], wo_r.at[0], mate).wait_recv()
    for j in range(RING):
        combine(j)
        if j >= 1:
            dispatch(j - 1)
    a_copy(3, mate_cols).wait_recv()
    mine = [out_side(3, d) for d in range(2)]
    for d in range(2):
        p_copy(d, 0).wait_recv()
        pacc[d] = (pown[:, sides[d]] + ropp[d].astype(F32)).astype(BF16)
        go(p_copy(d, 2))
    for d in range(2):
        p_copy(1 - d, 1).wait_recv()
        pown[:, sides[d]] = mine[d] + rdir[1 - d].astype(F32)
    for d in range(2):
        p_copy(d, 2).wait_recv()
        pown[:, sides[d]] += racc[d].astype(F32)

    row = t * CH + TXT * lax.min(lax.div(t * CH, HEAD_ROWS), 1)
    rows = pl.ds(pl.multiple_of(row, CH), CH)
    resid = jnp.concatenate(
        [
            xg[i, rows, :].astype(F32)
            + modv[i, pl.ds(2, 1), :] * pown[:, pl.ds(i * PAIR, PAIR)]
            for i in range(RING)
        ],
        axis=1,
    )
    row_mean = jnp.mean(resid, axis=-1, keepdims=True)
    resid = resid - row_mean
    row_var = jnp.mean(resid * resid, axis=-1, keepdims=True)
    resid = resid * lax.rsqrt(row_var + NORM_EPSILON)
    velocity = jnp.zeros((CH, CH), F32)
    for i in range(RING):
        n = resid[:, i * PAIR : (i + 1) * PAIR] * (1.0 + modv[i, pl.ds(6, 1), :]) + modv[
            i, pl.ds(5, 1), :
        ]
        velocity += lax.dot_general(
            n.astype(BF16),
            fw_ref[:, pl.ds(i * PAIR, PAIR)],
            (((1,), (1,)), ((), ())),
            preferred_element_type=F32,
        )

    total_steps = mod_ref.shape[0]
    count = total_steps + 1.0
    step_delta = -1.0 / count
    flow = (total_steps - jnp.full((1, CH), step, jnp.int32).astype(F32)) / count
    sigma = NOISE_LEVEL * jnp.sqrt(flow / (1.0 - flow))
    spread = sigma * math.sqrt(1.0 / count)
    pull = sigma * sigma / (2.0 * flow)

    def drift(state, v):
        return state + (v + pull * (state + (1.0 - flow) * v)) * step_delta

    latent = lat_ref[...]
    noise = noise_ref[...]
    step_mean = drift(latent, velocity)
    mean_ref[0] = step_mean
    shifted = noise + (drift(latent, old_ref[...].astype(F32)) - step_mean) / spread
    gap = noise * noise - shifted * shifted
    gap = jnp.sum(jnp.sum(gap, axis=1, keepdims=True), axis=0, keepdims=True) * 0.5
    me = s * 8 + t
    rat[me] = jnp.broadcast_to(gap, (1, 128))

    def spot(step, here):
        return lax.rem(here + step, RING)

    seqs = [(1 - xlo if a else xlo) * RING + spot(b, z) for a in range(2) for b in range(RING)]
    tens = [spot(b, y) * 2 + (1 - c if a else c) for a in range(2) for b in range(RING)]
    hops = (0, 1, 2, 1, 1, 2, 3, 2)
    pairs = [(i, j) for i in range(8) for j in range(8) if i or j]
    for i, j in sorted(pairs, key=lambda p: -hops[p[0]] - hops[p[1]]):
        where = {"seq": seqs[i], "tensor": tens[j]}
        remote(rat.at[me], rat.at[me], r_s.at[0], r_r.at[0], where).start()
    told = rat.at[pl.ds(0, 63)]
    everyone = remote(told, told, r_s.at[0], r_r.at[0], mate)
    everyone.wait_recv()
    elements = 64 * CH * CH
    ratio = jnp.sum(rat[...], axis=0) / elements
    ratio_ref[0] = ratio[0, 0]
    everyone.wait_send()
    for copy in sends:
        copy.wait_send()


def shards(
    image_states,
    text_states,
    image_qkv,
    text_qkv,
    image_out,
    final_weight,
    query_gain,
    key_gain,
    modulation,
    latent,
    old_velocity,
    rollout_noise,
    group_ids,
    text_lengths,
    step_ids,
):
    smem = pl.BlockSpec(memory_space=pltpu.SMEM)
    vmem = pl.BlockSpec(memory_space=pltpu.VMEM)
    hbm = pl.BlockSpec(memory_space=pl.ANY)
    dma = pltpu.SemaphoreType.DMA
    half = WIDTH // 2
    return pl.pallas_call(
        block,
        out_shape=(
            pltpu.VMEM(latent.shape, F32),
            pltpu.SMEM((1,), F32),
        ),
        in_specs=[hbm] * 15,
        out_specs=(vmem, smem),
        scratch_shapes=[
            pltpu.SMEM((1,), jnp.int32),
            pltpu.SMEM((1,), jnp.int32),
            pltpu.SMEM((4,), jnp.int32),
            pltpu.VMEM(text_states.shape, BF16),
            pltpu.VMEM((WIDTH, 3 * FEAT), BF16),
            pltpu.VMEM((WIDTH, 3 * FEAT), BF16),
            pltpu.VMEM((PAIR, WIDTH), BF16),
            pltpu.VMEM((CH, WIDTH), BF16),
            pltpu.VMEM((1, HD), F32),
            pltpu.VMEM((1, HD), F32),
            pltpu.VMEM(modulation.shape, F32),
            pltpu.VMEM((CH, CH), F32),
            pltpu.VMEM((CH, CH), BF16),
            pltpu.VMEM((CH, CH), F32),
            pltpu.VMEM((RING, TOK, PAIR), BF16),
            pltpu.VMEM((RING, 8, PAIR), F32),
            pltpu.VMEM((PAD, 128), F32),
            pltpu.VMEM((8, 2, PAD), F32),
            pltpu.VMEM((PAD, 128), F32),
            pltpu.VMEM((TOK, 3 * FEAT), F32),
            pltpu.VMEM((2, IMG, FEAT), BF16),
            pltpu.VMEM((RING, TOK, PAIR), BF16),
            pltpu.VMEM((2, HEADS, VROWS, IMG), F32),
            pltpu.VMEM((HEADS, VROWS, IMG), BF16),
            pltpu.VMEM((HEADS, VROWS, IMG), BF16),
            pltpu.VMEM((RING, 128, FEAT), BF16),
            pltpu.VMEM((RING, CH, PAIR), BF16),
            pltpu.VMEM((2, CH, half), BF16),
            pltpu.VMEM((2, CH, half), BF16),
            pltpu.VMEM((2, CH, half), BF16),
            pltpu.VMEM((CH, WIDTH), F32),
            pltpu.VMEM((2, CH, half), BF16),
            pltpu.VMEM((2, CH, half), BF16),
            pltpu.VMEM((2, CH, half), BF16),
            pltpu.VMEM((64, 1, 128), F32),
            dma((20,)),
            dma((8,)),
            dma((8,)),
            dma((1,)),
            dma((1,)),
            dma((2, 3, 3)),
            dma((2, 3, 3)),
            dma((2, 3, 3)),
            dma((2, 3, 3)),
            dma((2, 7, 3)),
            dma((2, 7, 3)),
            dma((3,)),
            dma((3,)),
            dma((6,)),
            dma((6,)),
            dma((RING,)),
            dma((RING,)),
            dma((1,)),
            dma((1,)),
            dma((2, 3)),
            dma((2, 3)),
            dma((1,)),
            dma((1,)),
        ],
        compiler_params=pltpu.CompilerParams(
            collective_id=0, has_side_effects=True, vmem_limit_bytes=62 * 1024 * 1024
        ),
    )(
        step_ids,
        group_ids,
        text_lengths,
        image_states,
        text_states,
        jnp.transpose(image_qkv, (1, 0, 2)),
        jnp.transpose(text_qkv, (1, 0, 2)),
        image_out,
        final_weight.T,
        query_gain.reshape(1, HD),
        key_gain.reshape(1, HD),
        modulation,
        latent,
        old_velocity,
        rollout_noise,
    )


def solution(mesh):
    placed = (
        P("dp", "seq", "tensor"),
        P(None, "seq", "tensor"),
        P(None, None, "tensor"),
        P(None, None, "tensor"),
        P("tensor", None),
        P(),
        P(),
        P(),
        P(),
        P("dp", ("seq", "tensor"), None),
        P("dp", ("seq", "tensor"), None),
        P("dp", ("seq", "tensor"), None),
        P("dp"),
        P(),
        P("dp"),
    )
    return jax.shard_map(
        shards,
        mesh=mesh,
        in_specs=placed,
        out_specs=(P("dp", ("seq", "tensor"), None), P("dp")),
        check_vma=False,
    )
```

```python
import functools
import math

import jax
import jax.numpy as jnp
from jax import lax
from jax.experimental import pallas as pl
from jax.experimental.pallas import tpu as pltpu
from jax.sharding import PartitionSpec as P

NORM_EPSILON = 1e-06
NOISE_LEVEL = 0.7
F32 = jnp.float32
BF16 = jnp.bfloat16

TXT, IMG, TOK = 64, 512, 576
FEAT, PAIR, WIDTH = 384, 768, 3072
HEADS, HD = 3, 128
CH = 64
RING = 4
HEAD_ROWS = 128
PARTS = ((0, 128), (128, 192), (320, 256))
EARLY = 96
EARLY_AT = 320
LATE_AT = EARLY_AT + EARLY
EPARTS = ((0, 3 * EARLY),)
ZPARTS = ((0, 128), (128, 192), (LATE_AT, TOK - LATE_AT))
EPAD = 384
GROUPS = ((0, 0, 3), (1, 0, 3), (2, 0, 1), (2, 1, 1), (2, 2, 1))
VROWS = HD + 16
PAD = 640


def remote(src, dst, send, recv, where):
    return pltpu.make_async_remote_copy(
        src_ref=src,
        dst_ref=dst,
        send_sem=send,
        recv_sem=recv,
        device_id=where,
        device_id_type=pl.DeviceIdType.MESH,
    )


def piece(part, sub, parts=PARTS):
    start, rows = parts[part]
    return pl.ds(start + sub * (rows // 2), rows // 2)


def block(
    step_hbm,
    group_hbm,
    length_hbm,
    x_hbm,
    text_hbm,
    wi_hbm,
    wt_hbm,
    wo_hbm,
    fw_hbm,
    qg_hbm,
    kg_hbm,
    mod_hbm,
    lat_hbm,
    old_hbm,
    noise_hbm,
    mean_ref,
    ratio_ref,
    step_ref,
    group_ref,
    length_ref,
    text_ref,
    wi,
    wt,
    wo,
    fw_ref,
    qg_ref,
    kg_ref,
    mod_ref,
    lat_ref,
    old_ref,
    noise_ref,
    xg,
    xe,
    modv,
    st_col,
    st_all,
    st_early,
    stat,
    stat_e,
    acc,
    acc_e,
    qall,
    kv,
    oacc,
    osend,
    orecv,
    atts,
    attb,
    pso,
    pdir,
    pacc,
    pown,
    ropp,
    rdir,
    racc,
    rat,
    w_sem,
    st_s,
    st_r,
    own_s,
    own_r,
    e_s,
    e_r,
    se_s,
    se_r,
    y_s,
    y_r,
    l_s,
    l_r,
    z_s,
    z_r,
    q_s,
    q_r,
    o_s,
    o_r,
    a_s,
    a_r,
    wo_s,
    wo_r,
    p_s,
    p_r,
    r_s,
    r_r,
):
    t = lax.axis_index("tensor")
    s = lax.axis_index("seq")
    y, c = lax.div(t, 2), lax.rem(t, 2)
    xlo, z = lax.div(s, RING), lax.rem(s, RING)
    yp, ym, yo = lax.rem(y + 1, RING), lax.rem(y + 3, RING), lax.rem(y + 2, RING)
    zp, zm, zo = lax.rem(z + 1, RING), lax.rem(z + 3, RING), lax.rem(z + 2, RING)
    mate = {"tensor": y * 2 + (1 - c)}
    y_dev = ({"tensor": yp * 2 + c}, {"tensor": ym * 2 + c})
    z_dev = ({"seq": xlo * RING + zp}, {"seq": xlo * RING + zm})
    x_dev = {"seq": (1 - xlo) * RING + z}
    cols = pl.ds(pl.multiple_of(c * FEAT, 128), FEAT)
    mate_cols = pl.ds(pl.multiple_of((1 - c) * FEAT, 128), FEAT)

    barrier = pltpu.get_barrier_semaphore()
    for j in range(1, 8):
        pl.semaphore_signal(
            barrier,
            inc=1,
            device_id={"tensor": lax.rem(t + j, 8)},
            device_id_type=pl.DeviceIdType.MESH,
        )
        pl.semaphore_signal(
            barrier,
            inc=1,
            device_id={"seq": lax.rem(s + j, 8)},
            device_id_type=pl.DeviceIdType.MESH,
        )

    def local(src, dst, k):
        copy = pltpu.make_async_copy(src, dst, w_sem.at[k])
        copy.start()
        return copy

    head_rows = pl.ds(0, HEAD_ROWS)
    rest_rows = pl.ds(HEAD_ROWS, IMG - HEAD_ROWS)
    moved_rows = pl.ds(HEAD_ROWS + TXT, IMG - HEAD_ROWS)
    x_load = local(x_hbm.at[0, head_rows], xg.at[y, head_rows, cols], 7)
    x_rest = local(x_hbm.at[0, rest_rows], xg.at[y, moved_rows, cols], 19)
    text_load = local(text_hbm, text_ref, 8)
    group_load = local(group_hbm, group_ref, 9)
    small = [
        local(step_hbm, step_ref, 10),
        local(length_hbm, length_ref, 11),
        local(mod_hbm, mod_ref, 12),
        local(qg_hbm, qg_ref, 13),
        local(kg_hbm, kg_ref, 14),
    ]
    loads = []
    for j in range(3):
        loads.append(local(wt_hbm.at[j], wt.at[:, pl.ds(j * FEAT, FEAT)], 3 + j))
        loads.append(local(wi_hbm.at[j], wi.at[:, pl.ds(j * FEAT, FEAT)], j))
    my_wo = wo.at[pl.ds(pl.multiple_of(c * FEAT, 128), FEAT)]
    late = [
        local(wo_hbm, my_wo, 6),
        local(fw_hbm, fw_ref, 15),
        local(lat_hbm.at[0], lat_ref, 16),
        local(old_hbm.at[0], old_ref, 17),
        local(noise_hbm.at[0], noise_ref, 18),
    ]

    text_load.wait()
    group_load.wait()
    group = group_ref[0]
    xg[y, pl.ds(HEAD_ROWS, TXT), cols] = text_ref[group]
    x_load.wait()
    x_rest.wait()

    def shard_stats(mine, pad):
        rows = mine.shape[0]
        part_mean = jnp.mean(mine, axis=-1, keepdims=True)
        centred = mine - part_mean
        part_sq = jnp.sum(centred * centred, axis=-1, keepdims=True)
        lane = lax.broadcasted_iota(jnp.int32, (rows, 128), 1)
        st_col[pl.ds(0, rows), :] = jnp.where(
            lane == 0, part_mean, jnp.where(lane == 1, part_sq, 0.0)
        )
        st_col[pl.ds(rows, pad - rows), :] = jnp.zeros((pad - rows, 128), F32)
        return st_col[pl.ds(0, pad), :].T[0:2, :]

    st_all[t] = shard_stats(xg[y, :, cols].astype(F32), PAD)

    pl.semaphore_wait(barrier, 14)

    def peer_copy(buf, send, recv, axis, me, j):
        slot = buf.at[me]
        return remote(slot, slot, send.at[j], recv.at[j], {axis: lax.rem(me + j, 8)})

    def peer_arrival(buf, send, recv, axis, me, j):
        slot = buf.at[lax.rem(me + 8 - j, 8)]
        return remote(slot, slot, send.at[j], recv.at[j], {axis: lax.rem(me + j, 8)})

    def y_slot(d, k, sending):
        if k < 2:
            return (y if sending else (ym, yp)[d]), (k if d == 0 else 1 - k)
        return ((ym, yp)[d] if sending else yo), d

    def held(slot, part, sub, columns):
        if part < 3:
            return xg.at[slot, piece(part, sub), columns]
        return xe.at[slot, piece(part - 3, sub, EPARTS), columns]

    def y_send(d, part, k):
        slot, sub = y_slot(d, k, True)
        ref = held(slot, part, sub, cols)
        return remote(ref, ref, y_s.at[d, part, k], y_r.at[d, part, k], y_dev[d])

    def y_arrival(d, part, k):
        slot, sub = y_slot(d, k, False)
        ref = held(slot, part, sub, cols)
        return remote(ref, ref, y_s.at[d, part, k], y_r.at[d, part, k], y_dev[d])

    def relay(d, part, k):
        slot, sub = y_slot(d, k, False)
        ref = held(slot, part, sub, cols)
        return remote(ref, ref, l_s.at[d, part, k], l_r.at[d, part, k], mate)

    def relay_arrival(d, part, k):
        slot, sub = y_slot(d, k, False)
        ref = held(slot, part, sub, mate_cols)
        return remote(ref, ref, l_s.at[d, part, k], l_r.at[d, part, k], mate)

    def own_copy(columns):
        ref = xg.at[y, :, columns]
        return remote(ref, ref, own_s.at[0], own_r.at[0], mate)

    sends = []

    def go(copy):
        copy.start()
        sends.append(copy)

    def y_own(part, pieces=(0, 1)):
        for k in pieces:
            for d in range(2):
                go(y_send(d, part, k))

    for j in range(1, 8):
        go(peer_copy(st_all, st_s, st_r, "tensor", t, j))
    y_own(0)

    def early_copy(k):
        to = (zp, zm, zo)[k]
        return remote(
            xg.at[y, pl.ds(EARLY_AT, EARLY), cols],
            xe.at[y, pl.ds(k * EARLY, EARLY), cols],
            e_s.at[k],
            e_r.at[k],
            {"seq": xlo * RING + to},
        )

    def early_mate(columns):
        ref = xe.at[y, :, columns]
        return remote(ref, ref, e_s.at[3], e_r.at[3], mate)

    for k in range(3):
        go(early_copy(k))
    go(own_copy(cols))

    def y_first(part):
        for d in range(2):
            y_arrival(d, part, 0).wait_recv()
            go(y_send(d, part, 2))
            go(relay(d, part, 0))

    def y_relay(part, k):
        for d in range(2):
            y_arrival(d, part, k).wait_recv()
            go(relay(d, part, k))

    def y_ready(part, k):
        for d in range(2):
            relay_arrival(d, part, k).wait_recv()

    for copy in small:
        copy.wait()
    step = step_ref[0]
    for i in range(RING):
        modv[i, pl.ds(0, 7), :] = mod_ref[step, :, pl.ds(i * PAIR, PAIR)]

    y_first(0)
    y_own(1)
    y_relay(0, 1)

    def token_stats(buf, pad):
        means = buf[:, 0, :]
        squares = buf[:, 1, :]
        mean = jnp.mean(means, axis=0, keepdims=True)
        off = means - mean
        total_sq = jnp.sum(squares, axis=0, keepdims=True) + FEAT * jnp.sum(
            off * off, axis=0, keepdims=True
        )
        scale = lax.rsqrt(total_sq * (1.0 / WIDTH) + NORM_EPSILON)
        sub_row = lax.broadcasted_iota(jnp.int32, (128, pad), 0)
        return jnp.where(sub_row == 0, mean, jnp.where(sub_row == 1, scale, 0.0)).T

    for j in range(1, 8):
        peer_arrival(st_all, st_s, st_r, "tensor", t, j).wait_recv()
    stat[...] = token_stats(st_all, PAD)

    for copy in loads:
        copy.wait()

    def project_rows(slot, start, rows, weight, shift_row, scale_row, first):
        at = pl.ds(start, rows)
        v = xg[slot, at, :].astype(F32)
        n = (v - stat[at, 0:1]) * stat[at, 1:2]
        n = n * (1.0 + modv[slot, pl.ds(scale_row, 1), :]) + modv[slot, pl.ds(shift_row, 1), :]
        w = weight[pl.ds(pl.multiple_of(slot * PAIR, 128), PAIR), :]
        p = jnp.dot(n.astype(BF16), w, preferred_element_type=F32)
        if first:
            acc[at, :] = p
        else:
            acc[at, :] += p

    def project(slot, part, first=False):
        start, rows = PARTS[part]
        if part == 1:
            project_rows(slot, start + TXT, rows - TXT, wi, 0, 1, first)
            project_rows(slot, start, TXT, wt, 3, 4, first)
        else:
            project_rows(slot, start, rows, wi, 0, 1, first)

    def project_early(slot, first=False):
        at = pl.ds(*EPARTS[0])
        n = (xe[slot, at, :].astype(F32) - stat_e[at, 0:1]) * stat_e[at, 1:2]
        n = n * (1.0 + modv[slot, pl.ds(1, 1), :]) + modv[slot, pl.ds(0, 1), :]
        w = wi[pl.ds(pl.multiple_of(slot * PAIR, 128), PAIR), pl.ds(FEAT, 2 * FEAT)]
        p = jnp.dot(n.astype(BF16), w, preferred_element_type=F32)
        if first:
            acc_e[at, :] = p
        else:
            acc_e[at, :] += p

    score_scale = math.log2(math.e) / math.sqrt(HD)

    def head_norm(values, gain):
        square = jnp.mean(values * values, axis=-1, keepdims=True)
        return (values * lax.rsqrt(square + NORM_EPSILON) * gain).astype(BF16)

    def q_rows(part):
        start, rows = PARTS[part]
        if part == 0:
            return start, start, rows
        skip = TXT if part == 1 else 0
        return start + skip, start + skip - TXT, rows - skip

    def finish(part):
        at = pl.ds(*PARTS[part])
        for h in range(HEADS):
            keys = acc[at, pl.ds(FEAT + h * HD, HD)]
            kv[z, at, pl.ds(2 * h * HD, HD)] = head_norm(keys, kg_ref[...])
            vals = acc[at, pl.ds(2 * FEAT + h * HD, HD)]
            kv[z, at, pl.ds((2 * h + 1) * HD, HD)] = vals.astype(BF16)
        token, query, rows = q_rows(part)
        for h in range(HEADS):
            q = acc[pl.ds(token, rows), pl.ds(h * HD, HD)]
            qall[0, pl.ds(query, rows), pl.ds(h * HD, HD)] = head_norm(
                q, qg_ref[...] * score_scale
            )

    def finish_early(k):
        slot = (zm, zp, zo)[k]
        at = pl.ds(k * EARLY, EARLY)
        to = pl.ds(EARLY_AT, EARLY)
        for h in range(HEADS):
            keys = acc_e[at, pl.ds(h * HD, HD)]
            kv[slot, to, pl.ds(2 * h * HD, HD)] = head_norm(keys, kg_ref[...])
            kv[slot, to, pl.ds((2 * h + 1) * HD, HD)] = acc_e[at, pl.ds(FEAT + h * HD, HD)].astype(BF16)

    def z_slot(d, k, sending):
        if k < 2:
            return (z if sending else (zm, zp)[d]), (k if d == 0 else 1 - k)
        return ((zm, zp)[d] if sending else zo), d

    def z_copy(d, g, k, sending):
        slot, sub = z_slot(d, k, sending)
        part, h, heads = GROUPS[g]
        ref = kv.at[slot, piece(part, sub, ZPARTS), pl.ds(2 * h * HD, 2 * heads * HD)]
        return remote(ref, ref, z_s.at[d, g, k], z_r.at[d, g, k], z_dev[d])

    def q_copy(part):
        _, query, rows = q_rows(part)
        at = pl.ds(query, rows)
        return remote(qall.at[0, at], qall.at[1, at], q_s.at[part], q_r.at[part], x_dev)

    def z_own(g, pieces=(0, 1)):
        for k in pieces:
            for d in range(2):
                go(z_copy(d, g, k, True))

    def z_first(g):
        for d in range(2):
            z_copy(d, g, 0, False).wait_recv()
            go(z_copy(d, g, 2, True))

    def z_wait(g, k):
        for d in range(2):
            z_copy(d, g, k, False).wait_recv()

    own_copy(mate_cols).wait_recv()
    project(y, 0, first=True)
    y_ready(0, 0)
    y_ready(0, 1)
    project(ym, 0)
    project(yp, 0)
    y_relay(0, 2)
    y_ready(0, 2)
    project(yo, 0)
    finish(0)
    z_own(0)
    go(q_copy(0))

    y_first(1)
    y_own(2)
    for k in range(3):
        early_copy(k).wait_recv()
    go(early_mate(cols))
    st_early[t] = shard_stats(xe[y, :, cols].astype(F32), EPAD)
    for j in range(1, 8):
        go(peer_copy(st_early, se_s, se_r, "tensor", t, j))
    project(y, 1, first=True)
    y_relay(1, 1)
    y_ready(1, 0)
    y_ready(1, 1)
    project(ym, 1)
    project(yp, 1)
    z_first(0)
    y_relay(1, 2)
    project(y, 2, first=True)
    y_ready(1, 2)
    project(yo, 1)
    finish(1)
    z_own(1)
    go(q_copy(1))

    y_first(2)
    y_own(3)
    y_relay(2, 1)
    y_ready(2, 0)
    y_ready(2, 1)
    project(ym, 2)
    project(yp, 2)
    z_first(1)
    y_relay(2, 2)
    for j in range(1, 8):
        peer_arrival(st_early, se_s, se_r, "tensor", t, j).wait_recv()
    stat_e[...] = token_stats(st_early, EPAD)
    early_mate(mate_cols).wait_recv()
    project_early(y, first=True)
    y_first(3)
    y_ready(2, 2)
    project(yo, 2)
    finish(2)
    z_own(2)
    z_own(3, (0,))
    go(q_copy(2))

    for copy in late:
        copy.wait()
    wo_send = remote(my_wo, my_wo, wo_s.at[0], wo_r.at[0], mate)
    go(wo_send)

    length = length_ref[group]

    def values(slot, start, rows, h):
        at = pl.ds(start, rows)
        vals = kv[slot, at, pl.ds((2 * h + 1) * HD, HD)].astype(F32).T
        ones = jnp.ones((VROWS - HD, rows), F32)
        if start <= HEAD_ROWS:
            pos = start - HEAD_ROWS + lax.broadcasted_iota(jnp.int32, (1, rows), 1)
            used = (pos < 0) | (pos >= TXT) | (pos + (xlo * RING + slot) * TXT < length)
            vals = jnp.where(used, vals, 0.0)
            ones = jnp.where(used, ones, 0.0)
        return jnp.concatenate([vals, ones], axis=0).astype(BF16)

    def weighted(slot, start, rows, h, ext, q, at_q):
        scores = lax.dot_general(
            kv[slot, pl.ds(start, rows), pl.ds(2 * h * HD, HD)],
            qall[q, at_q, pl.ds(h * HD, HD)],
            (((1,), (1,)), ((), ())),
            preferred_element_type=F32,
        )
        return jnp.dot(ext, jnp.exp2(scores).astype(BF16), preferred_element_type=F32)

    def attend(slot, h, sets, start=0, rows=TOK, first=False):
        ext = values(slot, start, rows, h)
        for q in sets:
            o = weighted(slot, start, rows, h, ext, q, pl.ds(0, IMG))
            if first:
                oacc[q, h] = o
            else:
                oacc[q, h] += o

    order = (yo, yp, ym, y)

    def lanes(i):
        return pl.ds(pl.multiple_of(i * 128, 128), 128)

    def o_copy(h, j):
        at = lanes(order[j])
        k = h * RING + j
        return remote(osend.at[h, :, at], orecv.at[h, :, at], o_s.at[k], o_r.at[k], x_dev)

    def pack(o, h, at):
        den = o[HD : HD + 1]
        high = den.astype(BF16).astype(F32)
        middle = (den - high).astype(BF16).astype(F32)
        low = den - high - middle
        osend[h, pl.ds(0, HD), at] = o[:HD].astype(BF16)
        pad = jnp.zeros((VROWS - HD - 3, den.shape[1]), F32)
        osend[h, pl.ds(HD, VROWS - HD), at] = jnp.concatenate(
            [high, middle, low, pad], axis=0
        ).astype(BF16)

    whole = pl.ds(0, IMG)

    for h in range(HEADS):
        attend(z, h, (0,), first=True)
    y_relay(3, 1)
    z_wait(0, 1)
    z_wait(0, 2)
    z_wait(1, 1)
    for h in range(HEADS):
        attend(zm, h, (0,), 0, EARLY_AT)
        attend(zp, h, (0,), 0, EARLY_AT)
    z_wait(1, 2)
    for h in range(HEADS):
        attend(zo, h, (0,), 0, EARLY_AT)
    z_first(2)
    z_own(3, (1,))
    z_own(4, (0,))
    y_ready(3, 0)
    y_ready(3, 1)
    project_early(ym)
    project_early(yp)
    y_relay(3, 2)
    z_first(3)
    z_own(4, (1,))
    for part in range(3):
        q_copy(part).wait_recv()
    for h in range(HEADS):
        attend(z, h, (1,), first=True)
    y_ready(3, 2)
    project_early(yo)
    for k in range(3):
        finish_early(k)
    z_wait(2, 1)
    attend(zm, 0, (1,))
    attend(zp, 0, (1,))
    z_first(4)
    z_wait(2, 2)
    attend(zo, 0, (1,))
    pack(oacc[1, 0], 0, whole)
    for j in range(3):
        go(o_copy(0, j))
    z_wait(3, 1)
    attend(zm, 1, (1,))
    attend(zp, 1, (1,))
    z_wait(3, 2)
    attend(zo, 1, (1,))
    pack(oacc[1, 1], 1, whole)
    for j in range(2):
        go(o_copy(1, j))
    z_wait(4, 1)
    attend(zm, 2, (1,))
    attend(zp, 2, (1,))
    attend(zo, 2, (1,), 0, LATE_AT)
    z_wait(4, 2)

    last = values(zo, *ZPARTS[2], 2)
    for j in range(RING):
        at = lanes(order[j])
        pack(oacc[1, 2, :, at] + weighted(zo, *ZPARTS[2], 2, last, 1, at), 2, at)
        go(o_copy(2, j))
        if j == 1:
            go(o_copy(1, 2))
        if j == 2:
            go(o_copy(0, 3))
            go(o_copy(1, 3))
    for h in range(HEADS):
        for slot in (zm, zp, zo):
            attend(slot, h, (0,), EARLY_AT, TOK - EARLY_AT)

    def a_copy(j, columns):
        return remote(
            atts.at[j, pl.ds(pl.multiple_of((1 - c) * CH, CH), CH)],
            attb.at[j, :, columns],
            a_s.at[j],
            a_r.at[j],
            mate,
        )

    def combine(j):
        at = lanes(order[j])
        for h in range(HEADS):
            o_copy(h, j).wait_recv()
        heads = []
        for h in range(HEADS):
            tail = orecv[h, pl.ds(HD, VROWS - HD), at].astype(F32)
            num = oacc[0, h, pl.ds(0, HD), at] + orecv[h, pl.ds(0, HD), at].astype(F32)
            den = oacc[0, h, pl.ds(HD, 1), at] + (tail[0:1] + tail[1:2] + tail[2:3])
            heads.append((num / den).T)
        atts[j] = jnp.concatenate(heads, axis=1).astype(BF16)
        go(a_copy(j, cols))
        attb[j, :, cols] = atts[j, pl.ds(pl.multiple_of(c * CH, CH), CH), :]

    half = WIDTH // 2
    sides = (pl.ds(0, half), pl.ds(half, half))

    def p_copy(d, k):
        src = (pso.at[d], pdir.at[d], pacc.at[d])[k]
        dst = (ropp.at[d], rdir.at[d], racc.at[d])[k]
        return remote(src, dst, p_s.at[d, k], p_r.at[d, k], y_dev[d])

    def out_side(j, d):
        return jnp.dot(attb[j], wo[:, sides[d]], preferred_element_type=F32)

    def dispatch(j):
        a_copy(j, mate_cols).wait_recv()
        if j == 0:
            for d in range(2):
                pso[d] = out_side(0, d).astype(BF16)
                go(p_copy(d, 0))
        else:
            keep, direct = j - 1, 2 - j
            pdir[keep] = out_side(j, direct).astype(BF16)
            go(p_copy(keep, 1))
            pown[:, sides[keep]] = out_side(j, keep)

    remote(my_wo, wo.at[pl.ds(pl.multiple_of((1 - c) * FEAT, 128), FEAT)], wo_s.at[0], wo_r.at[0], mate).wait_recv()
    for j in range(RING):
        combine(j)
        if j >= 1:
            dispatch(j - 1)
    a_copy(3, mate_cols).wait_recv()
    mine = [out_side(3, d) for d in range(2)]
    for d in range(2):
        p_copy(d, 0).wait_recv()
        pacc[d] = (pown[:, sides[d]] + ropp[d].astype(F32)).astype(BF16)
        go(p_copy(d, 2))
    for d in range(2):
        p_copy(1 - d, 1).wait_recv()
        pown[:, sides[d]] = mine[d] + rdir[1 - d].astype(F32)
    for d in range(2):
        p_copy(d, 2).wait_recv()
        pown[:, sides[d]] += racc[d].astype(F32)

    row = t * CH + TXT * lax.min(lax.div(t * CH, HEAD_ROWS), 1)
    rows = pl.ds(pl.multiple_of(row, CH), CH)
    resid = jnp.concatenate(
        [
            xg[i, rows, :].astype(F32)
            + modv[i, pl.ds(2, 1), :] * pown[:, pl.ds(i * PAIR, PAIR)]
            for i in range(RING)
        ],
        axis=1,
    )
    row_mean = jnp.mean(resid, axis=-1, keepdims=True)
    resid = resid - row_mean
    row_var = jnp.mean(resid * resid, axis=-1, keepdims=True)
    resid = resid * lax.rsqrt(row_var + NORM_EPSILON)
    velocity = jnp.zeros((CH, CH), F32)
    for i in range(RING):
        n = resid[:, i * PAIR : (i + 1) * PAIR] * (1.0 + modv[i, pl.ds(6, 1), :]) + modv[
            i, pl.ds(5, 1), :
        ]
        velocity += lax.dot_general(
            n.astype(BF16),
            fw_ref[:, pl.ds(i * PAIR, PAIR)],
            (((1,), (1,)), ((), ())),
            preferred_element_type=F32,
        )

    total_steps = mod_ref.shape[0]
    count = total_steps + 1.0
    step_delta = -1.0 / count
    flow = (total_steps - jnp.full((1, CH), step, jnp.int32).astype(F32)) / count
    sigma = NOISE_LEVEL * jnp.sqrt(flow / (1.0 - flow))
    spread = sigma * math.sqrt(1.0 / count)
    pull = sigma * sigma / (2.0 * flow)

    def drift(state, v):
        return state + (v + pull * (state + (1.0 - flow) * v)) * step_delta

    latent = lat_ref[...]
    noise = noise_ref[...]
    step_mean = drift(latent, velocity)
    mean_ref[0] = step_mean
    shifted = noise + (drift(latent, old_ref[...].astype(F32)) - step_mean) / spread
    gap = noise * noise - shifted * shifted
    gap = jnp.sum(jnp.sum(gap, axis=1, keepdims=True), axis=0, keepdims=True) * 0.5
    me = s * 8 + t
    rat[me] = jnp.broadcast_to(gap, (1, 128))

    def spot(step, here):
        return lax.rem(here + step, RING)

    seqs = [(1 - xlo if a else xlo) * RING + spot(b, z) for a in range(2) for b in range(RING)]
    tens = [spot(b, y) * 2 + (1 - c if a else c) for a in range(2) for b in range(RING)]
    hops = (0, 1, 2, 1, 1, 2, 3, 2)
    pairs = [(i, j) for i in range(8) for j in range(8) if i or j]
    for i, j in sorted(pairs, key=lambda p: -hops[p[0]] - hops[p[1]]):
        where = {"seq": seqs[i], "tensor": tens[j]}
        remote(rat.at[me], rat.at[me], r_s.at[0], r_r.at[0], where).start()
    told = rat.at[pl.ds(0, 63)]
    everyone = remote(told, told, r_s.at[0], r_r.at[0], mate)
    everyone.wait_recv()
    elements = 64 * CH * CH
    ratio = jnp.sum(rat[...], axis=0) / elements
    ratio_ref[0] = ratio[0, 0]
    everyone.wait_send()
    for copy in sends:
        copy.wait_send()


def shards(
    image_states,
    text_states,
    image_qkv,
    text_qkv,
    image_out,
    final_weight,
    query_gain,
    key_gain,
    modulation,
    latent,
    old_velocity,
    rollout_noise,
    group_ids,
    text_lengths,
    step_ids,
):
    smem = pl.BlockSpec(memory_space=pltpu.SMEM)
    vmem = pl.BlockSpec(memory_space=pltpu.VMEM)
    hbm = pl.BlockSpec(memory_space=pl.ANY)
    dma = pltpu.SemaphoreType.DMA
    half = WIDTH // 2
    return pl.pallas_call(
        block,
        out_shape=(
            pltpu.VMEM(latent.shape, F32),
            pltpu.SMEM((1,), F32),
        ),
        in_specs=[hbm] * 15,
        out_specs=(vmem, smem),
        scratch_shapes=[
            pltpu.SMEM((1,), jnp.int32),
            pltpu.SMEM((1,), jnp.int32),
            pltpu.SMEM((4,), jnp.int32),
            pltpu.VMEM(text_states.shape, BF16),
            pltpu.VMEM((WIDTH, 3 * FEAT), BF16),
            pltpu.VMEM((WIDTH, 3 * FEAT), BF16),
            pltpu.VMEM((PAIR, WIDTH), BF16),
            pltpu.VMEM((CH, WIDTH), BF16),
            pltpu.VMEM((1, HD), F32),
            pltpu.VMEM((1, HD), F32),
            pltpu.VMEM(modulation.shape, F32),
            pltpu.VMEM((CH, CH), F32),
            pltpu.VMEM((CH, CH), BF16),
            pltpu.VMEM((CH, CH), F32),
            pltpu.VMEM((RING, TOK, PAIR), BF16),
            pltpu.VMEM((RING, 3 * EARLY, PAIR), BF16),
            pltpu.VMEM((RING, 8, PAIR), F32),
            pltpu.VMEM((PAD, 128), F32),
            pltpu.VMEM((8, 2, PAD), F32),
            pltpu.VMEM((8, 2, EPAD), F32),
            pltpu.VMEM((PAD, 128), F32),
            pltpu.VMEM((EPAD, 128), F32),
            pltpu.VMEM((TOK, 3 * FEAT), F32),
            pltpu.VMEM((3 * EARLY, 2 * FEAT), F32),
            pltpu.VMEM((2, IMG, FEAT), BF16),
            pltpu.VMEM((RING, TOK, PAIR), BF16),
            pltpu.VMEM((2, HEADS, VROWS, IMG), F32),
            pltpu.VMEM((HEADS, VROWS, IMG), BF16),
            pltpu.VMEM((HEADS, VROWS, IMG), BF16),
            pltpu.VMEM((RING, 128, FEAT), BF16),
            pltpu.VMEM((RING, CH, PAIR), BF16),
            pltpu.VMEM((2, CH, half), BF16),
            pltpu.VMEM((2, CH, half), BF16),
            pltpu.VMEM((2, CH, half), BF16),
            pltpu.VMEM((CH, WIDTH), F32),
            pltpu.VMEM((2, CH, half), BF16),
            pltpu.VMEM((2, CH, half), BF16),
            pltpu.VMEM((2, CH, half), BF16),
            pltpu.VMEM((64, 1, 128), F32),
            dma((20,)),
            dma((8,)),
            dma((8,)),
            dma((1,)),
            dma((1,)),
            dma((4,)),
            dma((4,)),
            dma((8,)),
            dma((8,)),
            dma((2, 4, 3)),
            dma((2, 4, 3)),
            dma((2, 4, 3)),
            dma((2, 4, 3)),
            dma((2, 5, 3)),
            dma((2, 5, 3)),
            dma((3,)),
            dma((3,)),
            dma((12,)),
            dma((12,)),
            dma((RING,)),
            dma((RING,)),
            dma((1,)),
            dma((1,)),
            dma((2, 3)),
            dma((2, 3)),
            dma((1,)),
            dma((1,)),
        ],
        compiler_params=pltpu.CompilerParams(
            collective_id=0, has_side_effects=True, vmem_limit_bytes=62 * 1024 * 1024
        ),
    )(
        step_ids,
        group_ids,
        text_lengths,
        image_states,
        text_states,
        jnp.transpose(image_qkv, (1, 0, 2)),
        jnp.transpose(text_qkv, (1, 0, 2)),
        image_out,
        final_weight.T,
        query_gain.reshape(1, HD),
        key_gain.reshape(1, HD),
        modulation,
        latent,
        old_velocity,
        rollout_noise,
    )


def solution(mesh):
    placed = (
        P("dp", "seq", "tensor"),
        P(None, "seq", "tensor"),
        P(None, None, "tensor"),
        P(None, None, "tensor"),
        P("tensor", None),
        P(),
        P(),
        P(),
        P(),
        P("dp", ("seq", "tensor"), None),
        P("dp", ("seq", "tensor"), None),
        P("dp", ("seq", "tensor"), None),
        P("dp"),
        P(),
        P("dp"),
    )
    return jax.shard_map(
        shards,
        mesh=mesh,
        in_specs=placed,
        out_specs=(P("dp", ("seq", "tensor"), None), P("dp")),
        check_vma=False,
    )
```

```python
import functools
import math

import jax
import jax.numpy as jnp
from jax import lax
from jax.experimental import pallas as pl
from jax.experimental.pallas import tpu as pltpu
from jax.sharding import PartitionSpec as P

NORM_EPSILON = 1e-06
NOISE_LEVEL = 0.7
F32 = jnp.float32
BF16 = jnp.bfloat16

TXT, IMG, TOK = 64, 512, 576
FEAT, PAIR, WIDTH = 384, 768, 3072
HEADS, HD = 3, 128
CH = 64
RING = 4
HEAD_ROWS = 128
PARTS = ((0, 128), (128, 192), (320, 256))
EARLY = 64
EARLY_AT = 320
LATE_AT = EARLY_AT + EARLY
EPARTS = ((0, 3 * EARLY),)
ZPARTS = ((0, 128), (128, 192), (LATE_AT, TOK - LATE_AT))
EPAD = 256
GROUPS = ((0, 0, 3), (1, 0, 3), (2, 0, 1), (2, 1, 1), (2, 2, 1))
VROWS = HD + 16
PAD = 640


def remote(src, dst, send, recv, where):
    return pltpu.make_async_remote_copy(
        src_ref=src,
        dst_ref=dst,
        send_sem=send,
        recv_sem=recv,
        device_id=where,
        device_id_type=pl.DeviceIdType.MESH,
    )


def piece(part, sub, parts=PARTS):
    start, rows = parts[part]
    return pl.ds(start + sub * (rows // 2), rows // 2)


def block(
    step_hbm,
    group_hbm,
    length_hbm,
    x_hbm,
    text_hbm,
    wi_hbm,
    wt_hbm,
    wo_hbm,
    fw_hbm,
    qg_hbm,
    kg_hbm,
    mod_hbm,
    lat_hbm,
    old_hbm,
    noise_hbm,
    mean_ref,
    ratio_ref,
    step_ref,
    group_ref,
    length_ref,
    text_ref,
    wi,
    wt,
    wo,
    fw_ref,
    qg_ref,
    kg_ref,
    mod_ref,
    lat_ref,
    old_ref,
    noise_ref,
    xg,
    xe,
    modv,
    st_col,
    st_all,
    st_early,
    stat,
    stat_e,
    acc,
    acc_e,
    qall,
    kv,
    oacc,
    osend,
    orecv,
    atts,
    attb,
    pso,
    pdir,
    pacc,
    pown,
    ropp,
    rdir,
    racc,
    rat,
    w_sem,
    st_s,
    st_r,
    own_s,
    own_r,
    e_s,
    e_r,
    se_s,
    se_r,
    y_s,
    y_r,
    l_s,
    l_r,
    z_s,
    z_r,
    q_s,
    q_r,
    o_s,
    o_r,
    a_s,
    a_r,
    wo_s,
    wo_r,
    p_s,
    p_r,
    r_s,
    r_r,
):
    t = lax.axis_index("tensor")
    s = lax.axis_index("seq")
    y, c = lax.div(t, 2), lax.rem(t, 2)
    xlo, z = lax.div(s, RING), lax.rem(s, RING)
    yp, ym, yo = lax.rem(y + 1, RING), lax.rem(y + 3, RING), lax.rem(y + 2, RING)
    zp, zm, zo = lax.rem(z + 1, RING), lax.rem(z + 3, RING), lax.rem(z + 2, RING)
    mate = {"tensor": y * 2 + (1 - c)}
    y_dev = ({"tensor": yp * 2 + c}, {"tensor": ym * 2 + c})
    z_dev = ({"seq": xlo * RING + zp}, {"seq": xlo * RING + zm})
    x_dev = {"seq": (1 - xlo) * RING + z}
    cols = pl.ds(pl.multiple_of(c * FEAT, 128), FEAT)
    mate_cols = pl.ds(pl.multiple_of((1 - c) * FEAT, 128), FEAT)

    barrier = pltpu.get_barrier_semaphore()
    for j in range(1, 8):
        pl.semaphore_signal(
            barrier,
            inc=1,
            device_id={"tensor": lax.rem(t + j, 8)},
            device_id_type=pl.DeviceIdType.MESH,
        )
        pl.semaphore_signal(
            barrier,
            inc=1,
            device_id={"seq": lax.rem(s + j, 8)},
            device_id_type=pl.DeviceIdType.MESH,
        )

    def local(src, dst, k):
        copy = pltpu.make_async_copy(src, dst, w_sem.at[k])
        copy.start()
        return copy

    head_rows = pl.ds(0, HEAD_ROWS)
    rest_rows = pl.ds(HEAD_ROWS, IMG - HEAD_ROWS)
    moved_rows = pl.ds(HEAD_ROWS + TXT, IMG - HEAD_ROWS)
    x_load = local(x_hbm.at[0, head_rows], xg.at[y, head_rows, cols], 7)
    x_rest = local(x_hbm.at[0, rest_rows], xg.at[y, moved_rows, cols], 19)
    text_load = local(text_hbm, text_ref, 8)
    group_load = local(group_hbm, group_ref, 9)
    small = [
        local(step_hbm, step_ref, 10),
        local(length_hbm, length_ref, 11),
        local(mod_hbm, mod_ref, 12),
        local(qg_hbm, qg_ref, 13),
        local(kg_hbm, kg_ref, 14),
    ]
    loads = []
    for j in range(3):
        loads.append(local(wt_hbm.at[j], wt.at[:, pl.ds(j * FEAT, FEAT)], 3 + j))
        loads.append(local(wi_hbm.at[j], wi.at[:, pl.ds(j * FEAT, FEAT)], j))
    my_wo = wo.at[pl.ds(pl.multiple_of(c * FEAT, 128), FEAT)]
    late = [
        local(wo_hbm, my_wo, 6),
        local(fw_hbm, fw_ref, 15),
        local(lat_hbm.at[0], lat_ref, 16),
        local(old_hbm.at[0], old_ref, 17),
        local(noise_hbm.at[0], noise_ref, 18),
    ]

    text_load.wait()
    group_load.wait()
    group = group_ref[0]
    xg[y, pl.ds(HEAD_ROWS, TXT), cols] = text_ref[group]
    x_load.wait()
    x_rest.wait()

    def shard_stats(mine, pad):
        rows = mine.shape[0]
        part_mean = jnp.mean(mine, axis=-1, keepdims=True)
        centred = mine - part_mean
        part_sq = jnp.sum(centred * centred, axis=-1, keepdims=True)
        lane = lax.broadcasted_iota(jnp.int32, (rows, 128), 1)
        st_col[pl.ds(0, rows), :] = jnp.where(
            lane == 0, part_mean, jnp.where(lane == 1, part_sq, 0.0)
        )
        st_col[pl.ds(rows, pad - rows), :] = jnp.zeros((pad - rows, 128), F32)
        return st_col[pl.ds(0, pad), :].T[0:2, :]

    st_all[t] = shard_stats(xg[y, :, cols].astype(F32), PAD)

    pl.semaphore_wait(barrier, 14)

    def peer_copy(buf, send, recv, axis, me, j):
        slot = buf.at[me]
        return remote(slot, slot, send.at[j], recv.at[j], {axis: lax.rem(me + j, 8)})

    def peer_arrival(buf, send, recv, axis, me, j):
        slot = buf.at[lax.rem(me + 8 - j, 8)]
        return remote(slot, slot, send.at[j], recv.at[j], {axis: lax.rem(me + j, 8)})

    def y_slot(d, k, sending):
        if k < 2:
            return (y if sending else (ym, yp)[d]), (k if d == 0 else 1 - k)
        return ((ym, yp)[d] if sending else yo), d

    def held(slot, part, sub, columns):
        if part < 3:
            return xg.at[slot, piece(part, sub), columns]
        return xe.at[slot, piece(part - 3, sub, EPARTS), columns]

    def y_send(d, part, k):
        slot, sub = y_slot(d, k, True)
        ref = held(slot, part, sub, cols)
        return remote(ref, ref, y_s.at[d, part, k], y_r.at[d, part, k], y_dev[d])

    def y_arrival(d, part, k):
        slot, sub = y_slot(d, k, False)
        ref = held(slot, part, sub, cols)
        return remote(ref, ref, y_s.at[d, part, k], y_r.at[d, part, k], y_dev[d])

    def relay(d, part, k):
        slot, sub = y_slot(d, k, False)
        ref = held(slot, part, sub, cols)
        return remote(ref, ref, l_s.at[d, part, k], l_r.at[d, part, k], mate)

    def relay_arrival(d, part, k):
        slot, sub = y_slot(d, k, False)
        ref = held(slot, part, sub, mate_cols)
        return remote(ref, ref, l_s.at[d, part, k], l_r.at[d, part, k], mate)

    def own_copy(columns):
        ref = xg.at[y, :, columns]
        return remote(ref, ref, own_s.at[0], own_r.at[0], mate)

    sends = []

    def go(copy):
        copy.start()
        sends.append(copy)

    def y_own(part, pieces=(0, 1)):
        for k in pieces:
            for d in range(2):
                go(y_send(d, part, k))

    for j in range(1, 8):
        go(peer_copy(st_all, st_s, st_r, "tensor", t, j))
    y_own(0)

    def early_copy(k):
        to = (zp, zm, zo)[k]
        return remote(
            xg.at[y, pl.ds(EARLY_AT, EARLY), cols],
            xe.at[y, pl.ds(k * EARLY, EARLY), cols],
            e_s.at[k],
            e_r.at[k],
            {"seq": xlo * RING + to},
        )

    def early_mate(columns):
        ref = xe.at[y, :, columns]
        return remote(ref, ref, e_s.at[3], e_r.at[3], mate)

    for k in range(3):
        go(early_copy(k))
    go(own_copy(cols))

    def y_first(part):
        for d in range(2):
            y_arrival(d, part, 0).wait_recv()
            go(y_send(d, part, 2))
            go(relay(d, part, 0))

    def y_relay(part, k):
        for d in range(2):
            y_arrival(d, part, k).wait_recv()
            go(relay(d, part, k))

    def y_ready(part, k):
        for d in range(2):
            relay_arrival(d, part, k).wait_recv()

    for copy in small:
        copy.wait()
    step = step_ref[0]
    for i in range(RING):
        modv[i, pl.ds(0, 7), :] = mod_ref[step, :, pl.ds(i * PAIR, PAIR)]

    y_first(0)
    y_own(1)
    y_relay(0, 1)

    def token_stats(buf, pad):
        means = buf[:, 0, :]
        squares = buf[:, 1, :]
        mean = jnp.mean(means, axis=0, keepdims=True)
        off = means - mean
        total_sq = jnp.sum(squares, axis=0, keepdims=True) + FEAT * jnp.sum(
            off * off, axis=0, keepdims=True
        )
        scale = lax.rsqrt(total_sq * (1.0 / WIDTH) + NORM_EPSILON)
        sub_row = lax.broadcasted_iota(jnp.int32, (128, pad), 0)
        return jnp.where(sub_row == 0, mean, jnp.where(sub_row == 1, scale, 0.0)).T

    for j in range(1, 8):
        peer_arrival(st_all, st_s, st_r, "tensor", t, j).wait_recv()
    stat[...] = token_stats(st_all, PAD)

    for copy in loads:
        copy.wait()

    def project_rows(slot, start, rows, weight, shift_row, scale_row, first):
        at = pl.ds(start, rows)
        v = xg[slot, at, :].astype(F32)
        n = (v - stat[at, 0:1]) * stat[at, 1:2]
        n = n * (1.0 + modv[slot, pl.ds(scale_row, 1), :]) + modv[slot, pl.ds(shift_row, 1), :]
        w = weight[pl.ds(pl.multiple_of(slot * PAIR, 128), PAIR), :]
        p = jnp.dot(n.astype(BF16), w, preferred_element_type=F32)
        if first:
            acc[at, :] = p
        else:
            acc[at, :] += p

    def project(slot, part, first=False):
        start, rows = PARTS[part]
        if part == 1:
            project_rows(slot, start + TXT, rows - TXT, wi, 0, 1, first)
            project_rows(slot, start, TXT, wt, 3, 4, first)
        else:
            project_rows(slot, start, rows, wi, 0, 1, first)

    def project_early(slot, first=False):
        at = pl.ds(*EPARTS[0])
        n = (xe[slot, at, :].astype(F32) - stat_e[at, 0:1]) * stat_e[at, 1:2]
        n = n * (1.0 + modv[slot, pl.ds(1, 1), :]) + modv[slot, pl.ds(0, 1), :]
        w = wi[pl.ds(pl.multiple_of(slot * PAIR, 128), PAIR), pl.ds(FEAT, 2 * FEAT)]
        p = jnp.dot(n.astype(BF16), w, preferred_element_type=F32)
        if first:
            acc_e[at, :] = p
        else:
            acc_e[at, :] += p

    score_scale = math.log2(math.e) / math.sqrt(HD)

    def head_norm(values, gain):
        square = jnp.mean(values * values, axis=-1, keepdims=True)
        return (values * lax.rsqrt(square + NORM_EPSILON) * gain).astype(BF16)

    def q_rows(part):
        start, rows = PARTS[part]
        if part == 0:
            return start, start, rows
        skip = TXT if part == 1 else 0
        return start + skip, start + skip - TXT, rows - skip

    def finish(part):
        at = pl.ds(*PARTS[part])
        for h in range(HEADS):
            keys = acc[at, pl.ds(FEAT + h * HD, HD)]
            kv[z, at, pl.ds(2 * h * HD, HD)] = head_norm(keys, kg_ref[...])
            vals = acc[at, pl.ds(2 * FEAT + h * HD, HD)]
            kv[z, at, pl.ds((2 * h + 1) * HD, HD)] = vals.astype(BF16)
        token, query, rows = q_rows(part)
        for h in range(HEADS):
            q = acc[pl.ds(token, rows), pl.ds(h * HD, HD)]
            qall[0, pl.ds(query, rows), pl.ds(h * HD, HD)] = head_norm(
                q, qg_ref[...] * score_scale
            )

    def finish_early(k):
        slot = (zm, zp, zo)[k]
        at = pl.ds(k * EARLY, EARLY)
        to = pl.ds(EARLY_AT, EARLY)
        for h in range(HEADS):
            keys = acc_e[at, pl.ds(h * HD, HD)]
            kv[slot, to, pl.ds(2 * h * HD, HD)] = head_norm(keys, kg_ref[...])
            kv[slot, to, pl.ds((2 * h + 1) * HD, HD)] = acc_e[at, pl.ds(FEAT + h * HD, HD)].astype(BF16)

    def z_slot(d, k, sending):
        if k < 2:
            return (z if sending else (zm, zp)[d]), (k if d == 0 else 1 - k)
        return ((zm, zp)[d] if sending else zo), d

    def z_copy(d, g, k, sending):
        slot, sub = z_slot(d, k, sending)
        part, h, heads = GROUPS[g]
        ref = kv.at[slot, piece(part, sub, ZPARTS), pl.ds(2 * h * HD, 2 * heads * HD)]
        return remote(ref, ref, z_s.at[d, g, k], z_r.at[d, g, k], z_dev[d])

    def q_copy(part):
        _, query, rows = q_rows(part)
        at = pl.ds(query, rows)
        return remote(qall.at[0, at], qall.at[1, at], q_s.at[part], q_r.at[part], x_dev)

    def z_own(g, pieces=(0, 1)):
        for k in pieces:
            for d in range(2):
                go(z_copy(d, g, k, True))

    def z_first(g):
        for d in range(2):
            z_copy(d, g, 0, False).wait_recv()
            go(z_copy(d, g, 2, True))

    def z_wait(g, k):
        for d in range(2):
            z_copy(d, g, k, False).wait_recv()

    own_copy(mate_cols).wait_recv()
    project(y, 0, first=True)
    y_ready(0, 0)
    y_ready(0, 1)
    project(ym, 0)
    project(yp, 0)
    y_relay(0, 2)
    y_ready(0, 2)
    project(yo, 0)
    finish(0)
    z_own(0)
    go(q_copy(0))

    y_first(1)
    y_own(2)
    for k in range(3):
        early_copy(k).wait_recv()
    go(early_mate(cols))
    st_early[t] = shard_stats(xe[y, :, cols].astype(F32), EPAD)
    for j in range(1, 8):
        go(peer_copy(st_early, se_s, se_r, "tensor", t, j))
    project(y, 1, first=True)
    y_relay(1, 1)
    y_ready(1, 0)
    y_ready(1, 1)
    project(ym, 1)
    project(yp, 1)
    z_first(0)
    y_relay(1, 2)
    project(y, 2, first=True)
    y_ready(1, 2)
    project(yo, 1)
    finish(1)
    z_own(1)
    go(q_copy(1))

    y_first(2)
    y_own(3)
    y_relay(2, 1)
    y_ready(2, 0)
    y_ready(2, 1)
    project(ym, 2)
    project(yp, 2)
    z_first(1)
    y_relay(2, 2)
    for j in range(1, 8):
        peer_arrival(st_early, se_s, se_r, "tensor", t, j).wait_recv()
    stat_e[...] = token_stats(st_early, EPAD)
    early_mate(mate_cols).wait_recv()
    project_early(y, first=True)
    y_first(3)
    y_ready(2, 2)
    project(yo, 2)
    finish(2)
    z_own(2)
    z_own(3)
    z_own(4, (0,))
    go(q_copy(2))

    for copy in late:
        copy.wait()
    wo_send = remote(my_wo, my_wo, wo_s.at[0], wo_r.at[0], mate)
    go(wo_send)

    length = length_ref[group]

    def values(slot, start, rows, h):
        at = pl.ds(start, rows)
        vals = kv[slot, at, pl.ds((2 * h + 1) * HD, HD)].astype(F32).T
        ones = jnp.ones((VROWS - HD, rows), F32)
        if start <= HEAD_ROWS:
            pos = start - HEAD_ROWS + lax.broadcasted_iota(jnp.int32, (1, rows), 1)
            used = (pos < 0) | (pos >= TXT) | (pos + (xlo * RING + slot) * TXT < length)
            vals = jnp.where(used, vals, 0.0)
            ones = jnp.where(used, ones, 0.0)
        return jnp.concatenate([vals, ones], axis=0).astype(BF16)

    def weighted(slot, start, rows, h, ext, q, at_q):
        scores = lax.dot_general(
            kv[slot, pl.ds(start, rows), pl.ds(2 * h * HD, HD)],
            qall[q, at_q, pl.ds(h * HD, HD)],
            (((1,), (1,)), ((), ())),
            preferred_element_type=F32,
        )
        return jnp.dot(ext, jnp.exp2(scores).astype(BF16), preferred_element_type=F32)

    def attend(slot, h, sets, start=0, rows=TOK, first=False):
        ext = values(slot, start, rows, h)
        for q in sets:
            o = weighted(slot, start, rows, h, ext, q, pl.ds(0, IMG))
            if first:
                oacc[q, h] = o
            else:
                oacc[q, h] += o

    order = (yo, yp, ym, y)

    def lanes(i):
        return pl.ds(pl.multiple_of(i * 128, 128), 128)

    def o_copy(h, j):
        at = lanes(order[j])
        k = h * RING + j
        return remote(osend.at[h, :, at], orecv.at[h, :, at], o_s.at[k], o_r.at[k], x_dev)

    def pack(o, h, at):
        den = o[HD : HD + 1]
        high = den.astype(BF16).astype(F32)
        middle = (den - high).astype(BF16).astype(F32)
        low = den - high - middle
        osend[h, pl.ds(0, HD), at] = o[:HD].astype(BF16)
        pad = jnp.zeros((VROWS - HD - 3, den.shape[1]), F32)
        osend[h, pl.ds(HD, VROWS - HD), at] = jnp.concatenate(
            [high, middle, low, pad], axis=0
        ).astype(BF16)

    whole = pl.ds(0, IMG)

    for h in range(HEADS):
        attend(z, h, (0,), first=True)
    y_relay(3, 1)
    z_wait(0, 1)
    z_wait(0, 2)
    z_wait(1, 1)
    for h in range(HEADS):
        attend(zm, h, (0,), 0, EARLY_AT)
        attend(zp, h, (0,), 0, EARLY_AT)
    z_wait(1, 2)
    for h in range(HEADS):
        attend(zo, h, (0,), 0, EARLY_AT)
    z_first(2)
    z_own(4, (1,))
    y_ready(3, 0)
    y_ready(3, 1)
    project_early(ym)
    project_early(yp)
    y_relay(3, 2)
    for part in range(3):
        q_copy(part).wait_recv()
    for h in range(HEADS):
        attend(z, h, (1,), first=True)
        if h == 1:
            z_first(3)
    y_ready(3, 2)
    project_early(yo)
    for k in range(3):
        finish_early(k)
    z_wait(2, 1)
    attend(zm, 0, (1,))
    attend(zp, 0, (1,))
    z_first(4)
    z_wait(2, 2)
    attend(zo, 0, (1,))
    pack(oacc[1, 0], 0, whole)
    for j in range(3):
        go(o_copy(0, j))
    z_wait(3, 1)
    attend(zm, 1, (1,))
    attend(zp, 1, (1,))
    z_wait(3, 2)
    attend(zo, 1, (1,))
    pack(oacc[1, 1], 1, whole)
    for j in range(2):
        go(o_copy(1, j))
    z_wait(4, 1)
    attend(zm, 2, (1,))
    attend(zp, 2, (1,))
    attend(zo, 2, (1,), 0, LATE_AT)
    z_wait(4, 2)

    last = values(zo, *ZPARTS[2], 2)
    for j in range(RING):
        at = lanes(order[j])
        pack(oacc[1, 2, :, at] + weighted(zo, *ZPARTS[2], 2, last, 1, at), 2, at)
        go(o_copy(2, j))
        if j == 1:
            go(o_copy(1, 2))
        if j == 2:
            go(o_copy(0, 3))
            go(o_copy(1, 3))
    for h in range(HEADS):
        for slot in (zm, zp, zo):
            attend(slot, h, (0,), EARLY_AT, TOK - EARLY_AT)

    def a_copy(j, columns):
        return remote(
            atts.at[j, pl.ds(pl.multiple_of((1 - c) * CH, CH), CH)],
            attb.at[j, :, columns],
            a_s.at[j],
            a_r.at[j],
            mate,
        )

    def combine(j):
        at = lanes(order[j])
        for h in range(HEADS):
            o_copy(h, j).wait_recv()
        heads = []
        for h in range(HEADS):
            tail = orecv[h, pl.ds(HD, VROWS - HD), at].astype(F32)
            num = oacc[0, h, pl.ds(0, HD), at] + orecv[h, pl.ds(0, HD), at].astype(F32)
            den = oacc[0, h, pl.ds(HD, 1), at] + (tail[0:1] + tail[1:2] + tail[2:3])
            heads.append((num / den).T)
        atts[j] = jnp.concatenate(heads, axis=1).astype(BF16)
        go(a_copy(j, cols))
        attb[j, :, cols] = atts[j, pl.ds(pl.multiple_of(c * CH, CH), CH), :]

    half = WIDTH // 2
    sides = (pl.ds(0, half), pl.ds(half, half))

    def p_copy(d, k):
        src = (pso.at[d], pdir.at[d], pacc.at[d])[k]
        dst = (ropp.at[d], rdir.at[d], racc.at[d])[k]
        return remote(src, dst, p_s.at[d, k], p_r.at[d, k], y_dev[d])

    def out_side(j, d):
        return jnp.dot(attb[j], wo[:, sides[d]], preferred_element_type=F32)

    def dispatch(j):
        a_copy(j, mate_cols).wait_recv()
        if j == 0:
            for d in range(2):
                pso[d] = out_side(0, d).astype(BF16)
                go(p_copy(d, 0))
        else:
            keep, direct = j - 1, 2 - j
            pdir[keep] = out_side(j, direct).astype(BF16)
            go(p_copy(keep, 1))
            pown[:, sides[keep]] = out_side(j, keep)

    remote(my_wo, wo.at[pl.ds(pl.multiple_of((1 - c) * FEAT, 128), FEAT)], wo_s.at[0], wo_r.at[0], mate).wait_recv()
    for j in range(3):
        combine(j)
        dispatch(j)
    for d in range(2):
        p_copy(d, 0).wait_recv()
        pacc[d] = (pown[:, sides[d]] + ropp[d].astype(F32)).astype(BF16)
        go(p_copy(d, 2))
    combine(3)
    a_copy(3, mate_cols).wait_recv()
    mine = [out_side(3, d) for d in range(2)]
    for d in range(2):
        p_copy(1 - d, 1).wait_recv()
        pown[:, sides[d]] = mine[d] + rdir[1 - d].astype(F32)
    for d in range(2):
        p_copy(d, 2).wait_recv()
        pown[:, sides[d]] += racc[d].astype(F32)

    row = t * CH + TXT * lax.min(lax.div(t * CH, HEAD_ROWS), 1)
    rows = pl.ds(pl.multiple_of(row, CH), CH)
    resid = jnp.concatenate(
        [
            xg[i, rows, :].astype(F32)
            + modv[i, pl.ds(2, 1), :] * pown[:, pl.ds(i * PAIR, PAIR)]
            for i in range(RING)
        ],
        axis=1,
    )
    row_mean = jnp.mean(resid, axis=-1, keepdims=True)
    resid = resid - row_mean
    row_var = jnp.mean(resid * resid, axis=-1, keepdims=True)
    resid = resid * lax.rsqrt(row_var + NORM_EPSILON)
    velocity = jnp.zeros((CH, CH), F32)
    for i in range(RING):
        n = resid[:, i * PAIR : (i + 1) * PAIR] * (1.0 + modv[i, pl.ds(6, 1), :]) + modv[
            i, pl.ds(5, 1), :
        ]
        velocity += lax.dot_general(
            n.astype(BF16),
            fw_ref[:, pl.ds(i * PAIR, PAIR)],
            (((1,), (1,)), ((), ())),
            preferred_element_type=F32,
        )

    total_steps = mod_ref.shape[0]
    count = total_steps + 1.0
    step_delta = -1.0 / count
    flow = (total_steps - jnp.full((1, CH), step, jnp.int32).astype(F32)) / count
    sigma = NOISE_LEVEL * jnp.sqrt(flow / (1.0 - flow))
    spread = sigma * math.sqrt(1.0 / count)
    pull = sigma * sigma / (2.0 * flow)

    def drift(state, v):
        return state + (v + pull * (state + (1.0 - flow) * v)) * step_delta

    latent = lat_ref[...]
    noise = noise_ref[...]
    step_mean = drift(latent, velocity)
    mean_ref[0] = step_mean
    shifted = noise + (drift(latent, old_ref[...].astype(F32)) - step_mean) / spread
    gap = noise * noise - shifted * shifted
    gap = jnp.sum(jnp.sum(gap, axis=1, keepdims=True), axis=0, keepdims=True) * 0.5
    me = s * 8 + t
    rat[me] = jnp.broadcast_to(gap, (1, 128))

    def spot(step, here):
        return lax.rem(here + step, RING)

    seqs = [(1 - xlo if a else xlo) * RING + spot(b, z) for a in range(2) for b in range(RING)]
    tens = [spot(b, y) * 2 + (1 - c if a else c) for a in range(2) for b in range(RING)]
    hops = (0, 1, 2, 1, 1, 2, 3, 2)
    pairs = [(i, j) for i in range(8) for j in range(8) if i or j]
    for i, j in sorted(pairs, key=lambda p: -hops[p[0]] - hops[p[1]]):
        where = {"seq": seqs[i], "tensor": tens[j]}
        remote(rat.at[me], rat.at[me], r_s.at[0], r_r.at[0], where).start()
    told = rat.at[pl.ds(0, 63)]
    everyone = remote(told, told, r_s.at[0], r_r.at[0], mate)
    everyone.wait_recv()
    elements = 64 * CH * CH
    ratio = jnp.sum(rat[...], axis=0) / elements
    ratio_ref[0] = ratio[0, 0]
    everyone.wait_send()
    for copy in sends:
        copy.wait_send()


def shards(
    image_states,
    text_states,
    image_qkv,
    text_qkv,
    image_out,
    final_weight,
    query_gain,
    key_gain,
    modulation,
    latent,
    old_velocity,
    rollout_noise,
    group_ids,
    text_lengths,
    step_ids,
):
    smem = pl.BlockSpec(memory_space=pltpu.SMEM)
    vmem = pl.BlockSpec(memory_space=pltpu.VMEM)
    hbm = pl.BlockSpec(memory_space=pl.ANY)
    dma = pltpu.SemaphoreType.DMA
    half = WIDTH // 2
    return pl.pallas_call(
        block,
        out_shape=(
            pltpu.VMEM(latent.shape, F32),
            pltpu.SMEM((1,), F32),
        ),
        in_specs=[hbm] * 15,
        out_specs=(vmem, smem),
        scratch_shapes=[
            pltpu.SMEM((1,), jnp.int32),
            pltpu.SMEM((1,), jnp.int32),
            pltpu.SMEM((4,), jnp.int32),
            pltpu.VMEM(text_states.shape, BF16),
            pltpu.VMEM((WIDTH, 3 * FEAT), BF16),
            pltpu.VMEM((WIDTH, 3 * FEAT), BF16),
            pltpu.VMEM((PAIR, WIDTH), BF16),
            pltpu.VMEM((CH, WIDTH), BF16),
            pltpu.VMEM((1, HD), F32),
            pltpu.VMEM((1, HD), F32),
            pltpu.VMEM(modulation.shape, F32),
            pltpu.VMEM((CH, CH), F32),
            pltpu.VMEM((CH, CH), BF16),
            pltpu.VMEM((CH, CH), F32),
            pltpu.VMEM((RING, TOK, PAIR), BF16),
            pltpu.VMEM((RING, 3 * EARLY, PAIR), BF16),
            pltpu.VMEM((RING, 8, PAIR), F32),
            pltpu.VMEM((PAD, 128), F32),
            pltpu.VMEM((8, 2, PAD), F32),
            pltpu.VMEM((8, 2, EPAD), F32),
            pltpu.VMEM((PAD, 128), F32),
            pltpu.VMEM((EPAD, 128), F32),
            pltpu.VMEM((TOK, 3 * FEAT), F32),
            pltpu.VMEM((3 * EARLY, 2 * FEAT), F32),
            pltpu.VMEM((2, IMG, FEAT), BF16),
            pltpu.VMEM((RING, TOK, PAIR), BF16),
            pltpu.VMEM((2, HEADS, VROWS, IMG), F32),
            pltpu.VMEM((HEADS, VROWS, IMG), BF16),
            pltpu.VMEM((HEADS, VROWS, IMG), BF16),
            pltpu.VMEM((RING, 128, FEAT), BF16),
            pltpu.VMEM((RING, CH, PAIR), BF16),
            pltpu.VMEM((2, CH, half), BF16),
            pltpu.VMEM((2, CH, half), BF16),
            pltpu.VMEM((2, CH, half), BF16),
            pltpu.VMEM((CH, WIDTH), F32),
            pltpu.VMEM((2, CH, half), BF16),
            pltpu.VMEM((2, CH, half), BF16),
            pltpu.VMEM((2, CH, half), BF16),
            pltpu.VMEM((64, 1, 128), F32),
            dma((20,)),
            dma((8,)),
            dma((8,)),
            dma((1,)),
            dma((1,)),
            dma((4,)),
            dma((4,)),
            dma((8,)),
            dma((8,)),
            dma((2, 4, 3)),
            dma((2, 4, 3)),
            dma((2, 4, 3)),
            dma((2, 4, 3)),
            dma((2, 5, 3)),
            dma((2, 5, 3)),
            dma((3,)),
            dma((3,)),
            dma((12,)),
            dma((12,)),
            dma((RING,)),
            dma((RING,)),
            dma((1,)),
            dma((1,)),
            dma((2, 3)),
            dma((2, 3)),
            dma((1,)),
            dma((1,)),
        ],
        compiler_params=pltpu.CompilerParams(
            collective_id=0, has_side_effects=True, vmem_limit_bytes=62 * 1024 * 1024
        ),
    )(
        step_ids,
        group_ids,
        text_lengths,
        image_states,
        text_states,
        jnp.transpose(image_qkv, (1, 0, 2)),
        jnp.transpose(text_qkv, (1, 0, 2)),
        image_out,
        final_weight.T,
        query_gain.reshape(1, HD),
        key_gain.reshape(1, HD),
        modulation,
        latent,
        old_velocity,
        rollout_noise,
    )


def solution(mesh):
    placed = (
        P("dp", "seq", "tensor"),
        P(None, "seq", "tensor"),
        P(None, None, "tensor"),
        P(None, None, "tensor"),
        P("tensor", None),
        P(),
        P(),
        P(),
        P(),
        P("dp", ("seq", "tensor"), None),
        P("dp", ("seq", "tensor"), None),
        P("dp", ("seq", "tensor"), None),
        P("dp"),
        P(),
        P("dp"),
    )
    return jax.shard_map(
        shards,
        mesh=mesh,
        in_specs=placed,
        out_specs=(P("dp", ("seq", "tensor"), None), P("dp")),
        check_vma=False,
    )
```

```python
import functools
import math

import jax
import jax.numpy as jnp
from jax import lax
from jax.experimental import pallas as pl
from jax.experimental.pallas import tpu as pltpu
from jax.sharding import PartitionSpec as P

NORM_EPSILON = 1e-06
NOISE_LEVEL = 0.7
F32 = jnp.float32
BF16 = jnp.bfloat16

TXT, IMG, TOK = 64, 512, 576
FEAT, PAIR, WIDTH = 384, 768, 3072
HEADS, HD = 3, 128
CH = 64
RING = 4
HEAD_ROWS = 128
PARTS = ((0, 128), (128, 192), (320, 256))
EARLY = 64
EARLY_AT = 320
LATE_AT = EARLY_AT + EARLY
EPARTS = ((0, 3 * EARLY),)
ZPARTS = ((0, 128), (128, 192), (LATE_AT, TOK - LATE_AT))
EPAD = 256
GROUPS = ((0, 0, 3), (1, 0, 3), (2, 0, 1), (2, 1, 1), (2, 2, 1))
VROWS = HD + 16
PAD = 640


def remote(src, dst, send, recv, where):
    return pltpu.make_async_remote_copy(
        src_ref=src,
        dst_ref=dst,
        send_sem=send,
        recv_sem=recv,
        device_id=where,
        device_id_type=pl.DeviceIdType.MESH,
    )


def piece(part, sub, parts=PARTS):
    start, rows = parts[part]
    return pl.ds(start + sub * (rows // 2), rows // 2)


def block(
    step_hbm,
    group_hbm,
    length_hbm,
    x_hbm,
    text_hbm,
    wi_hbm,
    wt_hbm,
    wo_hbm,
    fw_hbm,
    qg_hbm,
    kg_hbm,
    mod_hbm,
    lat_hbm,
    old_hbm,
    noise_hbm,
    mean_ref,
    ratio_ref,
    step_ref,
    group_ref,
    length_ref,
    text_ref,
    wi,
    wt,
    wo,
    fw_ref,
    qg_ref,
    kg_ref,
    mod_ref,
    lat_ref,
    old_ref,
    noise_ref,
    xg,
    xe,
    modv,
    st_col,
    st_all,
    st_early,
    stat,
    stat_e,
    acc,
    acc_e,
    qall,
    kv,
    oacc,
    osend,
    orecv,
    atts,
    attb,
    pso,
    pdir,
    pacc,
    pown,
    ropp,
    rdir,
    racc,
    rat,
    w_sem,
    st_s,
    st_r,
    own_s,
    own_r,
    e_s,
    e_r,
    se_s,
    se_r,
    y_s,
    y_r,
    l_s,
    l_r,
    z_s,
    z_r,
    q_s,
    q_r,
    o_s,
    o_r,
    a_s,
    a_r,
    wo_s,
    wo_r,
    p_s,
    p_r,
    r_s,
    r_r,
):
    t = lax.axis_index("tensor")
    s = lax.axis_index("seq")
    y, c = lax.div(t, 2), lax.rem(t, 2)
    xlo, z = lax.div(s, RING), lax.rem(s, RING)
    yp, ym, yo = lax.rem(y + 1, RING), lax.rem(y + 3, RING), lax.rem(y + 2, RING)
    zp, zm, zo = lax.rem(z + 1, RING), lax.rem(z + 3, RING), lax.rem(z + 2, RING)
    mate = {"tensor": y * 2 + (1 - c)}
    y_dev = ({"tensor": yp * 2 + c}, {"tensor": ym * 2 + c})
    z_dev = ({"seq": xlo * RING + zp}, {"seq": xlo * RING + zm})
    x_dev = {"seq": (1 - xlo) * RING + z}
    cols = pl.ds(pl.multiple_of(c * FEAT, 128), FEAT)
    mate_cols = pl.ds(pl.multiple_of((1 - c) * FEAT, 128), FEAT)

    barrier = pltpu.get_barrier_semaphore()
    for j in range(1, 8):
        pl.semaphore_signal(
            barrier,
            inc=1,
            device_id={"tensor": lax.rem(t + j, 8)},
            device_id_type=pl.DeviceIdType.MESH,
        )
        pl.semaphore_signal(
            barrier,
            inc=1,
            device_id={"seq": lax.rem(s + j, 8)},
            device_id_type=pl.DeviceIdType.MESH,
        )

    def local(src, dst, k):
        copy = pltpu.make_async_copy(src, dst, w_sem.at[k])
        copy.start()
        return copy

    head_rows = pl.ds(0, HEAD_ROWS)
    rest_rows = pl.ds(HEAD_ROWS, IMG - HEAD_ROWS)
    moved_rows = pl.ds(HEAD_ROWS + TXT, IMG - HEAD_ROWS)
    x_load = local(x_hbm.at[0, head_rows], xg.at[y, head_rows, cols], 7)
    x_rest = local(x_hbm.at[0, rest_rows], xg.at[y, moved_rows, cols], 19)
    text_load = local(text_hbm, text_ref, 8)
    group_load = local(group_hbm, group_ref, 9)
    small = [
        local(step_hbm, step_ref, 10),
        local(length_hbm, length_ref, 11),
        local(mod_hbm, mod_ref, 12),
        local(qg_hbm, qg_ref, 13),
        local(kg_hbm, kg_ref, 14),
    ]
    loads = []
    for j in range(3):
        loads.append(local(wt_hbm.at[j], wt.at[:, pl.ds(j * FEAT, FEAT)], 3 + j))
        loads.append(local(wi_hbm.at[j], wi.at[:, pl.ds(j * FEAT, FEAT)], j))
    my_wo = wo.at[pl.ds(pl.multiple_of(c * FEAT, 128), FEAT)]
    late = [
        local(wo_hbm, my_wo, 6),
        local(fw_hbm, fw_ref, 15),
        local(lat_hbm.at[0], lat_ref, 16),
        local(old_hbm.at[0], old_ref, 17),
        local(noise_hbm.at[0], noise_ref, 18),
    ]

    text_load.wait()
    group_load.wait()
    group = group_ref[0]
    xg[y, pl.ds(HEAD_ROWS, TXT), cols] = text_ref[group]
    x_load.wait()
    x_rest.wait()

    def shard_stats(mine, pad):
        rows = mine.shape[0]
        part_mean = jnp.mean(mine, axis=-1, keepdims=True)
        centred = mine - part_mean
        part_sq = jnp.sum(centred * centred, axis=-1, keepdims=True)
        lane = lax.broadcasted_iota(jnp.int32, (rows, 128), 1)
        st_col[pl.ds(0, rows), :] = jnp.where(
            lane == 0, part_mean, jnp.where(lane == 1, part_sq, 0.0)
        )
        st_col[pl.ds(rows, pad - rows), :] = jnp.zeros((pad - rows, 128), F32)
        return st_col[pl.ds(0, pad), :].T[0:2, :]

    st_all[t] = shard_stats(xg[y, :, cols].astype(F32), PAD)

    pl.semaphore_wait(barrier, 14)

    def peer_copy(buf, send, recv, axis, me, j):
        slot = buf.at[me]
        return remote(slot, slot, send.at[j], recv.at[j], {axis: lax.rem(me + j, 8)})

    def peer_arrival(buf, send, recv, axis, me, j):
        slot = buf.at[lax.rem(me + 8 - j, 8)]
        return remote(slot, slot, send.at[j], recv.at[j], {axis: lax.rem(me + j, 8)})

    def y_slot(d, k, sending):
        if k < 2:
            return (y if sending else (ym, yp)[d]), (k if d == 0 else 1 - k)
        return ((ym, yp)[d] if sending else yo), d

    def held(slot, part, sub, columns):
        if part < 3:
            return xg.at[slot, piece(part, sub), columns]
        return xe.at[slot, piece(part - 3, sub, EPARTS), columns]

    def y_send(d, part, k):
        slot, sub = y_slot(d, k, True)
        ref = held(slot, part, sub, cols)
        return remote(ref, ref, y_s.at[d, part, k], y_r.at[d, part, k], y_dev[d])

    def y_arrival(d, part, k):
        slot, sub = y_slot(d, k, False)
        ref = held(slot, part, sub, cols)
        return remote(ref, ref, y_s.at[d, part, k], y_r.at[d, part, k], y_dev[d])

    def relay(d, part, k):
        slot, sub = y_slot(d, k, False)
        ref = held(slot, part, sub, cols)
        return remote(ref, ref, l_s.at[d, part, k], l_r.at[d, part, k], mate)

    def relay_arrival(d, part, k):
        slot, sub = y_slot(d, k, False)
        ref = held(slot, part, sub, mate_cols)
        return remote(ref, ref, l_s.at[d, part, k], l_r.at[d, part, k], mate)

    def own_copy(columns):
        ref = xg.at[y, :, columns]
        return remote(ref, ref, own_s.at[0], own_r.at[0], mate)

    sends = []

    def go(copy):
        copy.start()
        sends.append(copy)

    def y_own(part, pieces=(0, 1)):
        for k in pieces:
            for d in range(2):
                go(y_send(d, part, k))

    for j in range(1, 8):
        go(peer_copy(st_all, st_s, st_r, "tensor", t, j))
    y_own(0)

    def early_copy(k):
        to = (zp, zm, zo)[k]
        return remote(
            xg.at[y, pl.ds(EARLY_AT, EARLY), cols],
            xe.at[y, pl.ds(k * EARLY, EARLY), cols],
            e_s.at[k],
            e_r.at[k],
            {"seq": xlo * RING + to},
        )

    def early_mate(columns):
        ref = xe.at[y, :, columns]
        return remote(ref, ref, e_s.at[3], e_r.at[3], mate)

    for k in range(3):
        go(early_copy(k))
    go(own_copy(cols))

    def y_first(part):
        for d in range(2):
            y_arrival(d, part, 0).wait_recv()
            go(y_send(d, part, 2))
            go(relay(d, part, 0))

    def y_relay(part, k):
        for d in range(2):
            y_arrival(d, part, k).wait_recv()
            go(relay(d, part, k))

    def y_ready(part, k):
        for d in range(2):
            relay_arrival(d, part, k).wait_recv()

    for copy in small:
        copy.wait()
    step = step_ref[0]
    for i in range(RING):
        modv[i, pl.ds(0, 7), :] = mod_ref[step, :, pl.ds(i * PAIR, PAIR)]

    y_first(0)
    y_own(1)
    y_relay(0, 1)

    def token_stats(buf, pad):
        means = buf[:, 0, :]
        squares = buf[:, 1, :]
        mean = jnp.mean(means, axis=0, keepdims=True)
        off = means - mean
        total_sq = jnp.sum(squares, axis=0, keepdims=True) + FEAT * jnp.sum(
            off * off, axis=0, keepdims=True
        )
        scale = lax.rsqrt(total_sq * (1.0 / WIDTH) + NORM_EPSILON)
        sub_row = lax.broadcasted_iota(jnp.int32, (128, pad), 0)
        return jnp.where(sub_row == 0, mean, jnp.where(sub_row == 1, scale, 0.0)).T

    for j in range(1, 8):
        peer_arrival(st_all, st_s, st_r, "tensor", t, j).wait_recv()
    stat[...] = token_stats(st_all, PAD)

    for copy in loads:
        copy.wait()

    def project_rows(slot, start, rows, weight, shift_row, scale_row, first):
        at = pl.ds(start, rows)
        v = xg[slot, at, :].astype(F32)
        n = (v - stat[at, 0:1]) * stat[at, 1:2]
        n = n * (1.0 + modv[slot, pl.ds(scale_row, 1), :]) + modv[slot, pl.ds(shift_row, 1), :]
        w = weight[pl.ds(pl.multiple_of(slot * PAIR, 128), PAIR), :]
        p = jnp.dot(n.astype(BF16), w, preferred_element_type=F32)
        if first:
            acc[at, :] = p
        else:
            acc[at, :] += p

    def project(slot, part, first=False):
        start, rows = PARTS[part]
        if part == 1:
            project_rows(slot, start + TXT, rows - TXT, wi, 0, 1, first)
            project_rows(slot, start, TXT, wt, 3, 4, first)
        else:
            project_rows(slot, start, rows, wi, 0, 1, first)

    def project_early(slot, first=False):
        at = pl.ds(*EPARTS[0])
        n = (xe[slot, at, :].astype(F32) - stat_e[at, 0:1]) * stat_e[at, 1:2]
        n = n * (1.0 + modv[slot, pl.ds(1, 1), :]) + modv[slot, pl.ds(0, 1), :]
        w = wi[pl.ds(pl.multiple_of(slot * PAIR, 128), PAIR), pl.ds(FEAT, 2 * FEAT)]
        p = jnp.dot(n.astype(BF16), w, preferred_element_type=F32)
        if first:
            acc_e[at, :] = p
        else:
            acc_e[at, :] += p

    score_scale = math.log2(math.e) / math.sqrt(HD)

    def head_norm(values, gain):
        square = jnp.mean(values * values, axis=-1, keepdims=True)
        return (values * lax.rsqrt(square + NORM_EPSILON) * gain).astype(BF16)

    def q_rows(part):
        start, rows = PARTS[part]
        if part == 0:
            return start, start, rows
        skip = TXT if part == 1 else 0
        return start + skip, start + skip - TXT, rows - skip

    def finish(part):
        at = pl.ds(*PARTS[part])
        for h in range(HEADS):
            keys = acc[at, pl.ds(FEAT + h * HD, HD)]
            kv[z, at, pl.ds(2 * h * HD, HD)] = head_norm(keys, kg_ref[...])
            vals = acc[at, pl.ds(2 * FEAT + h * HD, HD)]
            kv[z, at, pl.ds((2 * h + 1) * HD, HD)] = vals.astype(BF16)
        token, query, rows = q_rows(part)
        for h in range(HEADS):
            q = acc[pl.ds(token, rows), pl.ds(h * HD, HD)]
            qall[0, pl.ds(query, rows), pl.ds(h * HD, HD)] = head_norm(
                q, qg_ref[...] * score_scale
            )

    def finish_early(k):
        slot = (zm, zp, zo)[k]
        at = pl.ds(k * EARLY, EARLY)
        to = pl.ds(EARLY_AT, EARLY)
        for h in range(HEADS):
            keys = acc_e[at, pl.ds(h * HD, HD)]
            kv[slot, to, pl.ds(2 * h * HD, HD)] = head_norm(keys, kg_ref[...])
            kv[slot, to, pl.ds((2 * h + 1) * HD, HD)] = acc_e[at, pl.ds(FEAT + h * HD, HD)].astype(BF16)

    def z_slot(d, k, sending):
        if k < 2:
            return (z if sending else (zm, zp)[d]), (k if d == 0 else 1 - k)
        return ((zm, zp)[d] if sending else zo), d

    def z_copy(d, g, k, sending):
        slot, sub = z_slot(d, k, sending)
        part, h, heads = GROUPS[g]
        ref = kv.at[slot, piece(part, sub, ZPARTS), pl.ds(2 * h * HD, 2 * heads * HD)]
        return remote(ref, ref, z_s.at[d, g, k], z_r.at[d, g, k], z_dev[d])

    def q_copy(part):
        _, query, rows = q_rows(part)
        at = pl.ds(query, rows)
        return remote(qall.at[0, at], qall.at[1, at], q_s.at[part], q_r.at[part], x_dev)

    def z_own(g, pieces=(0, 1)):
        for k in pieces:
            for d in range(2):
                go(z_copy(d, g, k, True))

    def z_first(g):
        for d in range(2):
            z_copy(d, g, 0, False).wait_recv()
            go(z_copy(d, g, 2, True))

    def z_wait(g, k):
        for d in range(2):
            z_copy(d, g, k, False).wait_recv()

    own_copy(mate_cols).wait_recv()
    project(y, 0, first=True)
    y_ready(0, 0)
    y_ready(0, 1)
    project(ym, 0)
    project(yp, 0)
    y_relay(0, 2)
    y_ready(0, 2)
    project(yo, 0)
    finish(0)
    z_own(0)
    go(q_copy(0))

    y_first(1)
    y_own(2)
    for k in range(3):
        early_copy(k).wait_recv()
    go(early_mate(cols))
    st_early[t] = shard_stats(xe[y, :, cols].astype(F32), EPAD)
    for j in range(1, 8):
        go(peer_copy(st_early, se_s, se_r, "tensor", t, j))
    project(y, 1, first=True)
    y_relay(1, 1)
    y_ready(1, 0)
    y_ready(1, 1)
    project(ym, 1)
    project(yp, 1)
    z_first(0)
    y_relay(1, 2)
    project(y, 2, first=True)
    y_ready(1, 2)
    project(yo, 1)
    finish(1)
    z_own(1)
    go(q_copy(1))

    y_first(2)
    y_own(3)
    y_relay(2, 1)
    y_ready(2, 0)
    y_ready(2, 1)
    project(ym, 2)
    project(yp, 2)
    z_first(1)
    y_relay(2, 2)
    for j in range(1, 8):
        peer_arrival(st_early, se_s, se_r, "tensor", t, j).wait_recv()
    stat_e[...] = token_stats(st_early, EPAD)
    early_mate(mate_cols).wait_recv()
    project_early(y, first=True)
    y_first(3)
    y_ready(2, 2)
    project(yo, 2)
    finish(2)
    z_own(2)
    z_own(3)
    z_own(4, (0,))
    go(q_copy(2))

    for copy in late:
        copy.wait()
    wo_send = remote(my_wo, my_wo, wo_s.at[0], wo_r.at[0], mate)
    go(wo_send)

    length = length_ref[group]

    def values(slot, start, rows, h):
        at = pl.ds(start, rows)
        vals = kv[slot, at, pl.ds((2 * h + 1) * HD, HD)].astype(F32).T
        ones = jnp.ones((VROWS - HD, rows), F32)
        if start <= HEAD_ROWS:
            pos = start - HEAD_ROWS + lax.broadcasted_iota(jnp.int32, (1, rows), 1)
            used = (pos < 0) | (pos >= TXT) | (pos + (xlo * RING + slot) * TXT < length)
            vals = jnp.where(used, vals, 0.0)
            ones = jnp.where(used, ones, 0.0)
        return jnp.concatenate([vals, ones], axis=0).astype(BF16)

    def weighted(slot, start, rows, h, ext, q, at_q):
        scores = lax.dot_general(
            kv[slot, pl.ds(start, rows), pl.ds(2 * h * HD, HD)],
            qall[q, at_q, pl.ds(h * HD, HD)],
            (((1,), (1,)), ((), ())),
            preferred_element_type=F32,
        )
        return jnp.dot(ext, jnp.exp2(scores).astype(BF16), preferred_element_type=F32)

    def attend(slot, h, sets, start=0, rows=TOK, first=False):
        ext = values(slot, start, rows, h)
        for q in sets:
            o = weighted(slot, start, rows, h, ext, q, pl.ds(0, IMG))
            if first:
                oacc[q, h] = o
            else:
                oacc[q, h] += o

    order = (yo, yp, ym, y)

    def lanes(i):
        return pl.ds(pl.multiple_of(i * 128, 128), 128)

    def o_copy(h, j):
        at = lanes(order[j])
        k = h * RING + j
        return remote(osend.at[h, :, at], orecv.at[h, :, at], o_s.at[k], o_r.at[k], x_dev)

    def pack(o, h, at):
        den = o[HD : HD + 1]
        high = den.astype(BF16).astype(F32)
        middle = (den - high).astype(BF16).astype(F32)
        low = den - high - middle
        osend[h, pl.ds(0, HD), at] = o[:HD].astype(BF16)
        pad = jnp.zeros((VROWS - HD - 3, den.shape[1]), F32)
        osend[h, pl.ds(HD, VROWS - HD), at] = jnp.concatenate(
            [high, middle, low, pad], axis=0
        ).astype(BF16)

    whole = pl.ds(0, IMG)

    for h in range(HEADS):
        attend(z, h, (0,), first=True)
    y_relay(3, 1)
    z_wait(0, 1)
    z_wait(0, 2)
    z_wait(1, 1)
    for h in range(HEADS):
        attend(zm, h, (0,), 0, EARLY_AT)
        attend(zp, h, (0,), 0, EARLY_AT)
    z_wait(1, 2)
    for h in range(HEADS):
        attend(zo, h, (0,), 0, EARLY_AT)
    z_first(2)
    z_own(4, (1,))
    y_ready(3, 0)
    y_ready(3, 1)
    project_early(ym)
    project_early(yp)
    y_relay(3, 2)
    for part in range(3):
        q_copy(part).wait_recv()
    for h in range(HEADS):
        attend(z, h, (1,), first=True)
        if h == 1:
            z_first(3)
    y_ready(3, 2)
    project_early(yo)
    for k in range(3):
        finish_early(k)
    z_wait(2, 1)
    attend(zm, 0, (1,))
    attend(zp, 0, (1,))
    z_first(4)
    z_wait(3, 1)
    attend(zm, 1, (1,))
    attend(zp, 1, (1,))
    z_wait(2, 2)
    attend(zo, 0, (1,))
    pack(oacc[1, 0], 0, whole)
    for j in range(3):
        go(o_copy(0, j))
    z_wait(3, 2)
    attend(zo, 1, (1,))
    pack(oacc[1, 1], 1, whole)
    for j in range(2):
        go(o_copy(1, j))
    z_wait(4, 1)
    attend(zm, 2, (1,))
    attend(zp, 2, (1,))
    attend(zo, 2, (1,), 0, LATE_AT)
    z_wait(4, 2)

    last = values(zo, *ZPARTS[2], 2)
    for j in range(RING):
        at = lanes(order[j])
        pack(oacc[1, 2, :, at] + weighted(zo, *ZPARTS[2], 2, last, 1, at), 2, at)
        go(o_copy(2, j))
        if j == 1:
            go(o_copy(1, 2))
        if j == 2:
            go(o_copy(0, 3))
            go(o_copy(1, 3))
    for h in range(HEADS):
        for slot in (zm, zp, zo):
            attend(slot, h, (0,), EARLY_AT, TOK - EARLY_AT)

    def a_copy(j, columns):
        return remote(
            atts.at[j, pl.ds(pl.multiple_of((1 - c) * CH, CH), CH)],
            attb.at[j, :, columns],
            a_s.at[j],
            a_r.at[j],
            mate,
        )

    def combine(j):
        at = lanes(order[j])
        for h in range(HEADS):
            o_copy(h, j).wait_recv()
        heads = []
        for h in range(HEADS):
            tail = orecv[h, pl.ds(HD, VROWS - HD), at].astype(F32)
            num = oacc[0, h, pl.ds(0, HD), at] + orecv[h, pl.ds(0, HD), at].astype(F32)
            den = oacc[0, h, pl.ds(HD, 1), at] + (tail[0:1] + tail[1:2] + tail[2:3])
            heads.append((num / den).T)
        atts[j] = jnp.concatenate(heads, axis=1).astype(BF16)
        go(a_copy(j, cols))
        attb[j, :, cols] = atts[j, pl.ds(pl.multiple_of(c * CH, CH), CH), :]

    half = WIDTH // 2
    sides = (pl.ds(0, half), pl.ds(half, half))

    def p_copy(d, k):
        src = (pso.at[d], pdir.at[d], pacc.at[d])[k]
        dst = (ropp.at[d], rdir.at[d], racc.at[d])[k]
        return remote(src, dst, p_s.at[d, k], p_r.at[d, k], y_dev[d])

    def out_side(j, d):
        return jnp.dot(attb[j], wo[:, sides[d]], preferred_element_type=F32)

    def dispatch(j):
        a_copy(j, mate_cols).wait_recv()
        if j == 0:
            for d in range(2):
                pso[d] = out_side(0, d).astype(BF16)
                go(p_copy(d, 0))
        else:
            keep, direct = j - 1, 2 - j
            pdir[keep] = out_side(j, direct).astype(BF16)
            go(p_copy(keep, 1))
            pown[:, sides[keep]] = out_side(j, keep)

    remote(my_wo, wo.at[pl.ds(pl.multiple_of((1 - c) * FEAT, 128), FEAT)], wo_s.at[0], wo_r.at[0], mate).wait_recv()
    for j in range(3):
        combine(j)
        dispatch(j)
    for d in range(2):
        p_copy(d, 0).wait_recv()
        pacc[d] = (pown[:, sides[d]] + ropp[d].astype(F32)).astype(BF16)
        go(p_copy(d, 2))
    combine(3)
    a_copy(3, mate_cols).wait_recv()
    mine = [out_side(3, d) for d in range(2)]
    for d in range(2):
        p_copy(1 - d, 1).wait_recv()
        pown[:, sides[d]] = mine[d] + rdir[1 - d].astype(F32)
    for d in range(2):
        p_copy(d, 2).wait_recv()
        pown[:, sides[d]] += racc[d].astype(F32)

    row = t * CH + TXT * lax.min(lax.div(t * CH, HEAD_ROWS), 1)
    rows = pl.ds(pl.multiple_of(row, CH), CH)
    resid = jnp.concatenate(
        [
            xg[i, rows, :].astype(F32)
            + modv[i, pl.ds(2, 1), :] * pown[:, pl.ds(i * PAIR, PAIR)]
            for i in range(RING)
        ],
        axis=1,
    )
    row_mean = jnp.mean(resid, axis=-1, keepdims=True)
    resid = resid - row_mean
    row_var = jnp.mean(resid * resid, axis=-1, keepdims=True)
    resid = resid * lax.rsqrt(row_var + NORM_EPSILON)
    velocity = jnp.zeros((CH, CH), F32)
    for i in range(RING):
        n = resid[:, i * PAIR : (i + 1) * PAIR] * (1.0 + modv[i, pl.ds(6, 1), :]) + modv[
            i, pl.ds(5, 1), :
        ]
        velocity += lax.dot_general(
            n.astype(BF16),
            fw_ref[:, pl.ds(i * PAIR, PAIR)],
            (((1,), (1,)), ((), ())),
            preferred_element_type=F32,
        )

    total_steps = mod_ref.shape[0]
    count = total_steps + 1.0
    step_delta = -1.0 / count
    flow = (total_steps - jnp.full((1, CH), step, jnp.int32).astype(F32)) / count
    sigma = NOISE_LEVEL * jnp.sqrt(flow / (1.0 - flow))
    spread = sigma * math.sqrt(1.0 / count)
    pull = sigma * sigma / (2.0 * flow)

    def drift(state, v):
        return state + (v + pull * (state + (1.0 - flow) * v)) * step_delta

    latent = lat_ref[...]
    noise = noise_ref[...]
    step_mean = drift(latent, velocity)
    mean_ref[0] = step_mean
    shifted = noise + (drift(latent, old_ref[...].astype(F32)) - step_mean) / spread
    gap = noise * noise - shifted * shifted
    gap = jnp.sum(jnp.sum(gap, axis=1, keepdims=True), axis=0, keepdims=True) * 0.5
    me = s * 8 + t
    rat[me] = jnp.broadcast_to(gap, (1, 128))

    def spot(step, here):
        return lax.rem(here + step, RING)

    seqs = [(1 - xlo if a else xlo) * RING + spot(b, z) for a in range(2) for b in range(RING)]
    tens = [spot(b, y) * 2 + (1 - c if a else c) for a in range(2) for b in range(RING)]
    hops = (0, 1, 2, 1, 1, 2, 3, 2)
    pairs = [(i, j) for i in range(8) for j in range(8) if i or j]
    for i, j in sorted(pairs, key=lambda p: -hops[p[0]] - hops[p[1]]):
        where = {"seq": seqs[i], "tensor": tens[j]}
        remote(rat.at[me], rat.at[me], r_s.at[0], r_r.at[0], where).start()
    told = rat.at[pl.ds(0, 63)]
    everyone = remote(told, told, r_s.at[0], r_r.at[0], mate)
    everyone.wait_recv()
    elements = 64 * CH * CH
    ratio = jnp.sum(rat[...], axis=0) / elements
    ratio_ref[0] = ratio[0, 0]
    everyone.wait_send()
    for copy in sends:
        copy.wait_send()


def shards(
    image_states,
    text_states,
    image_qkv,
    text_qkv,
    image_out,
    final_weight,
    query_gain,
    key_gain,
    modulation,
    latent,
    old_velocity,
    rollout_noise,
    group_ids,
    text_lengths,
    step_ids,
):
    smem = pl.BlockSpec(memory_space=pltpu.SMEM)
    vmem = pl.BlockSpec(memory_space=pltpu.VMEM)
    hbm = pl.BlockSpec(memory_space=pl.ANY)
    dma = pltpu.SemaphoreType.DMA
    half = WIDTH // 2
    return pl.pallas_call(
        block,
        out_shape=(
            pltpu.VMEM(latent.shape, F32),
            pltpu.SMEM((1,), F32),
        ),
        in_specs=[hbm] * 15,
        out_specs=(vmem, smem),
        scratch_shapes=[
            pltpu.SMEM((1,), jnp.int32),
            pltpu.SMEM((1,), jnp.int32),
            pltpu.SMEM((4,), jnp.int32),
            pltpu.VMEM(text_states.shape, BF16),
            pltpu.VMEM((WIDTH, 3 * FEAT), BF16),
            pltpu.VMEM((WIDTH, 3 * FEAT), BF16),
            pltpu.VMEM((PAIR, WIDTH), BF16),
            pltpu.VMEM((CH, WIDTH), BF16),
            pltpu.VMEM((1, HD), F32),
            pltpu.VMEM((1, HD), F32),
            pltpu.VMEM(modulation.shape, F32),
            pltpu.VMEM((CH, CH), F32),
            pltpu.VMEM((CH, CH), BF16),
            pltpu.VMEM((CH, CH), F32),
            pltpu.VMEM((RING, TOK, PAIR), BF16),
            pltpu.VMEM((RING, 3 * EARLY, PAIR), BF16),
            pltpu.VMEM((RING, 8, PAIR), F32),
            pltpu.VMEM((PAD, 128), F32),
            pltpu.VMEM((8, 2, PAD), F32),
            pltpu.VMEM((8, 2, EPAD), F32),
            pltpu.VMEM((PAD, 128), F32),
            pltpu.VMEM((EPAD, 128), F32),
            pltpu.VMEM((TOK, 3 * FEAT), F32),
            pltpu.VMEM((3 * EARLY, 2 * FEAT), F32),
            pltpu.VMEM((2, IMG, FEAT), BF16),
            pltpu.VMEM((RING, TOK, PAIR), BF16),
            pltpu.VMEM((2, HEADS, VROWS, IMG), F32),
            pltpu.VMEM((HEADS, VROWS, IMG), BF16),
            pltpu.VMEM((HEADS, VROWS, IMG), BF16),
            pltpu.VMEM((RING, 128, FEAT), BF16),
            pltpu.VMEM((RING, CH, PAIR), BF16),
            pltpu.VMEM((2, CH, half), BF16),
            pltpu.VMEM((2, CH, half), BF16),
            pltpu.VMEM((2, CH, half), BF16),
            pltpu.VMEM((CH, WIDTH), F32),
            pltpu.VMEM((2, CH, half), BF16),
            pltpu.VMEM((2, CH, half), BF16),
            pltpu.VMEM((2, CH, half), BF16),
            pltpu.VMEM((64, 1, 128), F32),
            dma((20,)),
            dma((8,)),
            dma((8,)),
            dma((1,)),
            dma((1,)),
            dma((4,)),
            dma((4,)),
            dma((8,)),
            dma((8,)),
            dma((2, 4, 3)),
            dma((2, 4, 3)),
            dma((2, 4, 3)),
            dma((2, 4, 3)),
            dma((2, 5, 3)),
            dma((2, 5, 3)),
            dma((3,)),
            dma((3,)),
            dma((12,)),
            dma((12,)),
            dma((RING,)),
            dma((RING,)),
            dma((1,)),
            dma((1,)),
            dma((2, 3)),
            dma((2, 3)),
            dma((1,)),
            dma((1,)),
        ],
        compiler_params=pltpu.CompilerParams(
            collective_id=0, has_side_effects=True, vmem_limit_bytes=62 * 1024 * 1024
        ),
    )(
        step_ids,
        group_ids,
        text_lengths,
        image_states,
        text_states,
        jnp.transpose(image_qkv, (1, 0, 2)),
        jnp.transpose(text_qkv, (1, 0, 2)),
        image_out,
        final_weight.T,
        query_gain.reshape(1, HD),
        key_gain.reshape(1, HD),
        modulation,
        latent,
        old_velocity,
        rollout_noise,
    )


def solution(mesh):
    placed = (
        P("dp", "seq", "tensor"),
        P(None, "seq", "tensor"),
        P(None, None, "tensor"),
        P(None, None, "tensor"),
        P("tensor", None),
        P(),
        P(),
        P(),
        P(),
        P("dp", ("seq", "tensor"), None),
        P("dp", ("seq", "tensor"), None),
        P("dp", ("seq", "tensor"), None),
        P("dp"),
        P(),
        P("dp"),
    )
    return jax.shard_map(
        shards,
        mesh=mesh,
        in_specs=placed,
        out_specs=(P("dp", ("seq", "tensor"), None), P("dp")),
        check_vma=False,
    )
```

```python
import functools
import math

import jax
import jax.numpy as jnp
from jax import lax
from jax.experimental import pallas as pl
from jax.experimental.pallas import tpu as pltpu
from jax.sharding import PartitionSpec as P

NORM_EPSILON = 1e-06
NOISE_LEVEL = 0.7
F32 = jnp.float32
BF16 = jnp.bfloat16

TXT, IMG, TOK = 64, 512, 576
FEAT, PAIR, WIDTH = 384, 768, 3072
HEADS, HD = 3, 128
CH = 64
RING = 4
HEAD_ROWS = 128
PARTS = ((0, 128), (128, 192), (320, 256))
EARLY = 64
EARLY_AT = 320
LATE_AT = EARLY_AT + EARLY
EPARTS = ((0, 3 * EARLY),)
ZPARTS = ((0, 128), (128, 192), (LATE_AT, TOK - LATE_AT))
EPAD = 256
GROUPS = ((0, 0, 3), (1, 0, 3), (2, 0, 1), (2, 1, 1), (2, 2, 1))
VROWS = HD + 16
PAD = 640


def remote(src, dst, send, recv, where):
    return pltpu.make_async_remote_copy(
        src_ref=src,
        dst_ref=dst,
        send_sem=send,
        recv_sem=recv,
        device_id=where,
        device_id_type=pl.DeviceIdType.MESH,
    )


def piece(part, sub, parts=PARTS):
    start, rows = parts[part]
    return pl.ds(start + sub * (rows // 2), rows // 2)


def block(
    step_hbm,
    group_hbm,
    length_hbm,
    x_hbm,
    text_hbm,
    wi_hbm,
    wt_hbm,
    wo_hbm,
    fw_hbm,
    qg_hbm,
    kg_hbm,
    mod_hbm,
    lat_hbm,
    old_hbm,
    noise_hbm,
    mean_ref,
    ratio_ref,
    step_ref,
    group_ref,
    length_ref,
    text_ref,
    wi,
    wt,
    wo,
    fw_ref,
    qg_ref,
    kg_ref,
    mod_ref,
    lat_ref,
    old_ref,
    noise_ref,
    xg,
    xe,
    modv,
    st_col,
    st_all,
    st_early,
    stat,
    stat_e,
    acc,
    acc_e,
    qall,
    kv,
    oacc,
    osend,
    orecv,
    atts,
    attb,
    pso,
    pdir,
    pacc,
    pown,
    ropp,
    rdir,
    racc,
    rat,
    w_sem,
    st_s,
    st_r,
    own_s,
    own_r,
    e_s,
    e_r,
    se_s,
    se_r,
    y_s,
    y_r,
    l_s,
    l_r,
    z_s,
    z_r,
    q_s,
    q_r,
    o_s,
    o_r,
    a_s,
    a_r,
    wo_s,
    wo_r,
    p_s,
    p_r,
    r_s,
    r_r,
):
    t = lax.axis_index("tensor")
    s = lax.axis_index("seq")
    y, c = lax.div(t, 2), lax.rem(t, 2)
    xlo, z = lax.div(s, RING), lax.rem(s, RING)
    yp, ym, yo = lax.rem(y + 1, RING), lax.rem(y + 3, RING), lax.rem(y + 2, RING)
    zp, zm, zo = lax.rem(z + 1, RING), lax.rem(z + 3, RING), lax.rem(z + 2, RING)
    mate = {"tensor": y * 2 + (1 - c)}
    y_dev = ({"tensor": yp * 2 + c}, {"tensor": ym * 2 + c})
    z_dev = ({"seq": xlo * RING + zp}, {"seq": xlo * RING + zm})
    x_dev = {"seq": (1 - xlo) * RING + z}
    cols = pl.ds(pl.multiple_of(c * FEAT, 128), FEAT)
    mate_cols = pl.ds(pl.multiple_of((1 - c) * FEAT, 128), FEAT)

    barrier = pltpu.get_barrier_semaphore()
    for j in range(1, 8):
        pl.semaphore_signal(
            barrier,
            inc=1,
            device_id={"tensor": lax.rem(t + j, 8)},
            device_id_type=pl.DeviceIdType.MESH,
        )
        pl.semaphore_signal(
            barrier,
            inc=1,
            device_id={"seq": lax.rem(s + j, 8)},
            device_id_type=pl.DeviceIdType.MESH,
        )

    def local(src, dst, k):
        copy = pltpu.make_async_copy(src, dst, w_sem.at[k])
        copy.start()
        return copy

    head_rows = pl.ds(0, HEAD_ROWS)
    rest_rows = pl.ds(HEAD_ROWS, IMG - HEAD_ROWS)
    moved_rows = pl.ds(HEAD_ROWS + TXT, IMG - HEAD_ROWS)
    x_load = local(x_hbm.at[0, head_rows], xg.at[y, head_rows, cols], 7)
    x_rest = local(x_hbm.at[0, rest_rows], xg.at[y, moved_rows, cols], 19)
    text_load = local(text_hbm, text_ref, 8)
    group_load = local(group_hbm, group_ref, 9)
    small = [
        local(step_hbm, step_ref, 10),
        local(length_hbm, length_ref, 11),
        local(mod_hbm, mod_ref, 12),
        local(qg_hbm, qg_ref, 13),
        local(kg_hbm, kg_ref, 14),
    ]
    loads = []
    for j in range(3):
        loads.append(local(wt_hbm.at[j], wt.at[:, pl.ds(j * FEAT, FEAT)], 3 + j))
        loads.append(local(wi_hbm.at[j], wi.at[:, pl.ds(j * FEAT, FEAT)], j))
    my_wo = wo.at[pl.ds(pl.multiple_of(c * FEAT, 128), FEAT)]
    late = [
        local(wo_hbm, my_wo, 6),
        local(fw_hbm, fw_ref, 15),
        local(lat_hbm.at[0], lat_ref, 16),
        local(old_hbm.at[0], old_ref, 17),
        local(noise_hbm.at[0], noise_ref, 18),
    ]

    text_load.wait()
    group_load.wait()
    group = group_ref[0]
    xg[y, pl.ds(HEAD_ROWS, TXT), cols] = text_ref[group]
    x_load.wait()
    x_rest.wait()

    def shard_stats(mine, pad):
        rows = mine.shape[0]
        part_mean = jnp.mean(mine, axis=-1, keepdims=True)
        centred = mine - part_mean
        part_sq = jnp.sum(centred * centred, axis=-1, keepdims=True)
        lane = lax.broadcasted_iota(jnp.int32, (rows, 128), 1)
        st_col[pl.ds(0, rows), :] = jnp.where(
            lane == 0, part_mean, jnp.where(lane == 1, part_sq, 0.0)
        )
        st_col[pl.ds(rows, pad - rows), :] = jnp.zeros((pad - rows, 128), F32)
        return st_col[pl.ds(0, pad), :].T[0:2, :]

    st_all[t] = shard_stats(xg[y, :, cols].astype(F32), PAD)

    pl.semaphore_wait(barrier, 14)

    def peer_copy(buf, send, recv, axis, me, j):
        slot = buf.at[me]
        return remote(slot, slot, send.at[j], recv.at[j], {axis: lax.rem(me + j, 8)})

    def peer_arrival(buf, send, recv, axis, me, j):
        slot = buf.at[lax.rem(me + 8 - j, 8)]
        return remote(slot, slot, send.at[j], recv.at[j], {axis: lax.rem(me + j, 8)})

    def y_slot(d, k, sending):
        if k < 2:
            return (y if sending else (ym, yp)[d]), (k if d == 0 else 1 - k)
        return ((ym, yp)[d] if sending else yo), d

    def held(slot, part, sub, columns):
        if part < 3:
            return xg.at[slot, piece(part, sub), columns]
        return xe.at[slot, piece(part - 3, sub, EPARTS), columns]

    def y_send(d, part, k):
        slot, sub = y_slot(d, k, True)
        ref = held(slot, part, sub, cols)
        return remote(ref, ref, y_s.at[d, part, k], y_r.at[d, part, k], y_dev[d])

    def y_arrival(d, part, k):
        slot, sub = y_slot(d, k, False)
        ref = held(slot, part, sub, cols)
        return remote(ref, ref, y_s.at[d, part, k], y_r.at[d, part, k], y_dev[d])

    def relay(d, part, k):
        slot, sub = y_slot(d, k, False)
        ref = held(slot, part, sub, cols)
        return remote(ref, ref, l_s.at[d, part, k], l_r.at[d, part, k], mate)

    def relay_arrival(d, part, k):
        slot, sub = y_slot(d, k, False)
        ref = held(slot, part, sub, mate_cols)
        return remote(ref, ref, l_s.at[d, part, k], l_r.at[d, part, k], mate)

    def own_copy(columns):
        ref = xg.at[y, :, columns]
        return remote(ref, ref, own_s.at[0], own_r.at[0], mate)

    sends = []

    def go(copy):
        copy.start()
        sends.append(copy)

    def y_own(part, pieces=(0, 1)):
        for k in pieces:
            for d in range(2):
                go(y_send(d, part, k))

    for j in range(1, 8):
        go(peer_copy(st_all, st_s, st_r, "tensor", t, j))
    y_own(0)

    def early_copy(k):
        to = (zp, zm, zo)[k]
        return remote(
            xg.at[y, pl.ds(EARLY_AT, EARLY), cols],
            xe.at[y, pl.ds(k * EARLY, EARLY), cols],
            e_s.at[k],
            e_r.at[k],
            {"seq": xlo * RING + to},
        )

    def early_mate(columns):
        ref = xe.at[y, :, columns]
        return remote(ref, ref, e_s.at[3], e_r.at[3], mate)

    for k in range(3):
        go(early_copy(k))
    go(own_copy(cols))

    def y_first(part):
        for d in range(2):
            y_arrival(d, part, 0).wait_recv()
            go(y_send(d, part, 2))
            go(relay(d, part, 0))

    def y_relay(part, k):
        for d in range(2):
            y_arrival(d, part, k).wait_recv()
            go(relay(d, part, k))

    def y_ready(part, k):
        for d in range(2):
            relay_arrival(d, part, k).wait_recv()

    for copy in small:
        copy.wait()
    step = step_ref[0]
    for i in range(RING):
        modv[i, pl.ds(0, 7), :] = mod_ref[step, :, pl.ds(i * PAIR, PAIR)]

    y_first(0)
    y_own(1)
    y_relay(0, 1)

    def token_stats(buf, pad):
        means = buf[:, 0, :]
        squares = buf[:, 1, :]
        mean = jnp.mean(means, axis=0, keepdims=True)
        off = means - mean
        total_sq = jnp.sum(squares, axis=0, keepdims=True) + FEAT * jnp.sum(
            off * off, axis=0, keepdims=True
        )
        scale = lax.rsqrt(total_sq * (1.0 / WIDTH) + NORM_EPSILON)
        sub_row = lax.broadcasted_iota(jnp.int32, (128, pad), 0)
        return jnp.where(sub_row == 0, mean, jnp.where(sub_row == 1, scale, 0.0)).T

    for j in range(1, 8):
        peer_arrival(st_all, st_s, st_r, "tensor", t, j).wait_recv()
    stat[...] = token_stats(st_all, PAD)

    for copy in loads:
        copy.wait()

    def project_rows(slot, start, rows, weight, shift_row, scale_row, first):
        at = pl.ds(start, rows)
        v = xg[slot, at, :].astype(F32)
        n = (v - stat[at, 0:1]) * stat[at, 1:2]
        n = n * (1.0 + modv[slot, pl.ds(scale_row, 1), :]) + modv[slot, pl.ds(shift_row, 1), :]
        w = weight[pl.ds(pl.multiple_of(slot * PAIR, 128), PAIR), :]
        p = jnp.dot(n.astype(BF16), w, preferred_element_type=F32)
        if first:
            acc[at, :] = p
        else:
            acc[at, :] += p

    def project(slot, part, first=False):
        start, rows = PARTS[part]
        if part == 1:
            project_rows(slot, start + TXT, rows - TXT, wi, 0, 1, first)
            project_rows(slot, start, TXT, wt, 3, 4, first)
        else:
            project_rows(slot, start, rows, wi, 0, 1, first)

    def project_early(slot, first=False):
        at = pl.ds(*EPARTS[0])
        n = (xe[slot, at, :].astype(F32) - stat_e[at, 0:1]) * stat_e[at, 1:2]
        n = n * (1.0 + modv[slot, pl.ds(1, 1), :]) + modv[slot, pl.ds(0, 1), :]
        w = wi[pl.ds(pl.multiple_of(slot * PAIR, 128), PAIR), pl.ds(FEAT, 2 * FEAT)]
        p = jnp.dot(n.astype(BF16), w, preferred_element_type=F32)
        if first:
            acc_e[at, :] = p
        else:
            acc_e[at, :] += p

    score_scale = math.log2(math.e) / math.sqrt(HD)

    def head_norm(values, gain):
        square = jnp.mean(values * values, axis=-1, keepdims=True)
        return (values * lax.rsqrt(square + NORM_EPSILON) * gain).astype(BF16)

    def q_rows(part):
        start, rows = PARTS[part]
        if part == 0:
            return start, start, rows
        skip = TXT if part == 1 else 0
        return start + skip, start + skip - TXT, rows - skip

    def finish(part):
        at = pl.ds(*PARTS[part])
        for h in range(HEADS):
            keys = acc[at, pl.ds(FEAT + h * HD, HD)]
            kv[z, at, pl.ds(2 * h * HD, HD)] = head_norm(keys, kg_ref[...])
            vals = acc[at, pl.ds(2 * FEAT + h * HD, HD)]
            kv[z, at, pl.ds((2 * h + 1) * HD, HD)] = vals.astype(BF16)
        token, query, rows = q_rows(part)
        for h in range(HEADS):
            q = acc[pl.ds(token, rows), pl.ds(h * HD, HD)]
            qall[0, pl.ds(query, rows), pl.ds(h * HD, HD)] = head_norm(
                q, qg_ref[...] * score_scale
            )

    def finish_early(k):
        slot = (zm, zp, zo)[k]
        at = pl.ds(k * EARLY, EARLY)
        to = pl.ds(EARLY_AT, EARLY)
        for h in range(HEADS):
            keys = acc_e[at, pl.ds(h * HD, HD)]
            kv[slot, to, pl.ds(2 * h * HD, HD)] = head_norm(keys, kg_ref[...])
            kv[slot, to, pl.ds((2 * h + 1) * HD, HD)] = acc_e[at, pl.ds(FEAT + h * HD, HD)].astype(BF16)

    def z_slot(d, k, sending):
        if k < 2:
            return (z if sending else (zm, zp)[d]), (k if d == 0 else 1 - k)
        return ((zm, zp)[d] if sending else zo), d

    def z_copy(d, g, k, sending):
        slot, sub = z_slot(d, k, sending)
        part, h, heads = GROUPS[g]
        ref = kv.at[slot, piece(part, sub, ZPARTS), pl.ds(2 * h * HD, 2 * heads * HD)]
        return remote(ref, ref, z_s.at[d, g, k], z_r.at[d, g, k], z_dev[d])

    def q_copy(part):
        _, query, rows = q_rows(part)
        at = pl.ds(query, rows)
        return remote(qall.at[0, at], qall.at[1, at], q_s.at[part], q_r.at[part], x_dev)

    def z_own(g, pieces=(0, 1)):
        for k in pieces:
            for d in range(2):
                go(z_copy(d, g, k, True))

    def z_first(g):
        for d in range(2):
            z_copy(d, g, 0, False).wait_recv()
            go(z_copy(d, g, 2, True))

    def z_wait(g, k):
        for d in range(2):
            z_copy(d, g, k, False).wait_recv()

    own_copy(mate_cols).wait_recv()
    project(y, 0, first=True)
    y_ready(0, 0)
    y_ready(0, 1)
    project(ym, 0)
    project(yp, 0)
    y_relay(0, 2)
    y_ready(0, 2)
    project(yo, 0)
    finish(0)
    z_own(0)
    go(q_copy(0))

    y_first(1)
    y_own(2)
    for k in range(3):
        early_copy(k).wait_recv()
    go(early_mate(cols))
    st_early[t] = shard_stats(xe[y, :, cols].astype(F32), EPAD)
    for j in range(1, 8):
        go(peer_copy(st_early, se_s, se_r, "tensor", t, j))
    project(y, 1, first=True)
    y_relay(1, 1)
    y_ready(1, 0)
    y_ready(1, 1)
    project(ym, 1)
    project(yp, 1)
    z_first(0)
    y_relay(1, 2)
    project(y, 2, first=True)
    y_ready(1, 2)
    project(yo, 1)
    finish(1)
    z_own(1)
    go(q_copy(1))

    y_first(2)
    y_own(3)
    y_relay(2, 1)
    y_ready(2, 0)
    y_ready(2, 1)
    project(ym, 2)
    project(yp, 2)
    z_first(1)
    y_relay(2, 2)
    for j in range(1, 8):
        peer_arrival(st_early, se_s, se_r, "tensor", t, j).wait_recv()
    stat_e[...] = token_stats(st_early, EPAD)
    early_mate(mate_cols).wait_recv()
    project_early(y, first=True)
    y_first(3)
    y_ready(2, 2)
    project(yo, 2)
    finish(2)
    z_own(2)
    z_own(3)
    z_own(4, (0,))
    go(q_copy(2))

    for copy in late:
        copy.wait()
    wo_send = remote(my_wo, my_wo, wo_s.at[0], wo_r.at[0], mate)
    go(wo_send)

    length = length_ref[group]

    def values(slot, start, rows, h):
        at = pl.ds(start, rows)
        vals = kv[slot, at, pl.ds((2 * h + 1) * HD, HD)].astype(F32).T
        ones = jnp.ones((VROWS - HD, rows), F32)
        if start <= HEAD_ROWS:
            pos = start - HEAD_ROWS + lax.broadcasted_iota(jnp.int32, (1, rows), 1)
            used = (pos < 0) | (pos >= TXT) | (pos + (xlo * RING + slot) * TXT < length)
            vals = jnp.where(used, vals, 0.0)
            ones = jnp.where(used, ones, 0.0)
        return jnp.concatenate([vals, ones], axis=0).astype(BF16)

    def weighted(slot, start, rows, h, ext, q, at_q):
        scores = lax.dot_general(
            kv[slot, pl.ds(start, rows), pl.ds(2 * h * HD, HD)],
            qall[q, at_q, pl.ds(h * HD, HD)],
            (((1,), (1,)), ((), ())),
            preferred_element_type=F32,
        )
        return jnp.dot(ext, jnp.exp2(scores).astype(BF16), preferred_element_type=F32)

    def attend(slot, h, sets, start=0, rows=TOK, first=False):
        ext = values(slot, start, rows, h)
        for q in sets:
            o = weighted(slot, start, rows, h, ext, q, pl.ds(0, IMG))
            if first:
                oacc[q, h] = o
            else:
                oacc[q, h] += o

    order = (yo, yp, ym, y)

    def lanes(i):
        return pl.ds(pl.multiple_of(i * 128, 128), 128)

    def o_copy(h, j):
        at = lanes(order[j])
        k = h * RING + j
        return remote(osend.at[h, :, at], orecv.at[h, :, at], o_s.at[k], o_r.at[k], x_dev)

    def pack(o, h, at):
        den = o[HD : HD + 1]
        high = den.astype(BF16).astype(F32)
        middle = (den - high).astype(BF16).astype(F32)
        low = den - high - middle
        osend[h, pl.ds(0, HD), at] = o[:HD].astype(BF16)
        pad = jnp.zeros((VROWS - HD - 3, den.shape[1]), F32)
        osend[h, pl.ds(HD, VROWS - HD), at] = jnp.concatenate(
            [high, middle, low, pad], axis=0
        ).astype(BF16)

    whole = pl.ds(0, IMG)

    for h in range(HEADS):
        attend(z, h, (0,), first=True)
    y_relay(3, 1)
    z_wait(0, 1)
    z_wait(0, 2)
    z_wait(1, 1)
    for h in range(HEADS):
        attend(zm, h, (0,), 0, EARLY_AT)
        attend(zp, h, (0,), 0, EARLY_AT)
    z_wait(1, 2)
    for h in range(HEADS):
        attend(zo, h, (0,), 0, EARLY_AT)
    z_first(2)
    z_own(4, (1,))
    y_ready(3, 0)
    y_ready(3, 1)
    project_early(ym)
    project_early(yp)
    y_relay(3, 2)
    for part in range(3):
        q_copy(part).wait_recv()
    for h in range(HEADS):
        attend(z, h, (1,), first=True)
        if h == 1:
            z_first(3)
    y_ready(3, 2)
    project_early(yo)
    for k in range(3):
        finish_early(k)
    z_wait(2, 1)
    attend(zm, 0, (1,))
    attend(zp, 0, (1,))
    z_first(4)
    z_wait(3, 1)
    attend(zm, 1, (1,))
    attend(zp, 1, (1,))
    z_wait(2, 2)
    attend(zo, 0, (1,))
    pack(oacc[1, 0], 0, whole)
    for j in range(3):
        go(o_copy(0, j))
    z_wait(4, 1)
    attend(zm, 2, (1,))
    z_wait(3, 2)
    attend(zo, 1, (1,))
    pack(oacc[1, 1], 1, whole)
    for j in range(2):
        go(o_copy(1, j))
    attend(zp, 2, (1,))
    attend(zo, 2, (1,), 0, LATE_AT)
    z_wait(4, 2)

    last = values(zo, *ZPARTS[2], 2)
    for j in range(RING):
        at = lanes(order[j])
        pack(oacc[1, 2, :, at] + weighted(zo, *ZPARTS[2], 2, last, 1, at), 2, at)
        go(o_copy(2, j))
        if j == 1:
            go(o_copy(1, 2))
        if j == 2:
            go(o_copy(0, 3))
            go(o_copy(1, 3))
    for h in range(HEADS):
        for slot in (zm, zp, zo):
            attend(slot, h, (0,), EARLY_AT, TOK - EARLY_AT)

    def a_copy(j, columns):
        return remote(
            atts.at[j, pl.ds(pl.multiple_of((1 - c) * CH, CH), CH)],
            attb.at[j, :, columns],
            a_s.at[j],
            a_r.at[j],
            mate,
        )

    def combine(j):
        at = lanes(order[j])
        for h in range(HEADS):
            o_copy(h, j).wait_recv()
        heads = []
        for h in range(HEADS):
            tail = orecv[h, pl.ds(HD, VROWS - HD), at].astype(F32)
            num = oacc[0, h, pl.ds(0, HD), at] + orecv[h, pl.ds(0, HD), at].astype(F32)
            den = oacc[0, h, pl.ds(HD, 1), at] + (tail[0:1] + tail[1:2] + tail[2:3])
            heads.append((num / den).T)
        atts[j] = jnp.concatenate(heads, axis=1).astype(BF16)
        go(a_copy(j, cols))
        attb[j, :, cols] = atts[j, pl.ds(pl.multiple_of(c * CH, CH), CH), :]

    half = WIDTH // 2
    sides = (pl.ds(0, half), pl.ds(half, half))

    def p_copy(d, k):
        src = (pso.at[d], pdir.at[d], pacc.at[d])[k]
        dst = (ropp.at[d], rdir.at[d], racc.at[d])[k]
        return remote(src, dst, p_s.at[d, k], p_r.at[d, k], y_dev[d])

    def out_side(j, d):
        return jnp.dot(attb[j], wo[:, sides[d]], preferred_element_type=F32)

    def dispatch(j):
        a_copy(j, mate_cols).wait_recv()
        if j == 0:
            for d in range(2):
                pso[d] = out_side(0, d).astype(BF16)
                go(p_copy(d, 0))
        else:
            keep, direct = j - 1, 2 - j
            pdir[keep] = out_side(j, direct).astype(BF16)
            go(p_copy(keep, 1))
            pown[:, sides[keep]] = out_side(j, keep)

    remote(my_wo, wo.at[pl.ds(pl.multiple_of((1 - c) * FEAT, 128), FEAT)], wo_s.at[0], wo_r.at[0], mate).wait_recv()
    for j in range(3):
        combine(j)
        dispatch(j)
    for d in range(2):
        p_copy(d, 0).wait_recv()
        pacc[d] = (pown[:, sides[d]] + ropp[d].astype(F32)).astype(BF16)
        go(p_copy(d, 2))
    combine(3)
    a_copy(3, mate_cols).wait_recv()
    mine = [out_side(3, d) for d in range(2)]
    for d in range(2):
        p_copy(1 - d, 1).wait_recv()
        pown[:, sides[d]] = mine[d] + rdir[1 - d].astype(F32)
    for d in range(2):
        p_copy(d, 2).wait_recv()
        pown[:, sides[d]] += racc[d].astype(F32)

    row = t * CH + TXT * lax.min(lax.div(t * CH, HEAD_ROWS), 1)
    rows = pl.ds(pl.multiple_of(row, CH), CH)
    resid = jnp.concatenate(
        [
            xg[i, rows, :].astype(F32)
            + modv[i, pl.ds(2, 1), :] * pown[:, pl.ds(i * PAIR, PAIR)]
            for i in range(RING)
        ],
        axis=1,
    )
    row_mean = jnp.mean(resid, axis=-1, keepdims=True)
    resid = resid - row_mean
    row_var = jnp.mean(resid * resid, axis=-1, keepdims=True)
    resid = resid * lax.rsqrt(row_var + NORM_EPSILON)
    velocity = jnp.zeros((CH, CH), F32)
    for i in range(RING):
        n = resid[:, i * PAIR : (i + 1) * PAIR] * (1.0 + modv[i, pl.ds(6, 1), :]) + modv[
            i, pl.ds(5, 1), :
        ]
        velocity += lax.dot_general(
            n.astype(BF16),
            fw_ref[:, pl.ds(i * PAIR, PAIR)],
            (((1,), (1,)), ((), ())),
            preferred_element_type=F32,
        )

    total_steps = mod_ref.shape[0]
    count = total_steps + 1.0
    step_delta = -1.0 / count
    flow = (total_steps - jnp.full((1, CH), step, jnp.int32).astype(F32)) / count
    sigma = NOISE_LEVEL * jnp.sqrt(flow / (1.0 - flow))
    spread = sigma * math.sqrt(1.0 / count)
    pull = sigma * sigma / (2.0 * flow)

    def drift(state, v):
        return state + (v + pull * (state + (1.0 - flow) * v)) * step_delta

    latent = lat_ref[...]
    noise = noise_ref[...]
    step_mean = drift(latent, velocity)
    mean_ref[0] = step_mean
    shifted = noise + (drift(latent, old_ref[...].astype(F32)) - step_mean) / spread
    gap = noise * noise - shifted * shifted
    gap = jnp.sum(jnp.sum(gap, axis=1, keepdims=True), axis=0, keepdims=True) * 0.5
    me = s * 8 + t
    rat[me] = jnp.broadcast_to(gap, (1, 128))

    def spot(step, here):
        return lax.rem(here + step, RING)

    seqs = [(1 - xlo if a else xlo) * RING + spot(b, z) for a in range(2) for b in range(RING)]
    tens = [spot(b, y) * 2 + (1 - c if a else c) for a in range(2) for b in range(RING)]
    hops = (0, 1, 2, 1, 1, 2, 3, 2)
    pairs = [(i, j) for i in range(8) for j in range(8) if i or j]
    for i, j in sorted(pairs, key=lambda p: -hops[p[0]] - hops[p[1]]):
        where = {"seq": seqs[i], "tensor": tens[j]}
        remote(rat.at[me], rat.at[me], r_s.at[0], r_r.at[0], where).start()
    told = rat.at[pl.ds(0, 63)]
    everyone = remote(told, told, r_s.at[0], r_r.at[0], mate)
    everyone.wait_recv()
    elements = 64 * CH * CH
    ratio = jnp.sum(rat[...], axis=0) / elements
    ratio_ref[0] = ratio[0, 0]
    everyone.wait_send()
    for copy in sends:
        copy.wait_send()


def shards(
    image_states,
    text_states,
    image_qkv,
    text_qkv,
    image_out,
    final_weight,
    query_gain,
    key_gain,
    modulation,
    latent,
    old_velocity,
    rollout_noise,
    group_ids,
    text_lengths,
    step_ids,
):
    smem = pl.BlockSpec(memory_space=pltpu.SMEM)
    vmem = pl.BlockSpec(memory_space=pltpu.VMEM)
    hbm = pl.BlockSpec(memory_space=pl.ANY)
    dma = pltpu.SemaphoreType.DMA
    half = WIDTH // 2
    return pl.pallas_call(
        block,
        out_shape=(
            pltpu.VMEM(latent.shape, F32),
            pltpu.SMEM((1,), F32),
        ),
        in_specs=[hbm] * 15,
        out_specs=(vmem, smem),
        scratch_shapes=[
            pltpu.SMEM((1,), jnp.int32),
            pltpu.SMEM((1,), jnp.int32),
            pltpu.SMEM((4,), jnp.int32),
            pltpu.VMEM(text_states.shape, BF16),
            pltpu.VMEM((WIDTH, 3 * FEAT), BF16),
            pltpu.VMEM((WIDTH, 3 * FEAT), BF16),
            pltpu.VMEM((PAIR, WIDTH), BF16),
            pltpu.VMEM((CH, WIDTH), BF16),
            pltpu.VMEM((1, HD), F32),
            pltpu.VMEM((1, HD), F32),
            pltpu.VMEM(modulation.shape, F32),
            pltpu.VMEM((CH, CH), F32),
            pltpu.VMEM((CH, CH), BF16),
            pltpu.VMEM((CH, CH), F32),
            pltpu.VMEM((RING, TOK, PAIR), BF16),
            pltpu.VMEM((RING, 3 * EARLY, PAIR), BF16),
            pltpu.VMEM((RING, 8, PAIR), F32),
            pltpu.VMEM((PAD, 128), F32),
            pltpu.VMEM((8, 2, PAD), F32),
            pltpu.VMEM((8, 2, EPAD), F32),
            pltpu.VMEM((PAD, 128), F32),
            pltpu.VMEM((EPAD, 128), F32),
            pltpu.VMEM((TOK, 3 * FEAT), F32),
            pltpu.VMEM((3 * EARLY, 2 * FEAT), F32),
            pltpu.VMEM((2, IMG, FEAT), BF16),
            pltpu.VMEM((RING, TOK, PAIR), BF16),
            pltpu.VMEM((2, HEADS, VROWS, IMG), F32),
            pltpu.VMEM((HEADS, VROWS, IMG), BF16),
            pltpu.VMEM((HEADS, VROWS, IMG), BF16),
            pltpu.VMEM((RING, 128, FEAT), BF16),
            pltpu.VMEM((RING, CH, PAIR), BF16),
            pltpu.VMEM((2, CH, half), BF16),
            pltpu.VMEM((2, CH, half), BF16),
            pltpu.VMEM((2, CH, half), BF16),
            pltpu.VMEM((CH, WIDTH), F32),
            pltpu.VMEM((2, CH, half), BF16),
            pltpu.VMEM((2, CH, half), BF16),
            pltpu.VMEM((2, CH, half), BF16),
            pltpu.VMEM((64, 1, 128), F32),
            dma((20,)),
            dma((8,)),
            dma((8,)),
            dma((1,)),
            dma((1,)),
            dma((4,)),
            dma((4,)),
            dma((8,)),
            dma((8,)),
            dma((2, 4, 3)),
            dma((2, 4, 3)),
            dma((2, 4, 3)),
            dma((2, 4, 3)),
            dma((2, 5, 3)),
            dma((2, 5, 3)),
            dma((3,)),
            dma((3,)),
            dma((12,)),
            dma((12,)),
            dma((RING,)),
            dma((RING,)),
            dma((1,)),
            dma((1,)),
            dma((2, 3)),
            dma((2, 3)),
            dma((1,)),
            dma((1,)),
        ],
        compiler_params=pltpu.CompilerParams(
            collective_id=0, has_side_effects=True, vmem_limit_bytes=62 * 1024 * 1024
        ),
    )(
        step_ids,
        group_ids,
        text_lengths,
        image_states,
        text_states,
        jnp.transpose(image_qkv, (1, 0, 2)),
        jnp.transpose(text_qkv, (1, 0, 2)),
        image_out,
        final_weight.T,
        query_gain.reshape(1, HD),
        key_gain.reshape(1, HD),
        modulation,
        latent,
        old_velocity,
        rollout_noise,
    )


def solution(mesh):
    placed = (
        P("dp", "seq", "tensor"),
        P(None, "seq", "tensor"),
        P(None, None, "tensor"),
        P(None, None, "tensor"),
        P("tensor", None),
        P(),
        P(),
        P(),
        P(),
        P("dp", ("seq", "tensor"), None),
        P("dp", ("seq", "tensor"), None),
        P("dp", ("seq", "tensor"), None),
        P("dp"),
        P(),
        P("dp"),
    )
    return jax.shard_map(
        shards,
        mesh=mesh,
        in_specs=placed,
        out_specs=(P("dp", ("seq", "tensor"), None), P("dp")),
        check_vma=False,
    )
```
